32 devices in a mesh: row: 4 (over y, x), col: 8 (over z, core).
Axes of the slice: x: 2, y: 2, z: 4, core: 2. Of those that a mesh axis runs over, the one named last changes fastest.
Arguments:
- wrapped: float32 [1, 4096, 8192], P(None, 'row', 'col'), may hold values from -2.8 to 2.8
- col_steps: int32 [1, 4, 8], P(None, 'row', 'col'), may hold values from -2 to 2, as said below
- row_steps: int32 [1, 4, 8], P(None, 'row', 'col'), may hold values from -2 to 2, as said below
Outputs:
- unwrapped: float32 [1, 4096, 8192], P(None, 'row', 'col')
The draws below stay inside these ranges and needn't reach their ends.
Inputs may be any that keep to these rules, and one draw needn't show every extreme that they name: `col_steps`: nonzero whole numbers; the last tile column has no edge. `row_steps`: nonzero whole numbers; the last tile row has no edge.
All inputs are finite; a program needn't handle non-finite values.
Results may differ from the reference program's by a relative error of at most 0.0003.
Values sent between devices are 32-bit elements; how exact they have to be, the bound alone decides.
A program may use at most 64 MiB of HBM per device.

```python
import math
import jax
import jax.numpy as jnp
from jax import lax

FRAMES = 1
TILE_ROWS = 1024
TILE_COLS = 1024
ITERS = 2
IMAGE_ROWS = 4096
IMAGE_COLS = 8192
N_ROW = 4
N_COL = 8


TWO_PI = 2.0 * math.pi


def draw_wrapped(key, part):
    extent = (FRAMES, IMAGE_ROWS, IMAGE_COLS)
    levels = jax.random.randint(jax.random.fold_in(key, 1), extent, -3, 4)
    speckle = jax.random.randint(jax.random.fold_in(key, 2), extent, 0, 5)
    levels = jnp.where(speckle == 0, levels, 0)
    jitter = jnp.clip(0.04 * jax.random.normal(jax.random.fold_in(key, 3), extent, jnp.float32), -0.1, 0.1)
    return (TWO_PI / 7.0 * levels.astype(jnp.float32) + jitter).astype(jnp.float32)


def signed_steps(key):
    extent = (FRAMES, N_ROW, N_COL)
    magnitude = jax.random.randint(jax.random.fold_in(key, 1), extent, 1, 3)
    polarity = 2 * jax.random.randint(jax.random.fold_in(key, 2), extent, 0, 2) - 1
    return (magnitude * polarity).astype(jnp.int32)


def draw_col_steps(key, part):
    return signed_steps(jax.random.fold_in(key, 11))


def draw_row_steps(key, part):
    return signed_steps(jax.random.fold_in(key, 12))


def setup_inputs(seed: int = 0) -> dict:
    arg_keys = jax.random.split(jax.random.key(seed), 4)
    return {
        "wrapped": draw_wrapped(jax.random.fold_in(arg_keys[3], 71), 0),
        "col_steps": draw_col_steps(jax.random.fold_in(arg_keys[3], 71), 0),
        "row_steps": draw_row_steps(jax.random.fold_in(arg_keys[3], 71), 0),
    }


TWO_PI = 2.0 * math.pi


def wrap_diff(change):
    return change - TWO_PI * jnp.floor(change / TWO_PI + 0.5)


def unwrap_frame(inputs):
    wrapped, col_steps, row_steps = inputs
    grid_x = wrap_diff(wrapped[:, 1:] - wrapped[:, :-1])
    grid_x = jnp.concatenate([grid_x, jnp.zeros((IMAGE_ROWS, 1), grid_x.dtype)], axis=1)
    grid_y = wrap_diff(wrapped[1:, :] - wrapped[:-1, :])
    grid_y = jnp.concatenate([grid_y, jnp.zeros((1, IMAGE_COLS), grid_y.dtype)], axis=0)
    charge = (grid_x[:-1, :-1] + grid_y[:-1, 1:] - grid_x[1:, :-1] - grid_y[:-1, :-1]) / TWO_PI
    charge = jnp.pad(charge, ((1, 0), (1, 0)))
    weight = 1.0 / (1.0 + jnp.abs(charge))
    tiled_shape = (N_ROW, TILE_ROWS, N_COL, TILE_COLS)
    step_x = grid_x.reshape(tiled_shape)
    step_y = grid_y.reshape(tiled_shape)
    weight_tiles = weight.reshape(tiled_shape)
    along_cols = jnp.cumsum(step_x, axis=3) - step_x
    first_column = step_y[:, :, :, 0]
    downward = jnp.cumsum(first_column, axis=1) - first_column
    anchor = wrapped.reshape(tiled_shape)[:, 0, :, 0]
    current = (anchor[:, None, :] + downward)[:, :, :, None] + along_cols
    col_weight = weight_tiles[:, :, :, -1]
    cross_x = step_x[:, :, :, -1]
    row_weight = weight_tiles[:, -1, :, :]
    cross_y = step_y[:, -1, :, :]
    cycles_across = TWO_PI * col_steps.astype(jnp.float32)
    cycles_down = TWO_PI * row_steps.astype(jnp.float32)
    for sweep in range(ITERS):
        beyond_x = jnp.concatenate([current[:, :, 1:, 0], jnp.zeros((N_ROW, TILE_ROWS, 1), current.dtype)], axis=2)
        horizontal = jnp.sum(col_weight * (current[:, :, :, -1] + cross_x - beyond_x), axis=1) / jnp.sum(col_weight, axis=1)
        beyond_y = jnp.concatenate([current[1:, 0, :, :], jnp.zeros((1, N_COL, TILE_COLS), current.dtype)], axis=0)
        vertical = jnp.sum(row_weight * (current[:, -1, :, :] + cross_y - beyond_y), axis=2) / jnp.sum(row_weight, axis=2)
        horizontal = horizontal + cycles_across
        vertical = vertical + cycles_down
        prefix_across = jnp.cumsum(horizontal, axis=1) - horizontal
        prefix_down = jnp.cumsum(vertical, axis=0) - vertical
        offset = 0.5 * (prefix_across + prefix_across[0:1, :] + prefix_down + prefix_down[:, 0:1])
        current = current + offset[:, None, :, None]
    return (current / TWO_PI).reshape(IMAGE_ROWS, IMAGE_COLS)


def reference(wrapped, col_steps, row_steps):
    return lax.map(unwrap_frame, (wrapped, col_steps, row_steps))
```

```python
import functools
import math

import jax
import jax.numpy as jnp
from jax import lax
from jax.experimental import pallas as pl
from jax.experimental.pallas import tpu as pltpu
from jax.sharding import PartitionSpec as P

ITERS = 2
TWO_PI = 2.0 * math.pi
MESH = pl.DeviceIdType.MESH
LANES = 128
STRIP = 16


def cycles(change):
    return jnp.floor(change * (1.0 / TWO_PI) + 0.5)


def iota(shape, dim):
    return lax.broadcasted_iota(jnp.int32, shape, dim)


def total(values):
    return jnp.sum(values, axis=1, keepdims=True)


def shifted_in(values, first):
    lane = iota(values.shape, 1)
    return jnp.where(lane == 0, first, pltpu.roll(values, 1, 1))


def triangle(size, dim):
    ordered = iota((size, size), dim) <= iota((size, size), 1 - dim)
    return ordered.astype(jnp.float32).astype(jnp.bfloat16)


def line_counts(line, step):
    lane = iota(line.shape, 1)
    floors = jnp.where(lane == 0, 0.0, cycles(line - pltpu.roll(line, 1, 1)))
    floors = jnp.broadcast_to(floors, (16, line.shape[1]))
    upper, ones = triangle(step, 0), jnp.ones((step, step), jnp.bfloat16)
    earlier, counts = None, []
    for b in range(line.shape[1] // step):
        piece = floors[:, b * step : (b + 1) * step]
        count = jnp.dot(piece.astype(jnp.bfloat16), upper, preferred_element_type=jnp.float32)
        if b > 0:
            count = count + jnp.dot(
                earlier.astype(jnp.bfloat16), ones, preferred_element_type=jnp.float32
            )
        earlier = piece if b == 0 else earlier + piece
        counts.append(count[0:1, :])
    return jnp.concatenate(counts, axis=1)


def edge_kernel(
    names, sizes, rows_step, cols_step,
    wrapped, col_steps, row_steps,
    integ, offset,
    cells, left_out, right_in, rows_out, rows_in, corner_above, corner_diag,
    first_counts, end_lines, row_sums, floors, steps_across, steps_down, mine_h, mine_u,
    row_h, top_h, col_u, left_u,
    recv_sem, row_recv, top_recv, col_recv, left_recv, diag_in, row_in, far_in,
    load_sem, send_sem, h_send, u_send,
):
    row_name, col_name = names
    grid_rows, grid_cols = sizes
    tile_rows, tile_cols = cells.shape
    my_row, my_col = lax.axis_index(row_name), lax.axis_index(col_name)

    chunks = tile_rows // rows_step
    rest = pl.ds(LANES, tile_cols - LANES)
    regions = [
        (pl.ds(0, tile_rows), pl.ds(0, LANES)),
        (pl.ds(tile_rows - 16, 16), rest),
        (pl.ds(0, 16), rest),
    ]
    for q in range(chunks):
        top = max(q * rows_step, 16)
        bottom = min((q + 1) * rows_step, tile_rows - 16)
        regions.append((pl.ds(top, bottom - top), rest))
    loads = []
    for k, (rows, cols) in enumerate(regions):
        loads.append(
            pltpu.make_async_copy(wrapped.at[0, rows, cols], cells.at[rows, cols], load_sem.at[k])
        )
        loads[-1].start()
    for source, target in ((col_steps, steps_across), (row_steps, steps_down)):
        loads.append(pltpu.make_async_copy(source, target, load_sem.at[len(loads)]))
        loads[-1].start()

    def span(low, high, act):
        def step(k, carry):
            act(k)
            return carry

        lax.fori_loop(low, high, step, 0)

    def rows_below(act):
        span(my_row + 1, grid_rows, lambda r: act(r, my_col))

    def cols_right(act):
        span(my_col + 1, grid_cols, lambda c: act(my_row, c))

    def far_from_top(act):
        first = jnp.where(my_row == 0, 1, grid_rows)
        span(first, grid_rows, lambda r: span(my_col + 1, grid_cols, lambda c: act(r, c)))

    def far_from_left(act):
        first = jnp.where((my_row > 0) & (my_col == 0), my_row + 1, grid_rows)
        span(first, grid_rows, lambda r: span(1, grid_cols, lambda c: act(r, c)))

    def rows_further_below(act):
        span(my_row + 2, grid_rows, lambda r: act(r, my_col))

    def rows_further_above(act):
        span(0, my_row - 1, lambda r: act(r, my_col))

    def cols_left(act):
        span(0, my_col, lambda c: act(my_row, c))

    def tops_left(act):
        span(0, jnp.where(my_row > 0, my_col, 0), lambda c: act(0, c))

    def lefts_above(act):
        span(1, jnp.where(my_col > 0, my_row, 0), lambda r: act(r, 0))

    has_left, has_right = my_col > 0, my_col < grid_cols - 1
    has_above, has_below = my_row > 0, my_row < grid_rows - 1
    inner_diag = (my_row > 0) & (my_col > 0) & has_right & has_below
    inner_back = (my_row > 1) & (my_col > 1)

    zero_line = jnp.zeros((1, LANES), jnp.float32)
    for slots in (row_h, top_h, col_u, left_u):
        for k in range(slots.shape[0]):
            slots[k] = zero_line

    barrier = pltpu.get_barrier_semaphore()

    def await_signals(semaphore, count):

        @pl.when(count > 0)
        def _():
            pl.semaphore_wait(semaphore, count)

    def greet(semaphore):
        return lambda r, c: pl.semaphore_signal(
            semaphore, inc=1, device_id=(r, c), device_id_type=MESH
        )

    cols_right(greet(barrier))
    rows_further_below(greet(barrier))
    far_from_top(greet(barrier))
    far_from_left(greet(barrier))

    @pl.when(inner_diag)
    def _():
        greet(barrier)(my_row + 1, my_col + 1)

    @pl.when(has_above)
    def _():
        greet(barrier)(my_row - 1, my_col)

    @pl.when(jnp.logical_not(has_right))
    def _():
        right_in[...] = jnp.zeros(right_in.shape, jnp.float32)

    @pl.when(jnp.logical_not(has_above))
    def _():
        corner_above[...] = jnp.zeros(corner_above.shape, jnp.float32)

    @pl.when(jnp.logical_not(has_above & has_left))
    def _():
        corner_diag[...] = jnp.zeros(corner_diag.shape, jnp.float32)

    corner = cells.at[pl.ds(tile_rows - 8, 8), pl.ds(tile_cols - LANES, LANES)]
    links = (
        (left_out, right_in, 0, -1, has_left, has_right),
        (corner, corner_above, 1, 0, has_below, has_above),
        (rows_out, rows_in, 1, 0, has_below, has_above),
        (corner, corner_diag, 1, 1, has_below & has_right, has_above & has_left),
    )

    def link_copy(k):
        source, target, d_row, d_col, _, _ = links[k]
        place = (
            lax.rem(my_row + d_row + grid_rows, grid_rows),
            lax.rem(my_col + d_col + grid_cols, grid_cols),
        )
        return pltpu.make_async_remote_copy(
            src_ref=source, dst_ref=target, send_sem=send_sem.at[k], recv_sem=recv_sem.at[k],
            device_id=place, device_id_type=MESH,
        )

    first = my_row == grid_rows - 1
    last = (my_row == 0) & (my_col <= 1)
    between = jnp.logical_not(first | last)

    def enter():
        sources = my_col + jnp.maximum(my_row - 1, 0)
        sources = sources + jnp.where(my_row > 0, my_col, 0)
        sources = sources + jnp.where((my_col > 0) & (my_row > 0), my_row - 1, 0)
        sources = sources + jnp.where(inner_back, 1, 0) + jnp.where(has_below, 1, 0)
        await_signals(barrier, sources)

        cols_left(greet(row_in))
        rows_further_above(greet(far_in))
        tops_left(greet(far_in))
        lefts_above(greet(far_in))

        @pl.when(has_above & has_left)
        def _():
            greet(diag_in)(my_row - 1, my_col - 1)

    def push_left():

        @pl.when(has_left)
        def _():
            link_copy(0).start()

    def push_down():

        @pl.when(has_below)
        def _():
            link_copy(1).start()
            link_copy(2).start()

    with jax.named_scope("enter_0"):
        pl.when(first)(enter)

    with jax.named_scope("load_head"):
        loads[0].wait()
    with jax.named_scope("head"):
        for q in range(chunks):
            part = slice(q * rows_step, (q + 1) * rows_step)
            left_out[0:1, part] = cells[part, 0:LANES].T[0:1, :]
        left_out[1:2, :] = line_counts(left_out[0:1, :], rows_step)

    with jax.named_scope("enter_1"):
        pl.when(between)(enter)
        pl.when(jnp.logical_not(last))(push_left)

    with jax.named_scope("load_edges"):
        loads[1].wait()
        loads[-1].wait()
        loads[-2].wait()
    with jax.named_scope("last_row"):
        down_steps = steps_down[0].astype(jnp.float32)
        rows_out[0:1, :] = cells[tile_rows - 1 : tile_rows, :]
        rows_out[1:2, :] = cells[tile_rows - 2 : tile_rows - 1, :]
        rows_out[2:3, :] = (left_out[1:2, tile_rows - 1 :] - down_steps) + line_counts(
            cells[tile_rows - 1 : tile_rows, :], cols_step
        )

    pl.when(jnp.logical_not(last))(push_down)

    lane = iota((STRIP, LANES), 1)

    def strip(k, carry):
        rows = pl.ds(pl.multiple_of(k * STRIP, STRIP), STRIP)
        wrapped_around = cells[rows, 0:LANES]
        sums = jnp.zeros((STRIP, LANES), jnp.float32)
        for j in range(tile_cols // LANES):
            cols = slice(j * LANES, (j + 1) * LANES)
            here = cells[rows, cols]
            rolled = pltpu.roll(here, 1, 1)
            across = cycles(here - jnp.where(lane == 0, wrapped_around, rolled))
            wrapped_around = rolled
            floors[rows, cols] = across.astype(jnp.bfloat16)
            sums = sums + across
        row_sums[rows, :] = sums.astype(jnp.bfloat16)
        return carry

    per_chunk = rows_step // STRIP
    ones = jnp.ones((16, LANES), jnp.bfloat16)
    loads[2].wait()
    for q in range(chunks):
        with jax.named_scope(f"load_{q}"):
            loads[q + 3].wait()
        with jax.named_scope(f"floors_{q}"):
            lax.fori_loop(
                q * per_chunk, (q + 1) * per_chunk, strip, 0, unroll=math.gcd(per_chunk, 8)
            )
        if q == (chunks - 1) // 2:
            with jax.named_scope("enter_2"):

                @pl.when(last)
                def _():
                    enter()
                    push_left()
                    push_down()

    with jax.named_scope("ends"):
        for q in range(chunks):
            part = slice(q * rows_step, (q + 1) * rows_step)
            sums = lax.dot_general(
                ones, row_sums[part, :], (((1,), (1,)), ((), ())),
                preferred_element_type=jnp.float32,
            )
            end_lines[0:1, part] = left_out[1:2, part] + sums[0:1, :]
            end_lines[1:3, part] = cells[part, tile_cols - LANES :].T[LANES - 2 :, :]

    def arrived(k):

        @pl.when(links[k][5])
        def _():
            link_copy(k).wait_recv()

    def base(inner, outer, inner_before, outer_before, at_image_edge, first, count, beyond):
        over = cycles(outer - inner)
        over_before = shifted_in(over, cycles(outer_before - inner_before))
        along_outer = cycles(outer - shifted_in(outer, outer_before))
        along_inner = cycles(inner - shifted_in(inner, inner_before))
        charge = over_before + along_outer - over - along_inner
        charge = jnp.where((iota(charge.shape, 1) == 0) & at_image_edge, 0.0, charge)
        weight = 1.0 / (1.0 + jnp.abs(charge))
        jump = beyond - count - cycles(first - outer)
        return total(weight * jump) / total(weight)

    with jax.named_scope("halo_0"):
        arrived(0)
    with jax.named_scope("halo_1"):
        arrived(1)
    with jax.named_scope("base_h"):
        across_base = base(
            end_lines[1:2, :], end_lines[2:3, :],
            corner_above[7:8, LANES - 2 : LANES - 1], corner_above[7:8, LANES - 1 : LANES],
            my_row == 0, right_in[0:1, :], end_lines[0:1, :], right_in[1:2, :],
        ) + steps_across[0].astype(jnp.float32)
        mine_h[...] = jnp.broadcast_to(across_base, mine_h.shape)

    def h_copy(row, col, target, semaphore, owner):
        return pltpu.make_async_remote_copy(
            src_ref=mine_h, dst_ref=target.at[owner], send_sem=h_send.at[row * grid_cols + col],
            recv_sem=semaphore, device_id=(row, col), device_id_type=MESH,
        )

    def u_copy(row, col, target, semaphore, owner):
        return pltpu.make_async_remote_copy(
            src_ref=mine_u, dst_ref=target.at[owner], send_sem=u_send.at[row * grid_cols + col],
            recv_sem=semaphore, device_id=(row, col), device_id_type=MESH,
        )

    def row_copy(r, c, owner):
        return h_copy(r, c, row_h, row_recv, owner)

    def top_copy(r, c, owner):
        return h_copy(r, c, top_h, top_recv, owner)

    def col_copy(r, c, owner):
        return u_copy(r, c, col_u, col_recv, owner)

    def left_copy(r, c, owner):
        return u_copy(r, c, left_u, left_recv, owner)

    with jax.named_scope("row_in"):
        await_signals(row_in, grid_cols - 1 - my_col)
    with jax.named_scope("tell_row"):
        cols_right(lambda r, c: row_copy(r, c, my_col).start())

    with jax.named_scope("diag_in"):

        @pl.when(has_below & has_right)
        def _():
            pl.semaphore_wait(diag_in, 1)
            link_copy(3).start()

    with jax.named_scope("first_row"):

        @pl.when(has_above)
        def _():
            first_counts[...] = line_counts(cells[0:1, :], cols_step)

    with jax.named_scope("halo_2"):
        arrived(2)
        arrived(3)
    with jax.named_scope("base_u"):

        @pl.when(has_above)
        def _():
            down_base = base(
                rows_in[1:2, :], rows_in[0:1, :],
                corner_diag[6:7, LANES - 1 : LANES], corner_diag[7:8, LANES - 1 : LANES],
                my_col == 0, cells[0:1, :], rows_in[2:3, :], first_counts[...],
            )
            mine_u[...] = jnp.broadcast_to(down_base, mine_u.shape)

        @pl.when(jnp.logical_not(has_above))
        def _():
            mine_u[...] = zero_line

    with jax.named_scope("far_in"):
        below = grid_rows - 1 - my_row
        right = grid_cols - 1 - my_col
        edge = jnp.where((my_row == 0) | (my_col == 0), right, 0)
        await_signals(far_in, jnp.maximum(below - 1, 0) + below * edge)

    to_left_u = jnp.where((my_row > 0) & (my_col == 0), my_row, grid_rows)

    def all_left_u(act):
        span(to_left_u, grid_rows, lambda r: span(1, grid_cols, lambda c: act(r, c)))

    def rows_below_u(act):
        span(jnp.where(my_row > 0, my_row + 1, grid_rows), grid_rows, lambda r: act(r, my_col))

    with jax.named_scope("tell_far"):
        far_from_top(lambda r, c: top_copy(r, c, my_col).start())
        rows_below_u(lambda r, c: col_copy(r, c, my_row).start())
        all_left_u(lambda r, c: left_copy(r, c, my_row).start())

    with jax.named_scope("integrate"):
        upper, lower = triangle(cols_step, 0), triangle(rows_step, 1)
        down_carry = jnp.zeros((1, LANES), jnp.float32)
        for q in range(chunks):
            top = q * rows_step
            rows = pl.ds(top, rows_step)
            head = cells[rows, 0:LANES]
            above = cells[max(top - 1, 0) : max(top, 1), 0:LANES]
            before = jnp.where(iota(head.shape, 0) == 0, above, pltpu.roll(head, 1, 0))
            counts = down_carry + jnp.dot(
                lower, cycles(head - before).astype(jnp.bfloat16), preferred_element_type=jnp.float32
            )
            down_carry = counts[rows_step - 1 : rows_step, :]
            carry = counts[:, 0:1]
            for b in range(tile_cols // cols_step):
                cols = slice(b * cols_step, (b + 1) * cols_step)
                count = carry + jnp.dot(
                    floors[rows, cols], upper, preferred_element_type=jnp.float32
                )
                carry = count[:, cols_step - 1 : cols_step]
                integ[rows, cols] = cells[rows, cols] * (1.0 / TWO_PI) - count

    with jax.named_scope("sent"):
        for k in range(4):

            @pl.when(links[k][4])
            def _():
                link_copy(k).wait_send()

        cols_right(lambda r, c: row_copy(r, c, my_col).wait_send())
        far_from_top(lambda r, c: top_copy(r, c, my_col).wait_send())
        rows_below_u(lambda r, c: col_copy(r, c, my_row).wait_send())
        all_left_u(lambda r, c: left_copy(r, c, my_row).wait_send())

    def hear(slots, semaphore, first, count):
        for n in range(1, slots.shape[0]):

            @pl.when(count == n)
            def _():
                landed = slots.at[pl.ds(first, n)]
                pltpu.make_async_copy(landed, landed, semaphore).wait()

    with jax.named_scope("hear"):
        hear(row_h, row_recv, 0, my_col)
        hear(top_h, top_recv, 0, jnp.where(has_above, my_col, 0))
        hear(col_u, col_recv, 1, jnp.maximum(my_row - 1, 0))
        hear(left_u, left_recv, 1, jnp.where(has_left, my_row, 0))

    with jax.named_scope("finish"):

        def summed(slots):
            line = slots[0]
            for k in range(1, slots.shape[0]):
                line = line + slots[k]
            return line

        across_here = summed(row_h)
        across_top = jnp.where(has_above, summed(top_h), across_here)
        down_here = summed(col_u) + mine_u[...]
        down_left = jnp.where(has_left, summed(left_u), down_here)
        here = left = top = origin = zero_line
        for sweep in range(ITERS):
            prefix_across = across_here + (left - here)
            prefix_across_top = across_top + (origin - top)
            prefix_down = down_here + (top - here)
            prefix_down_left = down_left + (origin - left)
            here = here + 0.5 * (prefix_across + prefix_across_top + prefix_down + prefix_down_left)
            left = left + prefix_down_left
            top = top + prefix_across_top
        offset[...] = jnp.broadcast_to(here, offset.shape)


def place_kernel(integ, offset, out, ready, sems):
    parts = sems.shape[0]
    step = integ.shape[0] // parts
    shift = offset[0:1, 0:1]
    copies = []
    for q in range(parts):
        rows = pl.ds(q * step, step)
        ready[rows, :] = integ[rows, :] + shift
        copy = pltpu.make_async_copy(ready.at[rows], out.at[rows], sems.at[q])
        copy.start()
        copies.append(copy)
    for copy in copies:
        copy.wait()


def on_device(names, sizes, wrapped, col_steps, row_steps):
    frames, tile_rows, tile_cols = wrapped.shape
    devices = sizes[0] * sizes[1]
    rows_step = math.gcd(tile_rows, 256)
    cols_step = math.gcd(tile_cols, 256)
    f32 = jnp.float32


    def with_local_semaphores(*refs):
        dma = pltpu.SemaphoreType.DMA
        pl.run_scoped(
            functools.partial(edge_kernel, names, sizes, rows_step, cols_step, *refs),
            dma((tile_rows // rows_step + 5,)), dma((4,)), dma((devices,)), dma((devices,)),
        )

    call = pl.pallas_call(
        with_local_semaphores,
        out_shape=(
            pltpu.VMEM((tile_rows, tile_cols), f32),
            pltpu.VMEM((8, LANES), f32),
        ),
        in_specs=[
            pl.BlockSpec(memory_space=pltpu.HBM),
            pl.BlockSpec(memory_space=pltpu.HBM),
            pl.BlockSpec(memory_space=pltpu.HBM),
        ],
        out_specs=(
            pl.BlockSpec(memory_space=pltpu.VMEM),
            pl.BlockSpec(memory_space=pltpu.VMEM),
        ),
        scratch_shapes=[
            pltpu.VMEM((tile_rows, tile_cols), f32),
            pltpu.VMEM((2, tile_rows), f32),
            pltpu.VMEM((2, tile_rows), f32),
            pltpu.VMEM((3, tile_cols), f32),
            pltpu.VMEM((3, tile_cols), f32),
            pltpu.VMEM((8, LANES), f32),
            pltpu.VMEM((8, LANES), f32),
            pltpu.VMEM((1, tile_cols), f32),
            pltpu.VMEM((3, tile_rows), f32),
            pltpu.VMEM((tile_rows, LANES), jnp.bfloat16),
            pltpu.VMEM((tile_rows, tile_cols), jnp.bfloat16),
            pltpu.VMEM((1, 1, 1), jnp.int32),
            pltpu.VMEM((1, 1, 1), jnp.int32),
            pltpu.VMEM((1, LANES), f32),
            pltpu.VMEM((1, LANES), f32),
            pltpu.VMEM((sizes[1], 1, LANES), f32),
            pltpu.VMEM((sizes[1], 1, LANES), f32),
            pltpu.VMEM((sizes[0], 1, LANES), f32),
            pltpu.VMEM((sizes[0], 1, LANES), f32),
            pltpu.SemaphoreType.DMA((4,)),
            pltpu.SemaphoreType.DMA,
            pltpu.SemaphoreType.DMA,
            pltpu.SemaphoreType.DMA,
            pltpu.SemaphoreType.DMA,
            pltpu.SemaphoreType.REGULAR,
            pltpu.SemaphoreType.REGULAR,
            pltpu.SemaphoreType.REGULAR,
        ],
        compiler_params=pltpu.CompilerParams(
            collective_id=0, has_side_effects=True, vmem_limit_bytes=57 * 1024 * 1024
        ),
    )
    parts = math.gcd(tile_rows // 8, 16)
    place = pl.pallas_call(
        place_kernel,
        out_shape=jax.ShapeDtypeStruct((tile_rows, tile_cols), f32),
        in_specs=[pl.BlockSpec(memory_space=pltpu.VMEM), pl.BlockSpec(memory_space=pltpu.VMEM)],
        out_specs=pl.BlockSpec(memory_space=pltpu.HBM),
        scratch_shapes=[
            pltpu.VMEM((tile_rows, tile_cols), f32),
            pltpu.SemaphoreType.DMA((parts,)),
        ],
        compiler_params=pltpu.CompilerParams(vmem_limit_bytes=24 * 1024 * 1024),
    )
    outs = [
        place(*call(wrapped[f : f + 1], col_steps[f : f + 1], row_steps[f : f + 1]))
        for f in range(frames)
    ]
    return jnp.stack(outs)


def solution(mesh):
    spec = P(None, "row", "col")
    sizes = (mesh.shape["row"], mesh.shape["col"])
    return jax.shard_map(
        functools.partial(on_device, ("row", "col"), sizes),
        mesh=mesh, in_specs=(spec, spec, spec), out_specs=spec, check_vma=False,
    )
```

```python
import functools
import math

import jax
import jax.numpy as jnp
from jax import lax
from jax.experimental import pallas as pl
from jax.experimental.pallas import tpu as pltpu
from jax.sharding import PartitionSpec as P

ITERS = 2
TWO_PI = 2.0 * math.pi
MESH = pl.DeviceIdType.MESH
LANES = 128
STRIP = 16
RELAYS = 2


def cycles(change):
    return jnp.floor(change * (1.0 / TWO_PI) + 0.5)


def iota(shape, dim):
    return lax.broadcasted_iota(jnp.int32, shape, dim)


def total(values):
    return jnp.sum(values, axis=1, keepdims=True)


def previous(line, first):
    lane, row = iota(line.shape, 1), iota(line.shape, 0)
    along = pltpu.roll(line, 1, 1)
    across = pltpu.roll(along, 1, 0) if line.shape[0] > 1 else along
    return jnp.where(lane > 0, along, jnp.where(row > 0, across, first))


def summed(line):
    return total(jnp.sum(line, axis=0, keepdims=True))


def triangle(size, dim):
    ordered = iota((size, size), dim) <= iota((size, size), 1 - dim)
    return ordered.astype(jnp.float32).astype(jnp.bfloat16)


def line_counts(line):
    groups = line.shape[0]
    row = iota(line.shape, 0)
    floors = cycles(line - previous(line, line[0:1, 0:1]))
    whole, shift = floors, 1
    while shift < groups:
        whole = whole + jnp.where(row >= shift, pltpu.roll(whole, shift, 0), 0.0)
        shift *= 2
    pair = jnp.concatenate([floors, whole - floors], axis=1)
    pair = jnp.concatenate([pair] * (-(-16 // groups)), axis=0).astype(jnp.bfloat16)
    ones = jnp.ones((LANES, LANES), jnp.bfloat16)
    table = jnp.concatenate([triangle(LANES, 0), ones], axis=0)
    return jnp.dot(pair, table, preferred_element_type=jnp.float32)[0:groups, :]


def weights(inner, outer, inner_before, outer_before, at_image_edge):
    over = cycles(outer - inner)
    over_before = previous(over, cycles(outer_before - inner_before))
    along_outer = cycles(outer - previous(outer, outer_before))
    along_inner = cycles(inner - previous(inner, inner_before))
    charge = over_before + along_outer - over - along_inner
    start = (iota(charge.shape, 1) == 0) & (iota(charge.shape, 0) == 0)
    charge = jnp.where(start & at_image_edge, 0.0, charge)
    return 1.0 / (1.0 + jnp.abs(charge))


def mismatch(weight, outer, count, first, beyond):
    jump = beyond - count - cycles(first - outer)
    return summed(weight * jump) / summed(weight)


def edge_kernel(
    names, sizes, rows_step, cols_step,
    wrapped, col_steps, row_steps,
    integ, offset,
    cells, left_out, right_in, corner_above, corner_left, tops, bottom_out, bottoms, inner_row,
    floors, row_sums, steps_across, steps_down, mine_h, mine_y, row_h, top_h, col_h, left_d,
    link_recv, top_recv, bottom_recv, row_recv, far_recv, row_in, col_in, far_in,
    load_sem, link_send, top_send, bottom_send, h_send, c_send, t_send, d_send,
):
    row_name, col_name = names
    grid_rows, grid_cols = sizes
    tile_rows, tile_cols = cells.shape
    my_row, my_col = lax.axis_index(row_name), lax.axis_index(col_name)
    down, right = tile_rows // LANES, tile_cols // LANES

    chunks = tile_rows // rows_step
    rest = pl.ds(LANES, tile_cols - LANES)
    regions = [
        (pl.ds(0, tile_rows), pl.ds(0, LANES)),
        (pl.ds(tile_rows - 16, 16), rest),
        (pl.ds(0, 16), rest),
    ]
    for q in range(chunks):
        top = max(q * rows_step, 16)
        bottom = min((q + 1) * rows_step, tile_rows - 16)
        regions.append((pl.ds(top, bottom - top), rest))
    loads = []
    for k, (rows, cols) in enumerate(regions):
        loads.append(
            pltpu.make_async_copy(wrapped.at[0, rows, cols], cells.at[rows, cols], load_sem.at[k])
        )
        loads[-1].start()
    for source, target in ((col_steps, steps_across), (row_steps, steps_down)):
        loads.append(pltpu.make_async_copy(source, target, load_sem.at[len(loads)]))
        loads[-1].start()

    def span(low, high, act):
        def step(k, carry):
            act(k)
            return carry

        lax.fori_loop(low, high, step, 0)

    def along_row(low, high, act):
        span(low, high, lambda c: act(my_row, c))

    def along_col(low, high, act):
        span(low, high, lambda r: act(r, my_col))

    has_left, has_right = my_col > 0, my_col < grid_cols - 1
    has_above, has_below = my_row > 0, my_row < grid_rows - 1
    near = jnp.minimum(my_row + 3, grid_rows)
    relayed = my_col < RELAYS
    direct_top = (my_row == 0) & jnp.logical_not(relayed)

    def far_below(act):
        low = jnp.where(direct_top, 1, grid_rows)
        span(low, grid_rows, lambda r: span(my_col + 1, grid_cols, lambda c: act(r, c)))

    def direct_tops(act):
        span(RELAYS, jnp.where(has_above, my_col, 0), lambda c: act(0, c))

    zero_line = jnp.zeros((1, LANES), jnp.float32)
    for slots in (row_h, top_h):
        for k in range(grid_cols):
            slots[k] = zero_line

    barrier = pltpu.get_barrier_semaphore()

    def await_signals(semaphore, count):

        @pl.when(count > 0)
        def _():
            pl.semaphore_wait(semaphore, count)

    def greet(semaphore):
        return lambda r, c: pl.semaphore_signal(
            semaphore, inc=1, device_id=(r, c), device_id_type=MESH
        )

    along_row(my_col + 1, grid_cols, greet(barrier))
    along_row(jnp.where(has_below, jnp.maximum(my_col - 1, 0), my_col), my_col, greet(barrier))
    along_col(jnp.maximum(my_row - 2, 0), my_row, greet(barrier))
    along_col(my_row + 3, grid_rows, greet(barrier))
    far_below(greet(barrier))

    def clear(ref, unless):

        @pl.when(jnp.logical_not(unless))
        def _():
            ref[...] = jnp.zeros(ref.shape, ref.dtype)

    clear(right_in, has_right)
    clear(corner_above, has_above)
    clear(corner_left, has_left & has_below)
    clear(mine_y, has_above)

    first = jnp.logical_not(has_below)
    last = (my_row == 0) & relayed
    between = jnp.logical_not(first | last)

    def enter():
        sources = my_col + jnp.maximum(my_row - 2, 0)
        sources = sources + jnp.where(has_above, jnp.maximum(my_col - RELAYS, 0), 0)
        sources = sources + (near - 1 - my_row) + jnp.where(has_right & has_below, 1, 0)
        await_signals(barrier, sources)
        along_row(0, jnp.where(has_below, my_col - 1, my_col), greet(row_in))
        along_col(0, my_row - 2, greet(col_in))
        direct_tops(greet(far_in))

    corner = cells.at[pl.ds(tile_rows - 8, 8), pl.ds(tile_cols - LANES, LANES)]
    links = (
        (left_out, right_in, 0, -1, has_left, has_right),
        (corner, corner_above, 1, 0, has_below, has_above),
        (corner, corner_left, 0, 1, has_right & has_below, has_left & has_below),
    )

    def link_copy(k):
        source, target, d_row, d_col, _, _ = links[k]
        place = (
            lax.rem(my_row + d_row + grid_rows, grid_rows),
            lax.rem(my_col + d_col + grid_cols, grid_cols),
        )
        return pltpu.make_async_remote_copy(
            src_ref=source, dst_ref=target, send_sem=link_send.at[k], recv_sem=link_recv.at[k],
            device_id=place, device_id_type=MESH,
        )

    def push(k):

        @pl.when(links[k][4])
        def _():
            link_copy(k).start()

    def arrived(k):

        @pl.when(links[k][5])
        def _():
            link_copy(k).wait_recv()

    def send(source, target, send_sem, recv_sem, place):
        return pltpu.make_async_remote_copy(
            src_ref=source, dst_ref=target, send_sem=send_sem, recv_sem=recv_sem,
            device_id=place, device_id_type=MESH,
        )

    def top_copy(r, c):
        line = tops.at[my_row]
        return send(line, line, top_send.at[r], top_recv, (r, c))

    def bottom_copy(r, c):
        return send(bottom_out, bottoms.at[my_row], bottom_send.at[r], bottom_recv, (r, c))

    def row_copy(r, c):
        return send(mine_h, row_h.at[my_col], h_send.at[r * grid_cols + c], row_recv, (r, c))

    def far_copy(r, c):
        return send(mine_h, top_h.at[my_col], h_send.at[r * grid_cols + c], far_recv, (r, c))

    def relay_in(r, c):
        return send(mine_h, col_h, c_send.at[r], link_recv.at[3], (r, c))

    def relay_out(r, c):
        return send(col_h, top_h.at[my_col], t_send.at[c], far_recv, (r, c))

    def left_copy(r, c):
        return send(mine_y, left_d, d_send.at[c], link_recv.at[4], (r, c))

    def push_tops(low, high, act):
        along_col(jnp.where(has_above, low, grid_rows), high, act)

    def push_bottoms():
        along_col(my_row + 1, near, lambda r, c: bottom_copy(r, c).start())

    def down_weights():
        outer_row = bottom_out[0:right, :]
        bottom_out[right : 2 * right, :] = weights(
            inner_row[...], outer_row,
            corner_left[6:7, LANES - 1 : LANES], corner_left[7:8, LANES - 1 : LANES],
            my_col == 0,
        )

    def push_down():
        push(1)
        push(2)
        push_tops(my_row + 1, near, lambda r, c: top_copy(r, c).start())

        @pl.when(has_below & jnp.logical_not(has_left))
        def _():
            push_bottoms()

    def row_line(row):
        return jnp.concatenate(
            [cells[row : row + 1, k * LANES : (k + 1) * LANES] for k in range(right)], axis=0
        )

    def col_lines(block, low, high):
        turned = [
            cells[k * LANES : (k + 1) * LANES, block * LANES : (block + 1) * LANES].T
            for k in range(down)
        ]
        return [jnp.concatenate([t[j : j + 1, :] for t in turned], axis=0) for j in range(low, high)]

    with jax.named_scope("enter_0"):
        pl.when(first)(enter)
    with jax.named_scope("load_head"):
        loads[0].wait()
    with jax.named_scope("head"):
        head_line = col_lines(0, 0, 1)[0]
        left_out[0:down, :] = head_line
        left_out[down:, :] = line_counts(head_line)
    with jax.named_scope("enter_1"):
        pl.when(between)(enter)

        @pl.when(jnp.logical_not(last))
        def _():
            push(0)

    with jax.named_scope("load_edges"):
        loads[1].wait()
        loads[2].wait()
        loads[-1].wait()
        loads[-2].wait()
    with jax.named_scope("last_row"):
        outer_row = row_line(tile_rows - 1)
        down_count = left_out[2 * down - 1 :, LANES - 1 :] - steps_down[0].astype(jnp.float32)
        bottom_out[0:right, :] = outer_row
        bottom_out[2 * right :, :] = down_count + line_counts(outer_row)
        inner_row[...] = row_line(tile_rows - 2)
        tops[my_row] = row_line(0)

        @pl.when(jnp.logical_not(has_left))
        def _():
            down_weights()

        @pl.when(jnp.logical_not(last))
        def _():
            push_down()

    lane = iota((STRIP, LANES), 1)

    def strip(k, carry):
        rows = pl.ds(pl.multiple_of(k * STRIP, STRIP), STRIP)
        wrapped_around = cells[rows, 0:LANES]
        sums = jnp.zeros((STRIP, LANES), jnp.float32)
        for j in range(right):
            cols = slice(j * LANES, (j + 1) * LANES)
            here = cells[rows, cols]
            rolled = pltpu.roll(here, 1, 1)
            across = cycles(here - jnp.where(lane == 0, wrapped_around, rolled))
            wrapped_around = rolled
            floors[rows, cols] = across.astype(jnp.bfloat16)
            sums = sums + across
        row_sums[rows, :] = sums.astype(jnp.bfloat16)
        return carry

    per_chunk = rows_step // STRIP
    for q in range(chunks):
        with jax.named_scope(f"load_{q}"):
            loads[q + 3].wait()
        with jax.named_scope(f"floors_{q}"):
            lax.fori_loop(
                q * per_chunk, (q + 1) * per_chunk, strip, 0, unroll=math.gcd(per_chunk, 8)
            )
        if q == (chunks - 1) // 2:
            with jax.named_scope("enter_2"):

                @pl.when(last)
                def _():
                    enter()
                    push(0)
                    push_down()

    with jax.named_scope("corner_left"):

        @pl.when(has_left & has_below)
        def _():
            arrived(2)
            down_weights()
            push_bottoms()

    with jax.named_scope("ends"):
        ones = jnp.ones((16, LANES), jnp.bfloat16)
        pieces = []
        for k in range(down):
            sums = lax.dot_general(
                ones, row_sums[k * LANES : (k + 1) * LANES, :], (((1,), (1,)), ((), ())),
                preferred_element_type=jnp.float32,
            )
            pieces.append(sums[0:1, :])
        end_count = left_out[down:, :] + jnp.concatenate(pieces, axis=0)
        inner_col, outer_col = col_lines(right - 1, LANES - 2, LANES)

    with jax.named_scope("halo_0"):
        arrived(0)
    with jax.named_scope("halo_1"):
        arrived(1)
    with jax.named_scope("base_h"):
        weight = weights(
            inner_col, outer_col,
            corner_above[7:8, LANES - 2 : LANES - 1], corner_above[7:8, LANES - 1 : LANES],
            my_row == 0,
        )
        across_base = mismatch(
            weight, outer_col, end_count, right_in[0:down, :], right_in[down:, :]
        ) + steps_across[0].astype(jnp.float32)
        mine_h[...] = jnp.broadcast_to(across_base, mine_h.shape)

    to_relay = jnp.where((my_row == 0) & relayed & has_right, 1, grid_rows)
    from_relay = jnp.where(has_above & relayed, my_col + 1, grid_cols)
    to_right = jnp.where(has_above & jnp.logical_not(has_left), 1, grid_cols)

    with jax.named_scope("col_in"):
        await_signals(col_in, grid_rows - near)
        along_col(near, grid_rows, lambda r, c: bottom_copy(r, c).start())
        push_tops(near, grid_rows, lambda r, c: top_copy(r, c).start())
        along_col(to_relay, grid_rows, lambda r, c: relay_in(r, c).start())

    def tell():
        with jax.named_scope("row_in"):
            known = jnp.where(has_below, my_col + 1, my_col)
            await_signals(row_in, grid_cols - 1 - known)
            along_row(my_col + 1, grid_cols, lambda r, c: row_copy(r, c).start())
        with jax.named_scope("far_in"):
            right_count = grid_cols - 1 - my_col
            await_signals(far_in, jnp.where(direct_top, (grid_rows - 1) * right_count, 0))
            far_below(lambda r, c: far_copy(r, c).start())

    def hear(slots, semaphore, first, count):
        for n in range(1, slots.shape[0]):

            @pl.when(count == n)
            def _():
                landed = slots.at[pl.ds(first, n)]
                pltpu.make_async_copy(landed, landed, semaphore).wait()

    def hear_one(ref, semaphore):
        pltpu.make_async_copy(ref, ref, semaphore).wait()

    def pass_on():
        with jax.named_scope("relay"):

            @pl.when(has_above & relayed & has_right)
            def _():
                hear_one(col_h, link_recv.at[3])
                along_row(from_relay, grid_cols, lambda r, c: relay_out(r, c).start())

        with jax.named_scope("hear_y"):
            hear(bottoms, bottom_recv, 0, my_row)
            hear(tops, top_recv, 1, my_row - 1)
        with jax.named_scope("base_y"):

            @pl.when(has_above)
            def _():
                down_here = jnp.zeros((1, 1), jnp.float32)
                for k in range(grid_rows - 1):
                    first_row = tops[k + 1]
                    value = mismatch(
                        bottoms[k, right : 2 * right, :], bottoms[k, 0:right, :],
                        bottoms[k, 2 * right :, :], first_row, line_counts(first_row),
                    )
                    down_here = down_here + jnp.where(k < my_row, value, 0.0)
                mine_y[...] = jnp.broadcast_to(down_here, mine_y.shape)
                along_row(to_right, grid_cols, lambda r, c: left_copy(r, c).start())

    def integrate():
        with jax.named_scope("integrate"):
            upper, lower = triangle(cols_step, 0), triangle(rows_step, 1)
            down_carry = jnp.zeros((1, LANES), jnp.float32)
            for q in range(chunks):
                top = q * rows_step
                rows = pl.ds(top, rows_step)
                head = cells[rows, 0:LANES]
                above = cells[max(top - 1, 0) : max(top, 1), 0:LANES]
                before = jnp.where(iota(head.shape, 0) == 0, above, pltpu.roll(head, 1, 0))
                counts = down_carry + jnp.dot(
                    lower, cycles(head - before).astype(jnp.bfloat16),
                    preferred_element_type=jnp.float32,
                )
                down_carry = counts[rows_step - 1 : rows_step, :]
                carry = counts[:, 0:1]
                for b in range(tile_cols // cols_step):
                    cols = slice(b * cols_step, (b + 1) * cols_step)
                    count = carry + jnp.dot(
                        floors[rows, cols], upper, preferred_element_type=jnp.float32
                    )
                    carry = count[:, cols_step - 1 : cols_step]
                    integ[rows, cols] = cells[rows, cols] * (1.0 / TWO_PI) - count

    tell_at = jnp.where(last, 1, 0)
    pass_at = jnp.where(has_above & relayed, 1, 2)
    integrate_at = jnp.where(last, 0, jnp.where(has_above & relayed, 2, 1))

    def phase(k, carry):
        pl.when(k == tell_at)(tell)
        pl.when(k == pass_at)(pass_on)
        pl.when(k == integrate_at)(integrate)
        return carry

    lax.fori_loop(0, 3, phase, 0)

    with jax.named_scope("sent"):
        for k in range(3):

            @pl.when(links[k][4])
            def _():
                link_copy(k).wait_send()

        push_tops(my_row + 1, grid_rows, lambda r, c: top_copy(r, c).wait_send())
        along_col(my_row + 1, grid_rows, lambda r, c: bottom_copy(r, c).wait_send())
        along_col(to_relay, grid_rows, lambda r, c: relay_in(r, c).wait_send())
        along_row(my_col + 1, grid_cols, lambda r, c: row_copy(r, c).wait_send())
        far_below(lambda r, c: far_copy(r, c).wait_send())
        along_row(from_relay, grid_cols, lambda r, c: relay_out(r, c).wait_send())
        along_row(to_right, grid_cols, lambda r, c: left_copy(r, c).wait_send())

    with jax.named_scope("hear"):
        hear(row_h, row_recv, 0, my_col)
        hear(top_h, far_recv, 0, jnp.where(has_above, my_col, 0))

        @pl.when(has_above & has_left)
        def _():
            hear_one(left_d, link_recv.at[4])

    with jax.named_scope("finish"):

        def prefix(slots):
            line = slots[0]
            for k in range(1, grid_cols):
                line = line + slots[k]
            return line

        across_here = prefix(row_h)
        across_top = jnp.where(has_above, prefix(top_h), across_here)
        down_here = mine_y[...]
        down_left = jnp.where(has_left & has_above, left_d[...], down_here)
        here = left = top = origin = zero_line
        for sweep in range(ITERS):
            prefix_across = across_here + (left - here)
            prefix_across_top = across_top + (origin - top)
            prefix_down = down_here + (top - here)
            prefix_down_left = down_left + (origin - left)
            here = here + 0.5 * (prefix_across + prefix_across_top + prefix_down + prefix_down_left)
            left = left + prefix_down_left
            top = top + prefix_across_top
        offset[...] = jnp.broadcast_to(here, offset.shape)


def place_kernel(integ, offset, out, ready, sems):
    parts = sems.shape[0]
    step = integ.shape[0] // parts
    shift = offset[0:1, 0:1]
    copies = []
    for q in range(parts):
        rows = pl.ds(q * step, step)
        ready[rows, :] = integ[rows, :] + shift
        copy = pltpu.make_async_copy(ready.at[rows], out.at[rows], sems.at[q])
        copy.start()
        copies.append(copy)
    for copy in copies:
        copy.wait()


def on_device(names, sizes, wrapped, col_steps, row_steps):
    frames, tile_rows, tile_cols = wrapped.shape
    grid_rows, grid_cols = sizes
    down, right = tile_rows // LANES, tile_cols // LANES
    dma = pltpu.SemaphoreType.DMA
    rows_step = math.gcd(tile_rows, 256)
    cols_step = math.gcd(tile_cols, 256)
    f32 = jnp.float32

    def with_local_semaphores(*refs):
        pl.run_scoped(
            functools.partial(edge_kernel, names, sizes, rows_step, cols_step, *refs),
            dma((tile_rows // rows_step + 5,)), dma((3,)), dma((grid_rows,)), dma((grid_rows,)),
            dma((grid_rows * grid_cols,)), dma((grid_rows,)), dma((grid_cols,)), dma((grid_cols,)),
        )

    call = pl.pallas_call(
        with_local_semaphores,
        out_shape=(
            pltpu.VMEM((tile_rows, tile_cols), f32),
            pltpu.VMEM((8, LANES), f32),
        ),
        in_specs=[
            pl.BlockSpec(memory_space=pltpu.HBM),
            pl.BlockSpec(memory_space=pltpu.HBM),
            pl.BlockSpec(memory_space=pltpu.HBM),
        ],
        out_specs=(
            pl.BlockSpec(memory_space=pltpu.VMEM),
            pl.BlockSpec(memory_space=pltpu.VMEM),
        ),
        scratch_shapes=[
            pltpu.VMEM((tile_rows, tile_cols), f32),
            pltpu.VMEM((2 * down, LANES), f32),
            pltpu.VMEM((2 * down, LANES), f32),
            pltpu.VMEM((8, LANES), f32),
            pltpu.VMEM((8, LANES), f32),
            pltpu.VMEM((grid_rows, right, LANES), f32),
            pltpu.VMEM((3 * right, LANES), f32),
            pltpu.VMEM((grid_rows, 3 * right, LANES), f32),
            pltpu.VMEM((right, LANES), f32),
            pltpu.VMEM((tile_rows, tile_cols), jnp.bfloat16),
            pltpu.VMEM((tile_rows, LANES), jnp.bfloat16),
            pltpu.VMEM((1, 1, 1), jnp.int32),
            pltpu.VMEM((1, 1, 1), jnp.int32),
            pltpu.VMEM((1, LANES), f32),
            pltpu.VMEM((1, LANES), f32),
            pltpu.VMEM((grid_cols, 1, LANES), f32),
            pltpu.VMEM((grid_cols, 1, LANES), f32),
            pltpu.VMEM((1, LANES), f32),
            pltpu.VMEM((1, LANES), f32),
            dma((5,)), dma, dma, dma, dma,
            pltpu.SemaphoreType.REGULAR,
            pltpu.SemaphoreType.REGULAR,
            pltpu.SemaphoreType.REGULAR,
        ],
        compiler_params=pltpu.CompilerParams(
            collective_id=0, has_side_effects=True, vmem_limit_bytes=57 * 1024 * 1024
        ),
    )
    parts = math.gcd(tile_rows // 8, 16)
    place = pl.pallas_call(
        place_kernel,
        out_shape=jax.ShapeDtypeStruct((tile_rows, tile_cols), f32),
        in_specs=[pl.BlockSpec(memory_space=pltpu.VMEM), pl.BlockSpec(memory_space=pltpu.VMEM)],
        out_specs=pl.BlockSpec(memory_space=pltpu.HBM),
        scratch_shapes=[
            pltpu.VMEM((tile_rows, tile_cols), f32),
            pltpu.SemaphoreType.DMA((parts,)),
        ],
        compiler_params=pltpu.CompilerParams(vmem_limit_bytes=24 * 1024 * 1024),
    )
    outs = [
        place(*call(wrapped[f : f + 1], col_steps[f : f + 1], row_steps[f : f + 1]))
        for f in range(frames)
    ]
    return jnp.stack(outs)


def solution(mesh):
    spec = P(None, "row", "col")
    sizes = (mesh.shape["row"], mesh.shape["col"])
    return jax.shard_map(
        functools.partial(on_device, ("row", "col"), sizes),
        mesh=mesh, in_specs=(spec, spec, spec), out_specs=spec, check_vma=False,
    )
```

```python
import functools
import math

import jax
import jax.numpy as jnp
from jax import lax
from jax.experimental import pallas as pl
from jax.experimental.pallas import tpu as pltpu
from jax.sharding import PartitionSpec as P

ITERS = 2
TWO_PI = 2.0 * math.pi
MESH = pl.DeviceIdType.MESH
LANES = 128
STRIP = 16


def cycles(change):
    return jnp.floor(change * (1.0 / TWO_PI) + 0.5)


def iota(shape, dim):
    return lax.broadcasted_iota(jnp.int32, shape, dim)


def total(values):
    return jnp.sum(values, axis=1, keepdims=True)


def previous(line, first):
    lane, row = iota(line.shape, 1), iota(line.shape, 0)
    along = pltpu.roll(line, 1, 1)
    across = pltpu.roll(along, 1, 0) if line.shape[0] > 1 else along
    return jnp.where(lane > 0, along, jnp.where(row > 0, across, first))


def summed(line):
    return total(jnp.sum(line, axis=0, keepdims=True))


def triangle(size, dim):
    ordered = iota((size, size), dim) <= iota((size, size), 1 - dim)
    return ordered.astype(jnp.float32).astype(jnp.bfloat16)


def line_counts(line):
    groups = line.shape[0]
    row = iota(line.shape, 0)
    floors = cycles(line - previous(line, line[0:1, 0:1]))
    whole, shift = floors, 1
    while shift < groups:
        whole = whole + jnp.where(row >= shift, pltpu.roll(whole, shift, 0), 0.0)
        shift *= 2
    pair = jnp.concatenate([floors, whole - floors], axis=1)
    pair = jnp.concatenate([pair] * (-(-16 // groups)), axis=0).astype(jnp.bfloat16)
    ones = jnp.ones((LANES, LANES), jnp.bfloat16)
    table = jnp.concatenate([triangle(LANES, 0), ones], axis=0)
    return jnp.dot(pair, table, preferred_element_type=jnp.float32)[0:groups, :]


def weights(inner, outer, inner_before, outer_before, at_image_edge):
    over = cycles(outer - inner)
    over_before = previous(over, cycles(outer_before - inner_before))
    along_outer = cycles(outer - previous(outer, outer_before))
    along_inner = cycles(inner - previous(inner, inner_before))
    charge = over_before + along_outer - over - along_inner
    start = (iota(charge.shape, 1) == 0) & (iota(charge.shape, 0) == 0)
    charge = jnp.where(start & at_image_edge, 0.0, charge)
    return 1.0 / (1.0 + jnp.abs(charge))


def mismatch(weight, outer, count, first, beyond):
    jump = beyond - count - cycles(first - outer)
    return summed(weight * jump) / summed(weight)


def edge_kernel(
    names, sizes, rows_step, cols_step,
    wrapped, col_steps, row_steps,
    integ, offset,
    cells, left_out, right_in, corner_above, corner_left, tops, bottom_out, bottoms, inner_row,
    floors, row_sums, steps_across, steps_down, mine_h, mine_y, row_h, top_h, col_h, left_d, carried, ends,
    link_recv, top_recv, bottom_recv, row_recv, far_recv, row_in, col_in, far_in,
    load_sem, link_send, top_send, bottom_send, h_send, c_send, t_send, d_send,
):
    row_name, col_name = names
    grid_rows, grid_cols = sizes
    tile_rows, tile_cols = cells.shape
    my_row, my_col = lax.axis_index(row_name), lax.axis_index(col_name)
    down, right = tile_rows // LANES, tile_cols // LANES

    chunks = tile_rows // rows_step
    rest = pl.ds(LANES, tile_cols - LANES)
    regions = [
        (pl.ds(0, tile_rows), pl.ds(0, LANES)),
        (pl.ds(tile_rows - 16, 16), rest),
        (pl.ds(0, 16), rest),
    ]
    for q in range(chunks):
        top = max(q * rows_step, 16)
        bottom = min((q + 1) * rows_step, tile_rows - 16)
        regions.append((pl.ds(top, bottom - top), rest))
    loads = []
    for k, (rows, cols) in enumerate(regions):
        loads.append(
            pltpu.make_async_copy(wrapped.at[0, rows, cols], cells.at[rows, cols], load_sem.at[k])
        )
        loads[-1].start()
    for source, target in ((col_steps, steps_across), (row_steps, steps_down)):
        loads.append(pltpu.make_async_copy(source, target, load_sem.at[len(loads)]))
        loads[-1].start()

    def span(low, high, act):
        def step(k, carry):
            act(k)
            return carry

        lax.fori_loop(low, high, step, 0)

    def along_row(low, high, act):
        span(low, high, lambda c: act(my_row, c))

    def along_col(low, high, act):
        span(low, high, lambda r: act(r, my_col))

    has_left, has_right = my_col > 0, my_col < grid_cols - 1
    has_above, has_below = my_row > 0, my_row < grid_rows - 1
    even_row = has_above & (lax.rem(my_row, 2) == 0)
    tail_col = my_col >= grid_cols - 2
    tail = (my_row == 0) & tail_col
    unknown_above = jnp.maximum(my_row - 2, jnp.where(tail_col, jnp.minimum(my_row, 1), 0))
    near = jnp.where(tail, my_row + 1, jnp.minimum(my_row + 3, grid_rows))
    direct_top = (my_row == 0) & (my_col > 1)
    first_left = jnp.where(my_row == 0, 1, 0)
    greets_left = has_left & (has_below | (my_col == 1))
    knows_right = has_right & (has_below | (my_col == 0))
    pair = my_col == 1

    def far_below(act):
        low = jnp.where(direct_top, 1, grid_rows)
        span(low, grid_rows, lambda r: span(my_col + 1, grid_cols, lambda c: act(r, c)))

    def direct_tops(act):
        span(2, jnp.where(has_above, my_col, 0), lambda c: act(0, c))

    zero_line = jnp.zeros((1, LANES), jnp.float32)
    for slots in (row_h, top_h):
        for k in range(grid_cols):
            slots[k] = zero_line

    barrier = pltpu.get_barrier_semaphore()

    def await_signals(semaphore, count):

        @pl.when(count > 0)
        def _():
            pl.semaphore_wait(semaphore, count)

    def greet(semaphore):
        return lambda r, c: pl.semaphore_signal(
            semaphore, inc=1, device_id=(r, c), device_id_type=MESH
        )

    origin = (my_row == 0) & (my_col == 0)
    along_row(my_col + 1, jnp.where(origin, jnp.minimum(2, grid_cols), grid_cols), greet(barrier))
    along_row(jnp.where(greets_left, my_col - 1, my_col), my_col, greet(barrier))
    along_col(unknown_above, my_row, greet(barrier))
    along_col(jnp.where(tail, my_row + 1, my_row + 3), grid_rows, greet(barrier))
    far_below(greet(barrier))

    def clear(ref, unless):

        @pl.when(jnp.logical_not(unless))
        def _():
            ref[...] = jnp.zeros(ref.shape, ref.dtype)

    clear(right_in, has_right)
    clear(corner_above, has_above)
    clear(corner_left, has_left & has_below)
    clear(mine_y, has_above)

    first = jnp.logical_not(has_below) | tail
    last = (my_row == 0) & (my_col < 2) & jnp.logical_not(first)
    between = jnp.logical_not(first | last)

    def enter():
        sources = jnp.where(my_row == 0, jnp.where(pair, 1, jnp.maximum(my_col - 1, 0)), my_col)
        sources = sources + unknown_above
        sources = sources + jnp.where(has_above, jnp.maximum(my_col - 2, 0), 0)
        sources = sources + (near - 1 - my_row) + jnp.where(knows_right, 1, 0)
        await_signals(barrier, sources)

        @pl.when(jnp.logical_not(first | last))
        def _():
            push(0)

        along_row(first_left, jnp.where(greets_left, my_col - 1, my_col), greet(row_in))
        along_col(0, unknown_above, greet(col_in))
        direct_tops(greet(far_in))

    corner = cells.at[pl.ds(tile_rows - 8, 8), pl.ds(tile_cols - LANES, LANES)]
    links = (
        (left_out, right_in, 0, -1, has_left, has_right),
        (corner, corner_above, 1, 0, has_below, has_above),
        (corner, corner_left, 0, 1, has_right & has_below, has_left & has_below),
    )

    def link_copy(k):
        source, target, d_row, d_col, _, _ = links[k]
        place = (
            lax.rem(my_row + d_row + grid_rows, grid_rows),
            lax.rem(my_col + d_col + grid_cols, grid_cols),
        )
        return pltpu.make_async_remote_copy(
            src_ref=source, dst_ref=target, send_sem=link_send.at[k], recv_sem=link_recv.at[k],
            device_id=place, device_id_type=MESH,
        )

    def push(k):

        @pl.when(links[k][4])
        def _():
            link_copy(k).start()

    def arrived(k):

        @pl.when(links[k][5])
        def _():
            link_copy(k).wait_recv()

    def send(source, target, send_sem, recv_sem, place):
        return pltpu.make_async_remote_copy(
            src_ref=source, dst_ref=target, send_sem=send_sem, recv_sem=recv_sem,
            device_id=place, device_id_type=MESH,
        )

    def top_copy(r, c):
        line = tops.at[my_row]
        return send(line, line, top_send.at[r], top_recv, (r, c))

    def bottom_copy(r, c):
        return send(bottom_out, bottoms.at[my_row], bottom_send.at[r], bottom_recv, (r, c))

    def row_copy(r, c):
        return send(mine_h.at[1], row_h.at[my_col], h_send.at[r * grid_cols + c], row_recv, (r, c))

    def far_copy(r, c):
        return send(mine_h.at[1], top_h.at[my_col], h_send.at[r * grid_cols + c], far_recv, (r, c))

    def origin_copy(r, c):
        return send(mine_h.at[1], row_h.at[0], h_send.at[r * grid_cols + c], link_recv.at[5], (r, c))

    def relay_in(r, c):
        return send(mine_h, col_h, c_send.at[r], link_recv.at[3], (r, c))

    def relay_out(r, c):
        return send(col_h.at[1], top_h.at[my_col], t_send.at[c], far_recv, (r, c))

    def left_copy(r, c):
        return send(mine_y, left_d, d_send.at[c], link_recv.at[4], (r, c))

    def push_tops(low, high, act):
        along_col(jnp.where(has_above, low, grid_rows), high, act)

    def push_bottoms():
        along_col(my_row + 1, near, lambda r, c: bottom_copy(r, c).start())

    def down_weights():
        outer_row = bottom_out[0:right, :]
        bottom_out[right : 2 * right, :] = weights(
            inner_row[...], outer_row,
            corner_left[6:7, LANES - 1 : LANES], corner_left[7:8, LANES - 1 : LANES],
            my_col == 0,
        )

    def push_down():
        pl.when(jnp.logical_not(tail))(lambda: push(1))
        push(2)
        push_tops(my_row + 1, near, lambda r, c: top_copy(r, c).start())

        @pl.when(has_below & jnp.logical_not(has_left))
        def _():
            push_bottoms()

    def row_line(row):
        return jnp.concatenate(
            [cells[row : row + 1, k * LANES : (k + 1) * LANES] for k in range(right)], axis=0
        )

    def col_lines(block, low, high):
        turned = [
            cells[k * LANES : (k + 1) * LANES, block * LANES : (block + 1) * LANES].T
            for k in range(down)
        ]
        return [jnp.concatenate([t[j : j + 1, :] for t in turned], axis=0) for j in range(low, high)]

    with jax.named_scope("enter_0"):
        pl.when(first)(enter)
    with jax.named_scope("load_head"):
        loads[0].wait()
    with jax.named_scope("head"):
        head_line = col_lines(0, 0, 1)[0]
        left_out[0:down, :] = head_line
        left_out[down:, :] = line_counts(head_line)
    with jax.named_scope("push_first"):
        pl.when(first)(lambda: push(0))

    with jax.named_scope("load_edges"):
        loads[1].wait()
        loads[2].wait()
        loads[-1].wait()
        loads[-2].wait()
    with jax.named_scope("last_row"):
        outer_row = row_line(tile_rows - 1)
        down_count = left_out[2 * down - 1 :, LANES - 1 :] - steps_down[0].astype(jnp.float32)
        bottom_out[0:right, :] = outer_row
        bottom_out[2 * right :, :] = down_count + line_counts(outer_row)
        inner_row[...] = row_line(tile_rows - 2)
        tops[my_row] = row_line(0)

        @pl.when(jnp.logical_not(has_left))
        def _():
            down_weights()

    with jax.named_scope("enter_1"):
        pl.when(between)(enter)

        @pl.when(jnp.logical_not(last))
        def _():
            push_down()

    lane = iota((STRIP, LANES), 1)

    def strip(k, carry):
        rows = pl.ds(pl.multiple_of(k * STRIP, STRIP), STRIP)
        wrapped_around = cells[rows, 0:LANES]
        sums = jnp.zeros((STRIP, LANES), jnp.float32)
        for j in range(right):
            cols = slice(j * LANES, (j + 1) * LANES)
            here = cells[rows, cols]
            rolled = pltpu.roll(here, 1, 1)
            across = cycles(here - jnp.where(lane == 0, wrapped_around, rolled))
            wrapped_around = rolled
            floors[rows, cols] = across.astype(jnp.bfloat16)
            sums = sums + across
        row_sums[rows, :] = sums.astype(jnp.bfloat16)
        return carry

    def weigh_bottom():
        arrived(2)
        down_weights()
        push_bottoms()

    def push_further_tops():
        await_signals(col_in, grid_rows - near)
        pl.when(tail)(lambda: push(1))
        push_tops(near, grid_rows, lambda r, c: top_copy(r, c).start())

    per_chunk = rows_step // STRIP
    for q in range(chunks):
        if q == chunks - 1:
            with jax.named_scope("tail_in"):
                pl.when(tail)(push_further_tops)
                pl.when(has_left & has_below & jnp.logical_not(last))(weigh_bottom)
        with jax.named_scope(f"load_{q}"):
            loads[q + 3].wait()
        with jax.named_scope(f"floors_{q}"):
            lax.fori_loop(
                q * per_chunk, (q + 1) * per_chunk, strip, 0, unroll=math.gcd(per_chunk, 8)
            )
        if q == (chunks - 1) // 2:
            with jax.named_scope("enter_2"):

                @pl.when(last)
                def _():
                    enter()
                    push(0)
                    push_down()

    with jax.named_scope("corner_left"):
        pl.when(has_left & has_below & last)(weigh_bottom)

    with jax.named_scope("col_in"):
        pl.when(jnp.logical_not(tail))(push_further_tops)
        along_col(near, grid_rows, lambda r, c: bottom_copy(r, c).start())

    to_relay = jnp.where((my_row == 0) & pair, 1, grid_rows)
    from_relay = jnp.where(has_above & pair, my_col + 1, grid_cols)
    to_right = jnp.where(has_above & jnp.logical_not(has_left), 1, grid_cols)
    to_row = jnp.where(origin, grid_cols, my_col + 1)
    paired = (my_row == 0) & pair

    def hear_one(ref, semaphore):
        pltpu.make_async_copy(ref, ref, semaphore).wait()

    def across():
        with jax.named_scope("ends"):
            ones = jnp.ones((16, LANES), jnp.bfloat16)
            pieces = []
            for k in range(down):
                sums = lax.dot_general(
                    ones, row_sums[k * LANES : (k + 1) * LANES, :], (((1,), (1,)), ((), ())),
                    preferred_element_type=jnp.float32,
                )
                pieces.append(sums[0:1, :])
            end_count = left_out[down:, :] + jnp.concatenate(pieces, axis=0)
            end_count = end_count - steps_across[0].astype(jnp.float32)
            inner_col, outer_col = col_lines(right - 1, LANES - 2, LANES)
        with jax.named_scope("halo_1"):
            arrived(1)
        with jax.named_scope("weights_h"):
            weight = weights(
                inner_col, outer_col,
                corner_above[7:8, LANES - 2 : LANES - 1], corner_above[7:8, LANES - 1 : LANES],
                my_row == 0,
            )
            ends[0:down, :] = weight * (1.0 / summed(weight))
            ends[down : 2 * down, :] = outer_col
            ends[2 * down :, :] = end_count

    def across_mean():
        with jax.named_scope("halo_0"):
            arrived(0)
        with jax.named_scope("base_h"):
            jump = right_in[down:, :] - ends[2 * down :, :]
            jump = jump - cycles(right_in[0:down, :] - ends[down : 2 * down, :])
            mine_h[1] = jnp.broadcast_to(summed(ends[0:down, :] * jump), (1, LANES))

            @pl.when(paired)
            def _():
                hear_one(row_h.at[0], link_recv.at[5])
                mine_h[0] = row_h[0]
                mine_h[1] = mine_h[1] + row_h[0]

            @pl.when(origin & has_right)
            def _():
                origin_copy(my_row, 1).start()

            along_col(to_relay, grid_rows, lambda r, c: relay_in(r, c).start())

    sums_first = even_row & jnp.logical_not(has_left)

    def await_row():
        known = jnp.where(knows_right, my_col + 1, my_col)
        await_signals(row_in, jnp.where(origin, 0, grid_cols - 1 - known))

    def tell_left():
        along_row(to_right, grid_cols, lambda r, c: left_copy(r, c).start())

    def tell():
        with jax.named_scope("row_in"):
            pl.when(jnp.logical_not(sums_first))(await_row)
            along_row(to_row, grid_cols, lambda r, c: row_copy(r, c).start())
            pl.when(jnp.logical_not(even_row))(tell_left)

    def tell_far():
        with jax.named_scope("far_in"):
            right_count = grid_cols - 1 - my_col
            await_signals(far_in, jnp.where(direct_top, (grid_rows - 1) * right_count, 0))
            far_below(lambda r, c: far_copy(r, c).start())

    def hear(slots, semaphore, first, count):
        for n in range(1, slots.shape[0]):

            @pl.when(count == n)
            def _():
                landed = slots.at[pl.ds(first, n)]
                pltpu.make_async_copy(landed, landed, semaphore).wait()

    def relay():
        with jax.named_scope("relay"):

            @pl.when(has_above & pair)
            def _():
                hear_one(col_h, link_recv.at[3])
                along_row(from_relay, grid_cols, lambda r, c: relay_out(r, c).start())

    def down_sum():
        with jax.named_scope("hear_y"):
            hear(bottoms, bottom_recv, 0, my_row)
            hear(tops, top_recv, 1, my_row - 1)
        with jax.named_scope("base_y"):

            @pl.when(has_above)
            def _():
                down_here = jnp.zeros((1, 1), jnp.float32)
                for k in range(grid_rows - 1):
                    first_row = tops[k + 1]
                    value = mismatch(
                        bottoms[k, right : 2 * right, :], bottoms[k, 0:right, :],
                        bottoms[k, 2 * right :, :], first_row, line_counts(first_row),
                    )
                    down_here = down_here + jnp.where(k < my_row, value, 0.0)
                mine_y[...] = jnp.broadcast_to(down_here, mine_y.shape)

                @pl.when(sums_first)
                def _():
                    await_row()
                    tell_left()


    def integrate(low, high):
        with jax.named_scope(f"integrate_{low}"):
            upper, lower = triangle(cols_step, 0), triangle(rows_step, 1)
            down_carry = jnp.zeros((1, LANES), jnp.float32) if low == 0 else carried[...]
            for q in range(low, high):
                top = q * rows_step
                rows = pl.ds(top, rows_step)
                head = cells[rows, 0:LANES]
                above = cells[max(top - 1, 0) : max(top, 1), 0:LANES]
                before = jnp.where(iota(head.shape, 0) == 0, above, pltpu.roll(head, 1, 0))
                counts = down_carry + jnp.dot(
                    lower, cycles(head - before).astype(jnp.bfloat16),
                    preferred_element_type=jnp.float32,
                )
                down_carry = counts[rows_step - 1 : rows_step, :]
                carry = counts[:, 0:1]
                for b in range(tile_cols // cols_step):
                    cols = slice(b * cols_step, (b + 1) * cols_step)
                    count = carry + jnp.dot(
                        floors[rows, cols], upper, preferred_element_type=jnp.float32
                    )
                    carry = count[:, cols_step - 1 : cols_step]
                    integ[rows, cols] = cells[rows, cols] * (1.0 / TWO_PI) - count
            if high < chunks:
                carried[...] = down_carry

    left_side = has_above & jnp.logical_not(has_left)
    split = (even_row & has_left) | (tail_col & (my_row == 1))
    half = (chunks + 1) // 2
    left_odd, left_even, paired_at, split_at, otherwise = range(5)
    never = 8
    kind = jnp.where(pair, paired_at, jnp.where(split, split_at, otherwise))
    kind = jnp.where(left_side, jnp.where(even_row, left_even, left_odd), kind)

    def pick(*slots):
        chosen = slots[otherwise]
        for k in range(otherwise):
            chosen = jnp.where(kind == k, slots[k], chosen)
        return chosen

    order = (
        (across, jnp.where(has_right, pick(0, 1, 1, 1, 0), never)),
        (across_mean, jnp.where(has_right, pick(1, 3, 2, 2, 1), never)),
        (tell, pick(3, 4, 3, 3, 2)),
        (functools.partial(integrate, 0, half), pick(4, 0, 0, 0, 3)),
        (tell_far, jnp.where(direct_top, 4, never)),
        (functools.partial(integrate, half, chunks), pick(5, 5, 6, 4, 5)),
        (down_sum, pick(2, 2, jnp.where(even_row, 5, 4), 5, 6)),
        (relay, pick(6, 6, jnp.where(even_row, 4, 5), 6, 6)),
    )

    def phase(k, carry):
        for act, at in order:
            pl.when(k == at)(act)
        return carry

    lax.fori_loop(0, len(order), phase, 0)

    pl.when(jnp.logical_not(has_right))(lambda: arrived(1))

    with jax.named_scope("sent"):
        for k in range(3):

            @pl.when(links[k][4])
            def _():
                link_copy(k).wait_send()

        push_tops(my_row + 1, grid_rows, lambda r, c: top_copy(r, c).wait_send())
        along_col(my_row + 1, grid_rows, lambda r, c: bottom_copy(r, c).wait_send())
        along_col(to_relay, grid_rows, lambda r, c: relay_in(r, c).wait_send())
        along_row(to_row, grid_cols, lambda r, c: row_copy(r, c).wait_send())

        @pl.when(origin & has_right)
        def _():
            origin_copy(my_row, 1).wait_send()

        far_below(lambda r, c: far_copy(r, c).wait_send())
        along_row(from_relay, grid_cols, lambda r, c: relay_out(r, c).wait_send())
        along_row(to_right, grid_cols, lambda r, c: left_copy(r, c).wait_send())

    with jax.named_scope("hear"):
        hear(row_h, row_recv, 1, jnp.where(has_above, 0, my_col - 1))
        hear(row_h, row_recv, 0, jnp.where(has_above, my_col, 0))
        hear(top_h, far_recv, 1, jnp.where(has_above, my_col - 1, 0))

        @pl.when(has_above & has_left)
        def _():
            hear_one(left_d, link_recv.at[4])

    with jax.named_scope("finish"):

        def prefix(slots):
            line = slots[0]
            for k in range(1, grid_cols):
                line = line + slots[k]
            return line

        across_here = prefix(row_h)
        across_top = jnp.where(pair, col_h[0], prefix(top_h))
        across_top = jnp.where(has_above, across_top, across_here)
        down_here = mine_y[...]
        down_left = jnp.where(has_left & has_above, left_d[...], down_here)
        here = left = top = start = zero_line
        for sweep in range(ITERS):
            prefix_across = across_here + (left - here)
            prefix_across_top = across_top + (start - top)
            prefix_down = down_here + (top - here)
            prefix_down_left = down_left + (start - left)
            here = here + 0.5 * (prefix_across + prefix_across_top + prefix_down + prefix_down_left)
            left = left + prefix_down_left
            top = top + prefix_across_top
        offset[...] = jnp.broadcast_to(here, offset.shape)


def place_kernel(integ, offset, out, ready, sems):
    parts = sems.shape[0]
    step = integ.shape[0] // parts
    shift = offset[0:1, 0:1]
    copies = []
    for q in range(parts):
        rows = pl.ds(q * step, step)
        ready[rows, :] = integ[rows, :] + shift
        copy = pltpu.make_async_copy(ready.at[rows], out.at[rows], sems.at[q])
        copy.start()
        copies.append(copy)
    for copy in copies:
        copy.wait()


def on_device(names, sizes, wrapped, col_steps, row_steps):
    frames, tile_rows, tile_cols = wrapped.shape
    grid_rows, grid_cols = sizes
    down, right = tile_rows // LANES, tile_cols // LANES
    dma = pltpu.SemaphoreType.DMA
    rows_step = math.gcd(tile_rows, 256)
    cols_step = math.gcd(tile_cols, 256)
    f32 = jnp.float32

    def with_local_semaphores(*refs):
        pl.run_scoped(
            functools.partial(edge_kernel, names, sizes, rows_step, cols_step, *refs),
            dma((tile_rows // rows_step + 5,)), dma((3,)), dma((grid_rows,)), dma((grid_rows,)),
            dma((grid_rows * grid_cols,)), dma((grid_rows,)), dma((grid_cols,)), dma((grid_cols,)),
        )

    call = pl.pallas_call(
        with_local_semaphores,
        out_shape=(
            pltpu.VMEM((tile_rows, tile_cols), f32),
            pltpu.VMEM((8, LANES), f32),
        ),
        in_specs=[
            pl.BlockSpec(memory_space=pltpu.HBM),
            pl.BlockSpec(memory_space=pltpu.HBM),
            pl.BlockSpec(memory_space=pltpu.HBM),
        ],
        out_specs=(
            pl.BlockSpec(memory_space=pltpu.VMEM),
            pl.BlockSpec(memory_space=pltpu.VMEM),
        ),
        scratch_shapes=[
            pltpu.VMEM((tile_rows, tile_cols), f32),
            pltpu.VMEM((2 * down, LANES), f32),
            pltpu.VMEM((2 * down, LANES), f32),
            pltpu.VMEM((8, LANES), f32),
            pltpu.VMEM((8, LANES), f32),
            pltpu.VMEM((grid_rows, right, LANES), f32),
            pltpu.VMEM((3 * right, LANES), f32),
            pltpu.VMEM((grid_rows, 3 * right, LANES), f32),
            pltpu.VMEM((right, LANES), f32),
            pltpu.VMEM((tile_rows, tile_cols), jnp.bfloat16),
            pltpu.VMEM((tile_rows, LANES), jnp.bfloat16),
            pltpu.VMEM((1, 1, 1), jnp.int32),
            pltpu.VMEM((1, 1, 1), jnp.int32),
            pltpu.VMEM((2, 1, LANES), f32),
            pltpu.VMEM((1, LANES), f32),
            pltpu.VMEM((grid_cols, 1, LANES), f32),
            pltpu.VMEM((grid_cols, 1, LANES), f32),
            pltpu.VMEM((2, 1, LANES), f32),
            pltpu.VMEM((1, LANES), f32),
            pltpu.VMEM((1, LANES), f32),
            pltpu.VMEM((3 * down, LANES), f32),
            dma((6,)), dma, dma, dma, dma,
            pltpu.SemaphoreType.REGULAR,
            pltpu.SemaphoreType.REGULAR,
            pltpu.SemaphoreType.REGULAR,
        ],
        compiler_params=pltpu.CompilerParams(
            collective_id=0, has_side_effects=True, vmem_limit_bytes=57 * 1024 * 1024
        ),
    )
    parts = math.gcd(tile_rows // 8, 16)
    place = pl.pallas_call(
        place_kernel,
        out_shape=jax.ShapeDtypeStruct((tile_rows, tile_cols), f32),
        in_specs=[pl.BlockSpec(memory_space=pltpu.VMEM), pl.BlockSpec(memory_space=pltpu.VMEM)],
        out_specs=pl.BlockSpec(memory_space=pltpu.HBM),
        scratch_shapes=[
            pltpu.VMEM((tile_rows, tile_cols), f32),
            pltpu.SemaphoreType.DMA((parts,)),
        ],
        compiler_params=pltpu.CompilerParams(vmem_limit_bytes=24 * 1024 * 1024),
    )
    outs = [
        place(*call(wrapped[f : f + 1], col_steps[f : f + 1], row_steps[f : f + 1]))
        for f in range(frames)
    ]
    return jnp.stack(outs)


def solution(mesh):
    spec = P(None, "row", "col")
    sizes = (mesh.shape["row"], mesh.shape["col"])
    return jax.shard_map(
        functools.partial(on_device, ("row", "col"), sizes),
        mesh=mesh, in_specs=(spec, spec, spec), out_specs=spec, check_vma=False,
    )
```

```python
import functools
import math

import jax
import jax.numpy as jnp
from jax import lax
from jax.experimental import pallas as pl
from jax.experimental.pallas import tpu as pltpu
from jax.sharding import PartitionSpec as P

ITERS = 2
TWO_PI = 2.0 * math.pi
MESH = pl.DeviceIdType.MESH
LANES = 128
STRIP = 16


def cycles(change):
    return jnp.floor(change * (1.0 / TWO_PI) + 0.5)


def iota(shape, dim):
    return lax.broadcasted_iota(jnp.int32, shape, dim)


def total(values):
    return jnp.sum(values, axis=1, keepdims=True)


def previous(line, first):
    lane, row = iota(line.shape, 1), iota(line.shape, 0)
    along = pltpu.roll(line, 1, 1)
    across = pltpu.roll(along, 1, 0) if line.shape[0] > 1 else along
    return jnp.where(lane > 0, along, jnp.where(row > 0, across, first))


def summed(line):
    return total(jnp.sum(line, axis=0, keepdims=True))


def triangle(size, dim):
    ordered = iota((size, size), dim) <= iota((size, size), 1 - dim)
    return ordered.astype(jnp.float32).astype(jnp.bfloat16)


def line_counts(line):
    groups = line.shape[0]
    row = iota(line.shape, 0)
    floors = cycles(line - previous(line, line[0:1, 0:1]))
    whole, shift = floors, 1
    while shift < groups:
        whole = whole + jnp.where(row >= shift, pltpu.roll(whole, shift, 0), 0.0)
        shift *= 2
    pair = jnp.concatenate([floors, whole - floors], axis=1)
    pair = jnp.concatenate([pair] * (-(-16 // groups)), axis=0).astype(jnp.bfloat16)
    ones = jnp.ones((LANES, LANES), jnp.bfloat16)
    table = jnp.concatenate([triangle(LANES, 0), ones], axis=0)
    return jnp.dot(pair, table, preferred_element_type=jnp.float32)[0:groups, :]


def weights(inner, outer, inner_before, outer_before, at_image_edge):
    over = cycles(outer - inner)
    over_before = previous(over, cycles(outer_before - inner_before))
    along_outer = cycles(outer - previous(outer, outer_before))
    along_inner = cycles(inner - previous(inner, inner_before))
    charge = over_before + along_outer - over - along_inner
    start = (iota(charge.shape, 1) == 0) & (iota(charge.shape, 0) == 0)
    charge = jnp.where(start & at_image_edge, 0.0, charge)
    return 1.0 / (1.0 + jnp.abs(charge))


def mismatch(weight, outer, count, first, beyond):
    jump = beyond - count - cycles(first - outer)
    return summed(weight * jump) / summed(weight)


def edge_kernel(
    names, sizes, rows_step, cols_step,
    wrapped, col_steps, row_steps,
    integ, offset,
    cells, left_out, right_in, corner_above, corner_left, tops, bottom_out, bottoms, inner_row,
    floors, row_sums, steps_across, steps_down, mine_h, mine_y, row_h, top_h, col_h, left_d, carried, ends, ends_in, pair_in, first_inner, left_sums,
    link_recv, top_recv, bottom_recv, row_recv, far_recv, row_in, col_in, far_in,
    load_sem, link_send, top_send, bottom_send, h_send, c_send, d_send,
):
    row_name, col_name = names
    grid_rows, grid_cols = sizes
    tile_rows, tile_cols = cells.shape
    my_row, my_col = lax.axis_index(row_name), lax.axis_index(col_name)
    down, right = tile_rows // LANES, tile_cols // LANES

    chunks = tile_rows // rows_step
    rest = pl.ds(LANES, tile_cols - LANES)
    regions = [
        (pl.ds(0, tile_rows), pl.ds(0, LANES)),
        (pl.ds(tile_rows - 16, 16), rest),
        (pl.ds(0, 16), rest),
    ]
    for q in range(chunks):
        top = max(q * rows_step, 16)
        bottom = min((q + 1) * rows_step, tile_rows - 16)
        regions.append((pl.ds(top, bottom - top), rest))
    loads = []
    for k, (rows, cols) in enumerate(regions):
        loads.append(
            pltpu.make_async_copy(wrapped.at[0, rows, cols], cells.at[rows, cols], load_sem.at[k])
        )
    for source, target in ((col_steps, steps_across), (row_steps, steps_down)):
        loads.append(pltpu.make_async_copy(source, target, load_sem.at[len(loads)]))

    def start_loads():
        for load in loads:
            load.start()

    def span(low, high, act):
        def step(k, carry):
            act(k)
            return carry

        lax.fori_loop(low, high, step, 0)

    def along_row(low, high, act):
        span(low, high, lambda c: act(my_row, c))

    def along_col(low, high, act):
        span(low, high, lambda r: act(r, my_col))

    has_left, has_right = my_col > 0, my_col < grid_cols - 1
    has_above, has_below = my_row > 0, my_row < grid_rows - 1
    even_row = has_above & (lax.rem(my_row, 2) == 0)
    tail_col = my_col >= grid_cols - 2
    tail = tail_col & has_below & (lax.rem(my_row, 2) == 0)

    def unknown_to(row):
        return (row < my_row) & ((my_row - row > 2) | (tail_col & (lax.rem(row, 2) == 0)))

    unknown_above = sum(jnp.where(unknown_to(k), 1, 0) for k in range(grid_rows))
    near = jnp.where(tail, my_row + 1, jnp.minimum(my_row + 3, grid_rows))
    direct_top = (my_row == 0) & (my_col > 2)
    first_left = jnp.where(my_row == 0, 3, 0)
    lead = (my_row == 0) & (my_col < 3)
    pair = my_col == 1
    paired = (my_row == 0) & pair
    second = (my_row == 0) & (my_col == 3)
    before_second = (my_row == 0) & (my_col == 2)
    greets_left = has_left & (has_below | pair | second | before_second)
    knows_right = has_right & (has_below | (my_col == 0) | paired | before_second)

    def far_below(act):
        low = jnp.where(direct_top, 1, grid_rows)
        span(low, grid_rows, lambda r: span(my_col + 1, grid_cols, lambda c: act(r, c)))

    def left_below(act):
        span(jnp.where(second, 1, grid_rows), grid_rows, lambda r: act(r, my_col - 1))

    def direct_tops(act):
        span(3, jnp.where(has_above, my_col, 0), lambda c: act(0, c))

        @pl.when(has_above & (my_col == 2))
        def _():
            act(0, 3)

    zero_line = jnp.zeros((1, LANES), jnp.float32)
    barrier = pltpu.get_barrier_semaphore()

    def await_signals(semaphore, count):

        @pl.when(count > 0)
        def _():
            pl.semaphore_wait(semaphore, count)

    def greet(semaphore):
        return lambda r, c: pl.semaphore_signal(
            semaphore, inc=1, device_id=(r, c), device_id_type=MESH
        )

    origin = (my_row == 0) & (my_col == 0)

    def greet_above(semaphore, unknown):

        def greet_row(r, c):

            @pl.when(unknown_to(r) == unknown)
            def _():
                greet(semaphore)(r, c)

        along_col(0 if unknown else jnp.maximum(my_row - 2, 0), my_row, greet_row)

    for slots in (row_h, top_h):
        for k in range(grid_cols):
            slots[k] = zero_line

    greet_above(barrier, False)
    along_row(jnp.where(greets_left, my_col - 1, my_col), my_col, greet(barrier))
    start_loads()
    pair_top = (my_row == 0) & (my_col < 2)
    few = my_col + jnp.where(paired, 1, 2)
    along_row(my_col + 1, jnp.where(lead, few, grid_cols), greet(barrier))

    @pl.when(second)
    def _():
        greet(barrier)(0, 0)
        greet(barrier)(0, 1)

    along_col(jnp.where(tail, my_row + 1, my_row + 3), grid_rows, greet(barrier))
    far_below(greet(barrier))
    left_below(greet(barrier))

    def clear(ref, unless):

        @pl.when(jnp.logical_not(unless))
        def _():
            ref[...] = jnp.zeros(ref.shape, ref.dtype)

    clear(right_in, has_right)
    clear(corner_above, has_above)
    clear(corner_left, has_left & has_below)
    clear(mine_y, has_above)

    first = jnp.logical_not(has_below) | tail
    last = (my_row == 0) & (my_col < 2) & jnp.logical_not(first)
    between = jnp.logical_not(first | last)

    weighs_late = last | before_second

    def enter():
        top_sources = jnp.where(paired | second, 1, jnp.maximum(my_col - 3, 0))
        sources = jnp.where(my_row == 0, top_sources, my_col)
        sources = sources + jnp.where(pair_top, 1, 0)
        sources = sources + unknown_above
        sources = sources + jnp.where(has_above, jnp.maximum(my_col - 3, 0), 0)
        sources = sources + jnp.where(has_above & (my_col == 2), 1, 0)
        sources = sources + (near - 1 - my_row) + jnp.where(knows_right, 1, 0)
        await_signals(barrier, sources)

        @pl.when(jnp.logical_not(first | last))
        def _():
            push(0)
            push(4)

        along_row(first_left, jnp.where(greets_left, my_col - 1, my_col), greet(row_in))
        greet_above(col_in, True)
        direct_tops(greet(far_in))

    corner = cells.at[pl.ds(tile_rows - 8, 8), pl.ds(tile_cols - LANES, LANES)]
    links = (
        (left_out, right_in, 0, -1, has_left & jnp.logical_not(before_second), has_right & jnp.logical_not(paired)),
        (corner, corner_above, 1, 0, has_below, has_above),
        (corner, corner_left, 0, 1, has_right & has_below, has_left & has_below),
        (ends, ends_in, 0, 2, paired, second),
        (left_out, pair_in, 0, 1, before_second, second),
    )

    def link_copy(k):
        source, target, d_row, d_col, _, _ = links[k]
        place = (
            lax.rem(my_row + d_row + grid_rows, grid_rows),
            lax.rem(my_col + d_col + grid_cols, grid_cols),
        )
        return pltpu.make_async_remote_copy(
            src_ref=source, dst_ref=target, send_sem=link_send.at[k], recv_sem=link_recv.at[k],
            device_id=place, device_id_type=MESH,
        )

    def push(k):

        @pl.when(links[k][4])
        def _():
            link_copy(k).start()

    def arrived(k):

        @pl.when(links[k][5])
        def _():
            link_copy(k).wait_recv()

    def send(source, target, send_sem, recv_sem, place):
        return pltpu.make_async_remote_copy(
            src_ref=source, dst_ref=target, send_sem=send_sem, recv_sem=recv_sem,
            device_id=place, device_id_type=MESH,
        )

    def top_copy(r, c):
        line = tops.at[my_row]
        return send(line, line, top_send.at[r], top_recv, (r, c))

    def bottom_copy(r, c):
        return send(bottom_out, bottoms.at[my_row], bottom_send.at[r], bottom_recv, (r, c))

    def row_copy(r, c):
        return send(mine_h.at[1], row_h.at[my_col], h_send.at[r * grid_cols + c], row_recv, (r, c))

    def far_copy(r, c):
        return send(mine_h.at[1], top_h.at[my_col], h_send.at[r * grid_cols + c], far_recv, (r, c))

    def origin_copy(r, c):
        return send(mine_h.at[1], row_h.at[0], h_send.at[r * grid_cols + c], link_recv.at[5], (r, c))

    def relay_in(r, c):
        return send(mine_h.at[2], col_h, c_send.at[r], link_recv.at[6], (r, c))

    def relay_left(r, c):
        return send(mine_h.at[0], col_h, h_send.at[r * grid_cols + c], link_recv.at[6], (r, c))

    def relay_back(r, c):
        return send(mine_h.at[0], row_h.at[1], h_send.at[r * grid_cols + c], link_recv.at[5], (r, c))

    def left_copy(r, c):
        return send(mine_y, left_d, d_send.at[c], link_recv.at[7], (r, c))

    def push_tops(low, high, act):
        along_col(jnp.where(has_above, low, grid_rows), high, act)

    def push_bottoms():
        along_col(my_row + 1, near, lambda r, c: bottom_copy(r, c).start())

    def down_weights():
        outer_row = bottom_out[0:right, :]
        bottom_out[right : 2 * right, :] = weights(
            inner_row[...], outer_row,
            corner_left[6:7, LANES - 1 : LANES], corner_left[7:8, LANES - 1 : LANES],
            my_col == 0,
        )

    def push_down():
        pl.when(jnp.logical_not(tail))(lambda: push(1))
        push(2)

        @pl.when(has_below & jnp.logical_not(has_left))
        def _():
            push_bottoms()

    def row_line(row):
        return jnp.concatenate(
            [cells[row : row + 1, k * LANES : (k + 1) * LANES] for k in range(right)], axis=0
        )

    def col_lines(block, low, high):
        turned = [
            cells[k * LANES : (k + 1) * LANES, block * LANES : (block + 1) * LANES].T
            for k in range(down)
        ]
        return [jnp.concatenate([t[j : j + 1, :] for t in turned], axis=0) for j in range(low, high)]

    with jax.named_scope("enter_0"):
        pl.when(first)(enter)
    with jax.named_scope("load_head"):
        loads[0].wait()
    with jax.named_scope("head"):
        head_line = col_lines(0, 0, 1)[0]
        left_out[0:down, :] = head_line
        left_out[down:, :] = line_counts(head_line)
    with jax.named_scope("push_first"):

        @pl.when(first)
        def _():
            push(0)
            push(4)


    with jax.named_scope("load_edges"):
        loads[1].wait()
        loads[2].wait()
        loads[-1].wait()
        loads[-2].wait()
    with jax.named_scope("last_row"):
        outer_row = row_line(tile_rows - 1)
        down_count = left_out[2 * down - 1 :, LANES - 1 :] - steps_down[0].astype(jnp.float32)
        bottom_out[0:right, :] = outer_row
        bottom_out[2 * right :, :] = down_count + line_counts(outer_row)
        inner_row[...] = row_line(tile_rows - 2)

        @pl.when(jnp.logical_not(has_left))
        def _():
            down_weights()

    with jax.named_scope("enter_1"):
        pl.when(between)(enter)

        @pl.when(jnp.logical_not(last))
        def _():
            push_down()

    with jax.named_scope("first_row"):

        @pl.when(has_above)
        def _():
            first_row = row_line(0)
            tops[my_row, 0:right, :] = first_row
            tops[my_row, right:, :] = line_counts(first_row)

        push_tops(my_row + 1, near, lambda r, c: top_copy(r, c).start())

    lane = iota((STRIP, LANES), 1)

    def strip(k, carry):
        rows = pl.ds(pl.multiple_of(k * STRIP, STRIP), STRIP)
        wrapped_around = cells[rows, 0:LANES]
        sums = jnp.zeros((STRIP, LANES), jnp.float32)
        for j in range(right):
            cols = slice(j * LANES, (j + 1) * LANES)
            here = cells[rows, cols]
            rolled = pltpu.roll(here, 1, 1)
            across = cycles(here - jnp.where(lane == 0, wrapped_around, rolled))
            wrapped_around = rolled
            floors[rows, cols] = across.astype(jnp.bfloat16)
            sums = sums + across
        row_sums[rows, :] = sums.astype(jnp.bfloat16)
        return carry

    def weigh_bottom():
        arrived(2)
        down_weights()
        push_bottoms()

    def push_further_tops():
        await_signals(col_in, grid_rows - near)
        pl.when(tail)(lambda: push(1))
        push_tops(near, grid_rows, lambda r, c: top_copy(r, c).start())

    per_chunk = rows_step // STRIP
    for q in range(chunks):
        if q == chunks - 1:
            with jax.named_scope("tail_in"):
                pl.when(tail)(push_further_tops)
                pl.when(has_left & has_below & jnp.logical_not(weighs_late))(weigh_bottom)
        with jax.named_scope(f"load_{q}"):
            loads[q + 3].wait()
        with jax.named_scope(f"floors_{q}"):
            lax.fori_loop(
                q * per_chunk, (q + 1) * per_chunk, strip, 0, unroll=math.gcd(per_chunk, 8)
            )
        if q == (chunks - 1) // 2:
            with jax.named_scope("enter_2"):

                @pl.when(last)
                def _():
                    enter()
                    push(0)
                    push_down()

    with jax.named_scope("corner_left"):
        pl.when(has_left & has_below & weighs_late)(weigh_bottom)

    with jax.named_scope("col_in"):
        pl.when(jnp.logical_not(tail))(push_further_tops)
        along_col(near, grid_rows, lambda r, c: bottom_copy(r, c).start())

    relays = (my_col > 0) & (my_col < 4)
    to_relay = jnp.where(paired | second, 1, grid_rows)
    left_side = has_above & jnp.logical_not(has_left)
    to_right = jnp.where(left_side, 1, grid_cols)
    to_row = jnp.where(pair_top, grid_cols, my_col + 1)
    row_end = jnp.where(before_second, 4, grid_cols)

    def pair_places(act):
        span(jnp.where(origin, 0, 2), 2, lambda k: act(0, 1 + 2 * k))

    def hear_one(ref, semaphore):
        pltpu.make_async_copy(ref, ref, semaphore).wait()

    def end_values():
        with jax.named_scope("ends"):
            ones = jnp.ones((16, LANES), jnp.bfloat16)
            pieces = []
            for k in range(down):
                sums = lax.dot_general(
                    ones, row_sums[k * LANES : (k + 1) * LANES, :], (((1,), (1,)), ((), ())),
                    preferred_element_type=jnp.float32,
                )
                pieces.append(sums[0:1, :])
            end_count = left_out[down:, :] + jnp.concatenate(pieces, axis=0)
            end_count = end_count - steps_across[0].astype(jnp.float32)
            return (end_count, *col_lines(right - 1, LANES - 2, LANES))

    def rest_weights(inner_col, outer_col):
        weight = weights(inner_col, outer_col, inner_col[0:1, 0:1], outer_col[0:1, 0:1], True)
        start = (iota(weight.shape, 0) == 0) & (iota(weight.shape, 1) == 0)
        return jnp.where(start & has_above, 0.0, weight)

    def first_weight(inner, outer):
        inner_before = corner_above[7:8, LANES - 2 : LANES - 1]
        outer_before = corner_above[7:8, LANES - 1 : LANES]
        charge = cycles(outer_before - inner_before) + cycles(outer - outer_before)
        charge = charge - cycles(outer - inner) - cycles(inner - inner_before)
        return jnp.where(has_above, 1.0 / (1.0 + jnp.abs(charge)), 0.0)

    def end_sums(weight, outer_col, end_count, first_col, first_count):
        jump = first_count - end_count - cycles(first_col - outer_col)
        return summed(weight * jump), summed(weight), jump[0:1, 0:1]

    def finish_mean(sums, inner, outer):
        jumps, weight, first_jump = sums
        extra = first_weight(inner, outer)
        return jnp.broadcast_to((jumps + extra * first_jump) / (weight + extra), (1, LANES))

    def across():
        end_count, inner_col, outer_col = end_values()
        with jax.named_scope("weights_h"):
            ends[0:down, :] = rest_weights(inner_col, outer_col)
            ends[down : 2 * down, :] = outer_col
            ends[2 * down :, :] = end_count
            first_inner[...] = inner_col[0:1, :]
            push(3)

    def across_mean():
        with jax.named_scope("halo_0"):
            arrived(0)
        with jax.named_scope("base_h"):
            sums = end_sums(
                ends[0:down, :], ends[down : 2 * down, :], ends[2 * down :, :],
                right_in[0:down, :], right_in[down:, :],
            )
            arrived(1)
            mine_h[1] = finish_mean(sums, first_inner[0:1, 0:1], ends[down : down + 1, 0:1])
            pair_places(lambda r, c: origin_copy(r, c).start())

    def across_pair():
        with jax.named_scope("pair"):
            hear_one(row_h.at[0], link_recv.at[5])

            @pl.when(paired)
            def _():
                mine_h[2] = row_h[0]

            @pl.when(second)
            def _():
                arrived(4)
                hear_one(row_h.at[2], row_recv)
                arrived(3)
                jumps, weight, _ = end_sums(
                    ends_in[0:down, :], ends_in[down : 2 * down, :], ends_in[2 * down :, :],
                    pair_in[0:down, :], pair_in[down:, :],
                )
                before = jnp.broadcast_to(jumps / weight, (1, LANES))
                row_h[1] = before
                upto = row_h[0] + before
                mine_h[0] = upto
                mine_h[2] = upto + row_h[2]
                mine_h[1] = mine_h[1] + (upto + row_h[2])
                relay_back(0, 2).start()

            along_col(to_relay, grid_rows, lambda r, c: relay_in(r, c).start())

    def await_row():
        known = jnp.where(knows_right, my_col + 1, my_col)
        await_signals(row_in, jnp.where(lead, 0, grid_cols - 1 - known))

    def tell():
        with jax.named_scope("row_in"):
            await_row()
            along_row(to_row, row_end, lambda r, c: row_copy(r, c).start())

    def tell_far():
        with jax.named_scope("far_in"):
            right_count = grid_cols - 1 - my_col + jnp.where(second, 1, 0)
            await_signals(far_in, jnp.where(direct_top, (grid_rows - 1) * right_count, 0))
            left_below(lambda r, c: relay_left(r, c).start())
            far_below(lambda r, c: far_copy(r, c).start())

    def hear(slots, semaphore, first, count):
        for n in range(1, slots.shape[0] - max(first - 1, 0)):

            @pl.when(count == n)
            def _():
                landed = slots.at[pl.ds(first, n)]
                pltpu.make_async_copy(landed, landed, semaphore).wait()

    def hear_above():
        with jax.named_scope("hear_y"):
            hear(tops, top_recv, 1, my_row - 1)
            hear(bottoms, bottom_recv, 0, my_row)

    def sum_above():
        down_here = jnp.zeros((1, 1), jnp.float32)
        for k in range(grid_rows - 1):
            value = mismatch(
                bottoms[k, right : 2 * right, :], bottoms[k, 0:right, :],
                bottoms[k, 2 * right :, :], tops[k + 1, 0:right, :], tops[k + 1, right:, :],
            )
            down_here = down_here + jnp.where(k < my_row, value, 0.0)
        mine_y[...] = jnp.broadcast_to(down_here, mine_y.shape)

    def down_sum():
        hear_above()
        with jax.named_scope("base_y"):
            pl.when(has_above)(sum_above)

    def left_start():
        end_count, inner_col, outer_col = end_values()
        with jax.named_scope("halo_left"):
            arrived(0)
        with jax.named_scope("weights_left"):
            sums = end_sums(
                rest_weights(inner_col, outer_col), outer_col, end_count,
                right_in[0:down, :], right_in[down:, :],
            )
            for k, value in enumerate((*sums, inner_col[0:1, 0:1], outer_col[0:1, 0:1])):
                left_sums[k] = jnp.broadcast_to(value, (1, LANES))

    def left_finish():
        with jax.named_scope("halo_left_1"):
            arrived(1)
            jumps, weight, jump, inner, outer = (left_sums[k] for k in range(5))
            mine_h[1] = finish_mean((jumps, weight, jump), inner, outer)
        hear_above()
        with jax.named_scope("base_left"):
            sum_above()
        with jax.named_scope("row_in_left"):
            await_row()
            along_row(to_right, grid_cols, lambda r, c: left_copy(r, c).start())
            along_row(to_row, row_end, lambda r, c: row_copy(r, c).start())

    def integrate(low, high):
        with jax.named_scope(f"integrate_{low}"):
            upper, lower = triangle(cols_step, 0), triangle(rows_step, 1)
            down_carry = jnp.zeros((1, LANES), jnp.float32) if low == 0 else carried[...]
            for q in range(low, high):
                top = q * rows_step
                rows = pl.ds(top, rows_step)
                head = cells[rows, 0:LANES]
                above = cells[max(top - 1, 0) : max(top, 1), 0:LANES]
                before = jnp.where(iota(head.shape, 0) == 0, above, pltpu.roll(head, 1, 0))
                counts = down_carry + jnp.dot(
                    lower, cycles(head - before).astype(jnp.bfloat16),
                    preferred_element_type=jnp.float32,
                )
                down_carry = counts[rows_step - 1 : rows_step, :]
                carry = counts[:, 0:1]
                for b in range(tile_cols // cols_step):
                    cols = slice(b * cols_step, (b + 1) * cols_step)
                    count = carry + jnp.dot(
                        floors[rows, cols], upper, preferred_element_type=jnp.float32
                    )
                    carry = count[:, cols_step - 1 : cols_step]
                    integ[rows, cols] = cells[rows, cols] * (1.0 / TWO_PI) - count
            if high < chunks:
                carried[...] = down_carry

    odd_row = lax.rem(my_row, 2) == 1
    far_early = (my_row == 0) & (my_col > 3)
    split = (even_row & has_left) | (tail_col & odd_row)
    half = (chunks + 1) // 2
    never = 10
    at_left, at_top, at_pair, at_split, at_second, otherwise = range(6)
    kind = jnp.where(second, at_second, jnp.where(split, at_split, otherwise))
    kind = jnp.where(pair, jnp.where(paired, at_top, at_pair), kind)
    kind = jnp.where(left_side, at_left, kind)

    def pick(*slots):
        chosen = slots[otherwise]
        for k in range(otherwise):
            chosen = jnp.where(kind == k, slots[k], chosen)
        return chosen

    order = (
        (left_start, pick(0, never, never, never, never, never)),
        (left_finish, pick(2, never, never, never, never, never)),
        (across, jnp.where(has_right, pick(never, 0, 1, 1, 1, 0), never)),
        (across_mean, jnp.where(has_right, pick(never, never, 2, 2, 2, 1), never)),
        (across_pair, pick(never, 2, never, never, 3, never)),
        (tell, pick(never, never, 3, 3, 4, 2)),
        (functools.partial(integrate, 0, half), pick(1, 1, 0, 0, 0, jnp.where(far_early, 4, 3))),
        (tell_far, jnp.where(direct_top, jnp.where(second, 5, jnp.where(far_early, 3, 4)), never)),
        (functools.partial(integrate, half, chunks), pick(3, 3, 5, 4, 6, 5)),
        (down_sum, pick(never, never, 4, 5, never, 6)),
    )

    def phase(k, carry):
        for act, at in order:
            pl.when(k == at)(act)
        return carry

    lax.fori_loop(0, len(order), phase, 0)

    pl.when(jnp.logical_not(has_right | left_side))(lambda: arrived(1))

    with jax.named_scope("sent"):
        for k in range(5):

            @pl.when(links[k][4])
            def _():
                link_copy(k).wait_send()

        push_tops(my_row + 1, grid_rows, lambda r, c: top_copy(r, c).wait_send())
        along_col(my_row + 1, grid_rows, lambda r, c: bottom_copy(r, c).wait_send())
        along_col(to_relay, grid_rows, lambda r, c: relay_in(r, c).wait_send())
        along_row(to_row, row_end, lambda r, c: row_copy(r, c).wait_send())
        pair_places(lambda r, c: origin_copy(r, c).wait_send())
        left_below(lambda r, c: relay_left(r, c).wait_send())

        @pl.when(second)
        def _():
            relay_back(0, 2).wait_send()

        far_below(lambda r, c: far_copy(r, c).wait_send())
        along_row(to_right, grid_cols, lambda r, c: left_copy(r, c).wait_send())

    with jax.named_scope("hear"):
        hear(row_h, row_recv, 3, jnp.where(has_above, 0, my_col - 3))
        hear(row_h, row_recv, 0, jnp.where(has_above, my_col, 0))
        hear(top_h, far_recv, 3, jnp.where(has_above, my_col - 3, 0))

        @pl.when(has_above & relays)
        def _():
            hear_one(col_h, link_recv.at[6])

        @pl.when(before_second)
        def _():
            hear_one(row_h.at[1], link_recv.at[5])

        @pl.when(has_above & has_left)
        def _():
            hear_one(left_d, link_recv.at[7])

    with jax.named_scope("finish"):

        def prefix(slots):
            line = slots[0]
            for k in range(1, grid_cols):
                line = line + slots[k]
            return line

        across_here = prefix(row_h)
        across_top = prefix(top_h) + jnp.where(relays, col_h[...], 0.0)
        across_top = jnp.where(has_above, across_top, across_here)
        down_here = mine_y[...]
        down_left = jnp.where(has_left & has_above, left_d[...], down_here)
        here = left = top = start = zero_line
        for sweep in range(ITERS):
            prefix_across = across_here + (left - here)
            prefix_across_top = across_top + (start - top)
            prefix_down = down_here + (top - here)
            prefix_down_left = down_left + (start - left)
            here = here + 0.5 * (prefix_across + prefix_across_top + prefix_down + prefix_down_left)
            left = left + prefix_down_left
            top = top + prefix_across_top
        offset[...] = jnp.broadcast_to(here, offset.shape)


def place_kernel(integ, offset, out, ready, sems):
    parts = sems.shape[0]
    step = integ.shape[0] // parts
    shift = offset[0:1, 0:1]
    copies = []
    for q in range(parts):
        rows = pl.ds(q * step, step)
        ready[rows, :] = integ[rows, :] + shift
        copy = pltpu.make_async_copy(ready.at[rows], out.at[rows], sems.at[q])
        copy.start()
        copies.append(copy)
    for copy in copies:
        copy.wait()


def on_device(names, sizes, wrapped, col_steps, row_steps):
    frames, tile_rows, tile_cols = wrapped.shape
    grid_rows, grid_cols = sizes
    down, right = tile_rows // LANES, tile_cols // LANES
    dma = pltpu.SemaphoreType.DMA
    rows_step = math.gcd(tile_rows, 256)
    cols_step = math.gcd(tile_cols, 256)
    f32 = jnp.float32

    def with_local_semaphores(*refs):
        pl.run_scoped(
            functools.partial(edge_kernel, names, sizes, rows_step, cols_step, *refs),
            dma((tile_rows // rows_step + 5,)), dma((5,)), dma((grid_rows,)), dma((grid_rows,)),
            dma((grid_rows * grid_cols,)), dma((grid_rows,)), dma((grid_cols,)),
        )

    call = pl.pallas_call(
        with_local_semaphores,
        out_shape=(
            pltpu.VMEM((tile_rows, tile_cols), f32),
            pltpu.VMEM((8, LANES), f32),
        ),
        in_specs=[
            pl.BlockSpec(memory_space=pltpu.HBM),
            pl.BlockSpec(memory_space=pltpu.HBM),
            pl.BlockSpec(memory_space=pltpu.HBM),
        ],
        out_specs=(
            pl.BlockSpec(memory_space=pltpu.VMEM),
            pl.BlockSpec(memory_space=pltpu.VMEM),
        ),
        scratch_shapes=[
            pltpu.VMEM((tile_rows, tile_cols), f32),
            pltpu.VMEM((2 * down, LANES), f32),
            pltpu.VMEM((2 * down, LANES), f32),
            pltpu.VMEM((8, LANES), f32),
            pltpu.VMEM((8, LANES), f32),
            pltpu.VMEM((grid_rows, 2 * right, LANES), f32),
            pltpu.VMEM((3 * right, LANES), f32),
            pltpu.VMEM((grid_rows, 3 * right, LANES), f32),
            pltpu.VMEM((right, LANES), f32),
            pltpu.VMEM((tile_rows, tile_cols), jnp.bfloat16),
            pltpu.VMEM((tile_rows, LANES), jnp.bfloat16),
            pltpu.VMEM((1, 1, 1), jnp.int32),
            pltpu.VMEM((1, 1, 1), jnp.int32),
            pltpu.VMEM((3, 1, LANES), f32),
            pltpu.VMEM((1, LANES), f32),
            pltpu.VMEM((grid_cols, 1, LANES), f32),
            pltpu.VMEM((grid_cols, 1, LANES), f32),
            pltpu.VMEM((1, LANES), f32),
            pltpu.VMEM((1, LANES), f32),
            pltpu.VMEM((1, LANES), f32),
            pltpu.VMEM((3 * down, LANES), f32),
            pltpu.VMEM((3 * down, LANES), f32),
            pltpu.VMEM((2 * down, LANES), f32),
            pltpu.VMEM((1, LANES), f32),
            pltpu.VMEM((5, 1, LANES), f32),
            dma((8,)), dma, dma, dma, dma,
            pltpu.SemaphoreType.REGULAR,
            pltpu.SemaphoreType.REGULAR,
            pltpu.SemaphoreType.REGULAR,
        ],
        compiler_params=pltpu.CompilerParams(
            collective_id=0, has_side_effects=True, vmem_limit_bytes=57 * 1024 * 1024
        ),
    )
    parts = math.gcd(tile_rows // 8, 16)
    place = pl.pallas_call(
        place_kernel,
        out_shape=jax.ShapeDtypeStruct((tile_rows, tile_cols), f32),
        in_specs=[pl.BlockSpec(memory_space=pltpu.VMEM), pl.BlockSpec(memory_space=pltpu.VMEM)],
        out_specs=pl.BlockSpec(memory_space=pltpu.HBM),
        scratch_shapes=[
            pltpu.VMEM((tile_rows, tile_cols), f32),
            pltpu.SemaphoreType.DMA((parts,)),
        ],
        compiler_params=pltpu.CompilerParams(vmem_limit_bytes=24 * 1024 * 1024),
    )
    outs = [
        place(*call(wrapped[f : f + 1], col_steps[f : f + 1], row_steps[f : f + 1]))
        for f in range(frames)
    ]
    return jnp.stack(outs)


def solution(mesh):
    spec = P(None, "row", "col")
    sizes = (mesh.shape["row"], mesh.shape["col"])
    return jax.shard_map(
        functools.partial(on_device, ("row", "col"), sizes),
        mesh=mesh, in_specs=(spec, spec, spec), out_specs=spec, check_vma=False,
    )
```

```python
import functools
import math

import jax
import jax.numpy as jnp
from jax import lax
from jax.experimental import pallas as pl
from jax.experimental.pallas import tpu as pltpu
from jax.sharding import PartitionSpec as P

ITERS = 2
TWO_PI = 2.0 * math.pi
MESH = pl.DeviceIdType.MESH
LANES = 128
STRIP = 16


def cycles(change):
    return jnp.floor(change * (1.0 / TWO_PI) + 0.5)


def iota(shape, dim):
    return lax.broadcasted_iota(jnp.int32, shape, dim)


def total(values):
    return jnp.sum(values, axis=1, keepdims=True)


def previous(line, first):
    lane, row = iota(line.shape, 1), iota(line.shape, 0)
    along = pltpu.roll(line, 1, 1)
    across = pltpu.roll(along, 1, 0) if line.shape[0] > 1 else along
    return jnp.where(lane > 0, along, jnp.where(row > 0, across, first))


def summed(line):
    return total(jnp.sum(line, axis=0, keepdims=True))


def triangle(size, dim):
    ordered = iota((size, size), dim) <= iota((size, size), 1 - dim)
    return ordered.astype(jnp.float32).astype(jnp.bfloat16)


def line_counts(line):
    groups = line.shape[0]
    row = iota(line.shape, 0)
    floors = cycles(line - previous(line, line[0:1, 0:1]))
    whole, shift = floors, 1
    while shift < groups:
        whole = whole + jnp.where(row >= shift, pltpu.roll(whole, shift, 0), 0.0)
        shift *= 2
    pair = jnp.concatenate([floors, whole - floors], axis=1)
    pair = jnp.concatenate([pair] * (-(-16 // groups)), axis=0).astype(jnp.bfloat16)
    ones = jnp.ones((LANES, LANES), jnp.bfloat16)
    table = jnp.concatenate([triangle(LANES, 0), ones], axis=0)
    return jnp.dot(pair, table, preferred_element_type=jnp.float32)[0:groups, :]


def weights(inner, outer, inner_before, outer_before, at_image_edge):
    over = cycles(outer - inner)
    over_before = previous(over, cycles(outer_before - inner_before))
    along_outer = cycles(outer - previous(outer, outer_before))
    along_inner = cycles(inner - previous(inner, inner_before))
    charge = over_before + along_outer - over - along_inner
    start = (iota(charge.shape, 1) == 0) & (iota(charge.shape, 0) == 0)
    charge = jnp.where(start & at_image_edge, 0.0, charge)
    return 1.0 / (1.0 + jnp.abs(charge))


def mismatch(weight, outer, count, first, beyond):
    jump = beyond - count - cycles(first - outer)
    return summed(weight * jump) / summed(weight)


def edge_kernel(
    names, sizes, rows_step, cols_step,
    wrapped, col_steps, row_steps,
    integ, offset,
    cells, left_out, right_in, corner_above, corner_left, tops, bottom_out, bottoms, inner_row,
    floors, row_sums, steps_across, steps_down, mine_h, mine_y, row_h, top_h, col_h, left_d, carried, ends, ends_in, pair_in, first_inner, left_sums,
    link_recv, top_recv, bottom_recv, row_recv, far_recv, row_in, col_in, far_in,
    load_sem, link_send, top_send, bottom_send, h_send, c_send, d_send, back_send,
):
    row_name, col_name = names
    grid_rows, grid_cols = sizes
    tile_rows, tile_cols = cells.shape
    my_row, my_col = lax.axis_index(row_name), lax.axis_index(col_name)
    down, right = tile_rows // LANES, tile_cols // LANES

    chunks = tile_rows // rows_step
    rest = pl.ds(LANES, tile_cols - LANES)
    regions = [
        (pl.ds(0, tile_rows), pl.ds(0, LANES)),
        (pl.ds(tile_rows - 16, 16), rest),
        (pl.ds(0, 16), rest),
    ]
    for q in range(chunks):
        top = max(q * rows_step, 16)
        bottom = min((q + 1) * rows_step, tile_rows - 16)
        regions.append((pl.ds(top, bottom - top), rest))
    loads = []
    for k, (rows, cols) in enumerate(regions):
        loads.append(
            pltpu.make_async_copy(wrapped.at[0, rows, cols], cells.at[rows, cols], load_sem.at[k])
        )
    for source, target in ((col_steps, steps_across), (row_steps, steps_down)):
        loads.append(pltpu.make_async_copy(source, target, load_sem.at[len(loads)]))

    def start_loads():
        for load in loads:
            load.start()

    def span(low, high, act):
        def step(k, carry):
            act(k)
            return carry

        lax.fori_loop(low, high, step, 0)

    def along_row(low, high, act):
        span(low, high, lambda c: act(my_row, c))

    def along_col(low, high, act):
        span(low, high, lambda r: act(r, my_col))

    has_left, has_right = my_col > 0, my_col < grid_cols - 1
    has_above, has_below = my_row > 0, my_row < grid_rows - 1
    even_row = has_above & (lax.rem(my_row, 2) == 0)
    tail_col = my_col >= grid_cols - 2
    tail = tail_col & has_below & (lax.rem(my_row, 2) == 0)

    def unknown_to(row):
        return (row < my_row) & ((my_row - row > 2) | (tail_col & (lax.rem(row, 2) == 0)))

    unknown_above = sum(jnp.where(unknown_to(k), 1, 0) for k in range(grid_rows))
    near = jnp.where(tail, my_row + 1, jnp.minimum(my_row + 3, grid_rows))
    direct_top = (my_row == 0) & (my_col > 2)
    first_left = jnp.where(my_row == 0, 3, 0)
    lead = (my_row == 0) & (my_col < 3)
    pair = my_col == 1
    paired = (my_row == 0) & pair
    second = (my_row == 0) & (my_col == 3)
    before_second = (my_row == 0) & (my_col == 2)
    greets_left = has_left & (has_below | pair | second | before_second)
    knows_right = has_right & (has_below | (my_col == 0) | paired | before_second)

    def far_below(act):
        low = jnp.where(direct_top, 1, grid_rows)
        span(low, grid_rows, lambda r: span(my_col + 1, grid_cols, lambda c: act(r, c)))

    def left_below(act):
        span(jnp.where(second, 1, grid_rows), grid_rows, lambda r: act(r, my_col - 1))

    def direct_tops(act):
        span(3, jnp.where(has_above, my_col, 0), lambda c: act(0, c))

        @pl.when(has_above & (my_col == 2))
        def _():
            act(0, 3)

    zero_line = jnp.zeros((1, LANES), jnp.float32)
    barrier = pltpu.get_barrier_semaphore()

    def await_signals(semaphore, count):

        @pl.when(count > 0)
        def _():
            pl.semaphore_wait(semaphore, count)

    def greet(semaphore):
        return lambda r, c: pl.semaphore_signal(
            semaphore, inc=1, device_id=(r, c), device_id_type=MESH
        )

    origin = (my_row == 0) & (my_col == 0)

    def greet_above(semaphore, unknown):

        def greet_row(r, c):

            @pl.when(unknown_to(r) == unknown)
            def _():
                greet(semaphore)(r, c)

        along_col(0 if unknown else jnp.maximum(my_row - 2, 0), my_row, greet_row)

    for slots in (row_h, top_h):
        for k in range(grid_cols):
            slots[k] = zero_line

    greet_above(barrier, False)
    along_row(jnp.where(greets_left, my_col - 1, my_col), my_col, greet(barrier))
    start_loads()
    pair_top = (my_row == 0) & (my_col < 2)
    few = my_col + jnp.where(paired, 1, 2)
    along_row(my_col + 1, jnp.where(lead, few, grid_cols), greet(barrier))

    @pl.when(second)
    def _():
        greet(barrier)(0, 0)
        greet(barrier)(0, 1)

    along_col(jnp.where(tail, my_row + 1, my_row + 3), grid_rows, greet(barrier))
    far_below(greet(barrier))
    left_below(greet(barrier))

    def clear(ref, unless):

        @pl.when(jnp.logical_not(unless))
        def _():
            ref[...] = jnp.zeros(ref.shape, ref.dtype)

    clear(right_in, has_right)
    clear(corner_above, has_above)
    clear(corner_left, has_left & has_below)
    clear(mine_y, has_above)

    first = jnp.logical_not(has_below) | tail
    last = (my_row == 0) & (my_col < 2) & jnp.logical_not(first)
    between = jnp.logical_not(first | last)

    weighs_late = last | before_second

    def enter():
        top_sources = jnp.where(paired | second, 1, jnp.maximum(my_col - 3, 0))
        sources = jnp.where(my_row == 0, top_sources, my_col)
        sources = sources + jnp.where(pair_top, 1, 0)
        sources = sources + unknown_above
        sources = sources + jnp.where(has_above, jnp.maximum(my_col - 3, 0), 0)
        sources = sources + jnp.where(has_above & (my_col == 2), 1, 0)
        sources = sources + (near - 1 - my_row) + jnp.where(knows_right, 1, 0)
        await_signals(barrier, sources)

        @pl.when(jnp.logical_not(first | last))
        def _():
            push(0)
            push(4)

        along_row(first_left, jnp.where(greets_left, my_col - 1, my_col), greet(row_in))
        greet_above(col_in, True)
        direct_tops(greet(far_in))

    corner = cells.at[pl.ds(tile_rows - 8, 8), pl.ds(tile_cols - LANES, LANES)]
    links = (
        (left_out, right_in, 0, -1, has_left & jnp.logical_not(before_second), has_right & jnp.logical_not(paired)),
        (corner, corner_above, 1, 0, has_below, has_above),
        (corner, corner_left, 0, 1, has_right & has_below, has_left & has_below),
        (ends, ends_in, 0, 2, paired, second),
        (left_out, pair_in, 0, 1, before_second, second),
    )

    def link_copy(k):
        source, target, d_row, d_col, _, _ = links[k]
        place = (
            lax.rem(my_row + d_row + grid_rows, grid_rows),
            lax.rem(my_col + d_col + grid_cols, grid_cols),
        )
        return pltpu.make_async_remote_copy(
            src_ref=source, dst_ref=target, send_sem=link_send.at[k], recv_sem=link_recv.at[k],
            device_id=place, device_id_type=MESH,
        )

    def push(k):

        @pl.when(links[k][4])
        def _():
            link_copy(k).start()

    def arrived(k):

        @pl.when(links[k][5])
        def _():
            link_copy(k).wait_recv()

    def send(source, target, send_sem, recv_sem, place):
        return pltpu.make_async_remote_copy(
            src_ref=source, dst_ref=target, send_sem=send_sem, recv_sem=recv_sem,
            device_id=place, device_id_type=MESH,
        )

    def top_copy(r, c):
        line = tops.at[my_row]
        return send(line, line, top_send.at[r], top_recv, (r, c))

    def bottom_copy(r, c):
        return send(bottom_out, bottoms.at[my_row], bottom_send.at[r], bottom_recv, (r, c))

    def row_copy(r, c):
        return send(mine_h.at[1], row_h.at[my_col], h_send.at[r], row_recv, (r, c))

    def far_copy(r, c):
        return send(mine_h.at[1], top_h.at[my_col], h_send.at[r], far_recv, (r, c))

    def origin_copy(r, c):
        return send(mine_h.at[1], row_h.at[0], h_send.at[r], link_recv.at[5], (r, c))

    def relay_in(r, c):
        return send(mine_h.at[2], col_h, c_send.at[r], link_recv.at[6], (r, c))

    def relay_left(r, c):
        return send(mine_h.at[0], col_h, h_send.at[r], link_recv.at[6], (r, c))

    def relay_back(r, c):
        return send(mine_h.at[0], row_h.at[1], back_send, link_recv.at[5], (r, c))

    def left_copy(r, c):
        return send(mine_y, left_d, d_send, link_recv.at[7], (r, c))

    def push_tops(low, high, act):
        along_col(jnp.where(has_above, low, grid_rows), high, act)

    def push_bottoms():
        along_col(my_row + 1, near, lambda r, c: bottom_copy(r, c).start())

    def down_weights():
        outer_row = bottom_out[0:right, :]
        bottom_out[right : 2 * right, :] = weights(
            inner_row[...], outer_row,
            corner_left[6:7, LANES - 1 : LANES], corner_left[7:8, LANES - 1 : LANES],
            my_col == 0,
        )

    def push_down():
        pl.when(jnp.logical_not(tail))(lambda: push(1))
        push(2)

        @pl.when(has_below & jnp.logical_not(has_left))
        def _():
            push_bottoms()

    def row_line(row):
        return jnp.concatenate(
            [cells[row : row + 1, k * LANES : (k + 1) * LANES] for k in range(right)], axis=0
        )

    def col_lines(block, low, high):
        turned = [
            cells[k * LANES : (k + 1) * LANES, block * LANES : (block + 1) * LANES].T
            for k in range(down)
        ]
        return [jnp.concatenate([t[j : j + 1, :] for t in turned], axis=0) for j in range(low, high)]

    with jax.named_scope("enter_0"):
        pl.when(first)(enter)
    with jax.named_scope("load_head"):
        loads[0].wait()
    with jax.named_scope("head"):
        head_line = col_lines(0, 0, 1)[0]
        left_out[0:down, :] = head_line
        left_out[down:, :] = line_counts(head_line)
    with jax.named_scope("push_first"):

        @pl.when(first)
        def _():
            push(0)
            push(4)


    with jax.named_scope("load_edges"):
        loads[1].wait()
        loads[2].wait()
        loads[-1].wait()
        loads[-2].wait()
    with jax.named_scope("last_row"):
        outer_row = row_line(tile_rows - 1)
        down_count = left_out[2 * down - 1 :, LANES - 1 :] - steps_down[0].astype(jnp.float32)
        bottom_out[0:right, :] = outer_row
        bottom_out[2 * right :, :] = down_count + line_counts(outer_row)
        inner_row[...] = row_line(tile_rows - 2)

        @pl.when(jnp.logical_not(has_left))
        def _():
            down_weights()

    with jax.named_scope("enter_1"):
        pl.when(between)(enter)

        @pl.when(jnp.logical_not(last))
        def _():
            push_down()

    with jax.named_scope("first_row"):

        @pl.when(has_above)
        def _():
            first_row = row_line(0)
            tops[my_row, 0:right, :] = first_row
            tops[my_row, right:, :] = line_counts(first_row)

        push_tops(my_row + 1, near, lambda r, c: top_copy(r, c).start())

    lane = iota((STRIP, LANES), 1)

    def strip(k, carry):
        rows = pl.ds(pl.multiple_of(k * STRIP, STRIP), STRIP)
        wrapped_around = cells[rows, 0:LANES]
        sums = jnp.zeros((STRIP, LANES), jnp.float32)
        for j in range(right):
            cols = slice(j * LANES, (j + 1) * LANES)
            here = cells[rows, cols]
            rolled = pltpu.roll(here, 1, 1)
            across = cycles(here - jnp.where(lane == 0, wrapped_around, rolled))
            wrapped_around = rolled
            floors[rows, cols] = across.astype(jnp.bfloat16)
            sums = sums + across
        row_sums[rows, :] = sums.astype(jnp.bfloat16)
        return carry

    def weigh_bottom():
        arrived(2)
        down_weights()
        push_bottoms()

    def push_further_tops():
        await_signals(col_in, grid_rows - near)
        pl.when(tail)(lambda: push(1))
        push_tops(near, grid_rows, lambda r, c: top_copy(r, c).start())

    per_chunk = rows_step // STRIP
    for q in range(chunks):
        if q == chunks - 1:
            with jax.named_scope("tail_in"):
                pl.when(tail)(push_further_tops)
                pl.when(has_left & has_below & jnp.logical_not(weighs_late))(weigh_bottom)
        with jax.named_scope(f"load_{q}"):
            loads[q + 3].wait()
        with jax.named_scope(f"floors_{q}"):
            lax.fori_loop(
                q * per_chunk, (q + 1) * per_chunk, strip, 0, unroll=math.gcd(per_chunk, 8)
            )
        if q == (chunks - 1) // 2:
            with jax.named_scope("enter_2"):

                @pl.when(last)
                def _():
                    enter()
                    push(0)
                    push_down()

    with jax.named_scope("corner_left"):
        pl.when(has_left & has_below & weighs_late)(weigh_bottom)

    with jax.named_scope("col_in"):
        pl.when(jnp.logical_not(tail))(push_further_tops)
        along_col(near, grid_rows, lambda r, c: bottom_copy(r, c).start())

    relays = (my_col > 0) & (my_col < 4)
    to_relay = jnp.where(paired | second, 1, grid_rows)
    left_side = has_above & jnp.logical_not(has_left)
    to_right = jnp.where(left_side, 1, grid_cols)
    to_row = jnp.where(pair_top, grid_cols, my_col + 1)
    row_end = jnp.where(before_second, 4, grid_cols)

    def pair_places(act):
        span(jnp.where(origin, 0, 2), 2, lambda k: act(0, 1 + 2 * k))

    def hear_one(ref, semaphore):
        pltpu.make_async_copy(ref, ref, semaphore).wait()

    def end_values():
        with jax.named_scope("ends"):
            ones = jnp.ones((16, LANES), jnp.bfloat16)
            pieces = []
            for k in range(down):
                sums = lax.dot_general(
                    ones, row_sums[k * LANES : (k + 1) * LANES, :], (((1,), (1,)), ((), ())),
                    preferred_element_type=jnp.float32,
                )
                pieces.append(sums[0:1, :])
            end_count = left_out[down:, :] + jnp.concatenate(pieces, axis=0)
            end_count = end_count - steps_across[0].astype(jnp.float32)
            return (end_count, *col_lines(right - 1, LANES - 2, LANES))

    def rest_weights(inner_col, outer_col):
        weight = weights(inner_col, outer_col, inner_col[0:1, 0:1], outer_col[0:1, 0:1], True)
        start = (iota(weight.shape, 0) == 0) & (iota(weight.shape, 1) == 0)
        return jnp.where(start & has_above, 0.0, weight)

    def first_weight(inner, outer):
        inner_before = corner_above[7:8, LANES - 2 : LANES - 1]
        outer_before = corner_above[7:8, LANES - 1 : LANES]
        charge = cycles(outer_before - inner_before) + cycles(outer - outer_before)
        charge = charge - cycles(outer - inner) - cycles(inner - inner_before)
        return jnp.where(has_above, 1.0 / (1.0 + jnp.abs(charge)), 0.0)

    def end_sums(weight, outer_col, end_count, first_col, first_count):
        jump = first_count - end_count - cycles(first_col - outer_col)
        return summed(weight * jump), summed(weight), jump[0:1, 0:1]

    def finish_mean(sums, inner, outer):
        jumps, weight, first_jump = sums
        extra = first_weight(inner, outer)
        return jnp.broadcast_to((jumps + extra * first_jump) / (weight + extra), (1, LANES))

    def across():
        end_count, inner_col, outer_col = end_values()
        with jax.named_scope("weights_h"):
            ends[0:down, :] = rest_weights(inner_col, outer_col)
            ends[down : 2 * down, :] = outer_col
            ends[2 * down :, :] = end_count
            first_inner[...] = inner_col[0:1, :]
            push(3)

    def across_mean():
        with jax.named_scope("halo_0"):
            arrived(0)
        with jax.named_scope("base_h"):
            sums = end_sums(
                ends[0:down, :], ends[down : 2 * down, :], ends[2 * down :, :],
                right_in[0:down, :], right_in[down:, :],
            )
            arrived(1)
            mine_h[1] = finish_mean(sums, first_inner[0:1, 0:1], ends[down : down + 1, 0:1])
            pair_places(lambda r, c: origin_copy(r, c).start())

    def across_pair():
        with jax.named_scope("pair"):
            hear_one(row_h.at[0], link_recv.at[5])

            @pl.when(paired)
            def _():
                mine_h[2] = row_h[0]

            @pl.when(second)
            def _():
                arrived(4)
                hear_one(row_h.at[2], row_recv)
                arrived(3)
                jumps, weight, _ = end_sums(
                    ends_in[0:down, :], ends_in[down : 2 * down, :], ends_in[2 * down :, :],
                    pair_in[0:down, :], pair_in[down:, :],
                )
                before = jnp.broadcast_to(jumps / weight, (1, LANES))
                row_h[1] = before
                upto = row_h[0] + before
                mine_h[0] = upto
                mine_h[2] = upto + row_h[2]
                mine_h[1] = mine_h[1] + (upto + row_h[2])
                relay_back(0, 2).start()

            along_col(to_relay, grid_rows, lambda r, c: relay_in(r, c).start())

    def await_row():
        known = jnp.where(knows_right, my_col + 1, my_col)
        await_signals(row_in, jnp.where(lead, 0, grid_cols - 1 - known))

    def tell():
        with jax.named_scope("row_in"):
            await_row()
            along_row(to_row, row_end, lambda r, c: row_copy(r, c).start())

    def tell_far():
        with jax.named_scope("far_in"):
            right_count = grid_cols - 1 - my_col + jnp.where(second, 1, 0)
            await_signals(far_in, jnp.where(direct_top, (grid_rows - 1) * right_count, 0))
            left_below(lambda r, c: relay_left(r, c).start())
            far_below(lambda r, c: far_copy(r, c).start())

    def hear(slots, semaphore, first, count):
        for n in range(1, slots.shape[0] - max(first - 1, 0)):

            @pl.when(count == n)
            def _():
                landed = slots.at[pl.ds(first, n)]
                pltpu.make_async_copy(landed, landed, semaphore).wait()

    def hear_above():
        with jax.named_scope("hear_y"):
            hear(tops, top_recv, 1, my_row - 1)
            hear(bottoms, bottom_recv, 0, my_row)

    def sum_above():
        down_here = jnp.zeros((1, 1), jnp.float32)
        for k in range(grid_rows - 1):
            value = mismatch(
                bottoms[k, right : 2 * right, :], bottoms[k, 0:right, :],
                bottoms[k, 2 * right :, :], tops[k + 1, 0:right, :], tops[k + 1, right:, :],
            )
            down_here = down_here + jnp.where(k < my_row, value, 0.0)
        mine_y[...] = jnp.broadcast_to(down_here, mine_y.shape)

    def down_sum():
        hear_above()
        with jax.named_scope("base_y"):
            pl.when(has_above)(sum_above)

    def left_start():
        end_count, inner_col, outer_col = end_values()
        with jax.named_scope("halo_left"):
            arrived(0)
        with jax.named_scope("weights_left"):
            sums = end_sums(
                rest_weights(inner_col, outer_col), outer_col, end_count,
                right_in[0:down, :], right_in[down:, :],
            )
            for k, value in enumerate((*sums, inner_col[0:1, 0:1], outer_col[0:1, 0:1])):
                left_sums[k] = jnp.broadcast_to(value, (1, LANES))

    def left_finish():
        with jax.named_scope("halo_left_1"):
            arrived(1)
            jumps, weight, jump, inner, outer = (left_sums[k] for k in range(5))
            mine_h[1] = finish_mean((jumps, weight, jump), inner, outer)
        hear_above()
        with jax.named_scope("base_left"):
            sum_above()
        with jax.named_scope("row_in_left"):
            await_row()
            along_row(to_right, grid_cols, lambda r, c: left_copy(r, c).start())
            along_row(to_row, row_end, lambda r, c: row_copy(r, c).start())

    def integrate(low, high):
        with jax.named_scope(f"integrate_{low}"):
            upper, lower = triangle(cols_step, 0), triangle(rows_step, 1)
            down_carry = jnp.zeros((1, LANES), jnp.float32) if low == 0 else carried[...]
            for q in range(low, high):
                top = q * rows_step
                rows = pl.ds(top, rows_step)
                head = cells[rows, 0:LANES]
                above = cells[max(top - 1, 0) : max(top, 1), 0:LANES]
                before = jnp.where(iota(head.shape, 0) == 0, above, pltpu.roll(head, 1, 0))
                counts = down_carry + jnp.dot(
                    lower, cycles(head - before).astype(jnp.bfloat16),
                    preferred_element_type=jnp.float32,
                )
                down_carry = counts[rows_step - 1 : rows_step, :]
                carry = counts[:, 0:1]
                for b in range(tile_cols // cols_step):
                    cols = slice(b * cols_step, (b + 1) * cols_step)
                    count = carry + jnp.dot(
                        floors[rows, cols], upper, preferred_element_type=jnp.float32
                    )
                    carry = count[:, cols_step - 1 : cols_step]
                    integ[rows, cols] = cells[rows, cols] * (1.0 / TWO_PI) - count
            if high < chunks:
                carried[...] = down_carry

    odd_row = lax.rem(my_row, 2) == 1
    far_early = (my_row == 0) & (my_col > 3)
    split = (even_row & has_left) | (tail_col & odd_row)
    half = (chunks + 1) // 2
    never = 10
    at_left, at_top, at_pair, at_split, at_second, otherwise = range(6)
    kind = jnp.where(second, at_second, jnp.where(split, at_split, otherwise))
    kind = jnp.where(pair, jnp.where(paired, at_top, at_pair), kind)
    kind = jnp.where(left_side, at_left, kind)

    def pick(*slots):
        chosen = slots[otherwise]
        for k in range(otherwise):
            chosen = jnp.where(kind == k, slots[k], chosen)
        return chosen

    order = (
        (left_start, pick(0, never, never, never, never, never)),
        (left_finish, pick(2, never, never, never, never, never)),
        (across, jnp.where(has_right, pick(never, 0, 1, 1, 1, 0), never)),
        (across_mean, jnp.where(has_right, pick(never, never, 2, 2, 2, 1), never)),
        (across_pair, pick(never, 2, never, never, 3, never)),
        (tell, pick(never, never, 3, 3, 4, 2)),
        (functools.partial(integrate, 0, half), pick(1, 1, 0, 0, 0, jnp.where(far_early, 4, 3))),
        (tell_far, jnp.where(direct_top, jnp.where(second, 5, jnp.where(far_early, 3, 4)), never)),
        (functools.partial(integrate, half, chunks), pick(3, 3, 5, 4, 6, 5)),
        (down_sum, pick(never, never, 4, 5, never, 6)),
    )

    def phase(k, carry):
        for act, at in order:
            pl.when(k == at)(act)
        return carry

    lax.fori_loop(0, len(order), phase, 0)

    pl.when(jnp.logical_not(has_right | left_side))(lambda: arrived(1))

    with jax.named_scope("sent"):
        for k in range(5):

            @pl.when(links[k][4])
            def _():
                link_copy(k).wait_send()

        push_tops(my_row + 1, grid_rows, lambda r, c: top_copy(r, c).wait_send())
        along_col(my_row + 1, grid_rows, lambda r, c: bottom_copy(r, c).wait_send())
        along_col(to_relay, grid_rows, lambda r, c: relay_in(r, c).wait_send())

        def sent(semaphore, count):
            for n in range(1, grid_cols):

                @pl.when(count == n)
                def _():
                    line = row_h.at[pl.ds(0, n)]
                    pltpu.make_async_copy(line, line, semaphore).wait()

        told = jnp.where(origin, 2, jnp.maximum(row_end - to_row, 0))
        sent(h_send.at[my_row], told)
        sent(d_send, jnp.maximum(grid_cols - to_right, 0))
        far_told = grid_cols - 1 - my_col + jnp.where(second, 1, 0)
        far_low = jnp.where(direct_top, 1, grid_rows)
        span(far_low, grid_rows, lambda r: sent(h_send.at[r], far_told))

        @pl.when(second)
        def _():
            relay_back(0, 2).wait_send()

    with jax.named_scope("hear"):
        hear(row_h, row_recv, 3, jnp.where(has_above, 0, my_col - 3))
        hear(row_h, row_recv, 0, jnp.where(has_above, my_col, 0))
        hear(top_h, far_recv, 3, jnp.where(has_above, my_col - 3, 0))

        @pl.when(has_above & relays)
        def _():
            hear_one(col_h, link_recv.at[6])

        @pl.when(before_second)
        def _():
            hear_one(row_h.at[1], link_recv.at[5])

        @pl.when(has_above & has_left)
        def _():
            hear_one(left_d, link_recv.at[7])

    with jax.named_scope("finish"):

        def prefix(slots):
            line = slots[0]
            for k in range(1, grid_cols):
                line = line + slots[k]
            return line

        across_here = prefix(row_h)
        across_top = prefix(top_h) + jnp.where(relays, col_h[...], 0.0)
        across_top = jnp.where(has_above, across_top, across_here)
        down_here = mine_y[...]
        down_left = jnp.where(has_left & has_above, left_d[...], down_here)
        here = left = top = start = zero_line
        for sweep in range(ITERS):
            prefix_across = across_here + (left - here)
            prefix_across_top = across_top + (start - top)
            prefix_down = down_here + (top - here)
            prefix_down_left = down_left + (start - left)
            here = here + 0.5 * (prefix_across + prefix_across_top + prefix_down + prefix_down_left)
            left = left + prefix_down_left
            top = top + prefix_across_top
        offset[...] = jnp.broadcast_to(here, offset.shape)


def place_kernel(parts, integ, offset, out, ready):
    pl.run_scoped(
        functools.partial(place_rows, parts, integ, offset, out, ready),
        pltpu.SemaphoreType.DMA((parts,)),
    )


def place_rows(parts, integ, offset, out, ready, sems):
    step = integ.shape[0] // parts
    shift = offset[0:1, 0:1]
    copies = []
    for q in range(parts):
        rows = pl.ds(q * step, step)
        ready[rows, :] = integ[rows, :] + shift
        copy = pltpu.make_async_copy(ready.at[rows], out.at[rows], sems.at[q])
        copy.start()
        copies.append(copy)
    for copy in copies:
        copy.wait()


def on_device(names, sizes, wrapped, col_steps, row_steps):
    frames, tile_rows, tile_cols = wrapped.shape
    grid_rows, grid_cols = sizes
    down, right = tile_rows // LANES, tile_cols // LANES
    dma = pltpu.SemaphoreType.DMA
    rows_step = math.gcd(tile_rows, 256)
    cols_step = math.gcd(tile_cols, 256)
    f32 = jnp.float32

    def with_local_semaphores(*refs):
        pl.run_scoped(
            functools.partial(edge_kernel, names, sizes, rows_step, cols_step, *refs),
            dma((8,)), dma, dma, dma, dma,
            pltpu.SemaphoreType.REGULAR, pltpu.SemaphoreType.REGULAR, pltpu.SemaphoreType.REGULAR,
            dma((tile_rows // rows_step + 5,)), dma((5,)), dma((grid_rows,)), dma((grid_rows,)),
            dma((grid_rows,)), dma((grid_rows,)), dma, dma,
        )

    call = pl.pallas_call(
        with_local_semaphores,
        out_shape=(
            pltpu.VMEM((tile_rows, tile_cols), f32),
            pltpu.VMEM((8, LANES), f32),
        ),
        in_specs=[
            pl.BlockSpec(memory_space=pltpu.HBM),
            pl.BlockSpec(memory_space=pltpu.HBM),
            pl.BlockSpec(memory_space=pltpu.HBM),
        ],
        out_specs=(
            pl.BlockSpec(memory_space=pltpu.VMEM),
            pl.BlockSpec(memory_space=pltpu.VMEM),
        ),
        scratch_shapes=[
            pltpu.VMEM((tile_rows, tile_cols), f32),
            pltpu.VMEM((2 * down, LANES), f32),
            pltpu.VMEM((2 * down, LANES), f32),
            pltpu.VMEM((8, LANES), f32),
            pltpu.VMEM((8, LANES), f32),
            pltpu.VMEM((grid_rows, 2 * right, LANES), f32),
            pltpu.VMEM((3 * right, LANES), f32),
            pltpu.VMEM((grid_rows, 3 * right, LANES), f32),
            pltpu.VMEM((right, LANES), f32),
            pltpu.VMEM((tile_rows, tile_cols), jnp.bfloat16),
            pltpu.VMEM((tile_rows, LANES), jnp.bfloat16),
            pltpu.VMEM((1, 1, 1), jnp.int32),
            pltpu.VMEM((1, 1, 1), jnp.int32),
            pltpu.VMEM((3, 1, LANES), f32),
            pltpu.VMEM((1, LANES), f32),
            pltpu.VMEM((grid_cols, 1, LANES), f32),
            pltpu.VMEM((grid_cols, 1, LANES), f32),
            pltpu.VMEM((1, LANES), f32),
            pltpu.VMEM((1, LANES), f32),
            pltpu.VMEM((1, LANES), f32),
            pltpu.VMEM((3 * down, LANES), f32),
            pltpu.VMEM((3 * down, LANES), f32),
            pltpu.VMEM((2 * down, LANES), f32),
            pltpu.VMEM((1, LANES), f32),
            pltpu.VMEM((5, 1, LANES), f32),
        ],
        compiler_params=pltpu.CompilerParams(
            collective_id=0, has_side_effects=True, vmem_limit_bytes=57 * 1024 * 1024
        ),
    )
    parts = math.gcd(tile_rows // 8, 16)
    place = pl.pallas_call(
        functools.partial(place_kernel, parts),
        out_shape=jax.ShapeDtypeStruct((tile_rows, tile_cols), f32),
        in_specs=[pl.BlockSpec(memory_space=pltpu.VMEM), pl.BlockSpec(memory_space=pltpu.VMEM)],
        out_specs=pl.BlockSpec(memory_space=pltpu.HBM),
        scratch_shapes=[pltpu.VMEM((tile_rows, tile_cols), f32)],
        compiler_params=pltpu.CompilerParams(vmem_limit_bytes=24 * 1024 * 1024),
    )
    outs = [
        place(*call(wrapped[f : f + 1], col_steps[f : f + 1], row_steps[f : f + 1]))
        for f in range(frames)
    ]
    return jnp.stack(outs)


def solution(mesh):
    spec = P(None, "row", "col")
    sizes = (mesh.shape["row"], mesh.shape["col"])
    return jax.shard_map(
        functools.partial(on_device, ("row", "col"), sizes),
        mesh=mesh, in_specs=(spec, spec, spec), out_specs=spec, check_vma=False,
    )
```

```python
import functools
import math

import jax
import jax.numpy as jnp
from jax import lax
from jax.experimental import pallas as pl
from jax.experimental.pallas import tpu as pltpu
from jax.sharding import PartitionSpec as P

ITERS = 2
TWO_PI = 2.0 * math.pi
MESH = pl.DeviceIdType.MESH
LANES = 128
STRIP = 16


def cycles(change):
    return jnp.floor(change * (1.0 / TWO_PI) + 0.5)


def iota(shape, dim):
    return lax.broadcasted_iota(jnp.int32, shape, dim)


def total(values):
    return jnp.sum(values, axis=1, keepdims=True)


def previous(line, first):
    lane, row = iota(line.shape, 1), iota(line.shape, 0)
    along = pltpu.roll(line, 1, 1)
    across = pltpu.roll(along, 1, 0) if line.shape[0] > 1 else along
    return jnp.where(lane > 0, along, jnp.where(row > 0, across, first))


def summed(line):
    return total(jnp.sum(line, axis=0, keepdims=True))


def triangle(size, dim):
    ordered = iota((size, size), dim) <= iota((size, size), 1 - dim)
    return ordered.astype(jnp.float32).astype(jnp.bfloat16)


def line_counts(line):
    groups = line.shape[0]
    row = iota(line.shape, 0)
    floors = cycles(line - previous(line, line[0:1, 0:1]))
    whole, shift = floors, 1
    while shift < groups:
        whole = whole + jnp.where(row >= shift, pltpu.roll(whole, shift, 0), 0.0)
        shift *= 2
    pair = jnp.concatenate([floors, whole - floors], axis=1)
    pair = jnp.concatenate([pair] * (-(-16 // groups)), axis=0).astype(jnp.bfloat16)
    ones = jnp.ones((LANES, LANES), jnp.bfloat16)
    table = jnp.concatenate([triangle(LANES, 0), ones], axis=0)
    return jnp.dot(pair, table, preferred_element_type=jnp.float32)[0:groups, :]


def weights(inner, outer, inner_before, outer_before, at_image_edge):
    over = cycles(outer - inner)
    over_before = previous(over, cycles(outer_before - inner_before))
    along_outer = cycles(outer - previous(outer, outer_before))
    along_inner = cycles(inner - previous(inner, inner_before))
    charge = over_before + along_outer - over - along_inner
    start = (iota(charge.shape, 1) == 0) & (iota(charge.shape, 0) == 0)
    charge = jnp.where(start & at_image_edge, 0.0, charge)
    return 1.0 / (1.0 + jnp.abs(charge))


def mismatch(weight, outer, count, first, beyond):
    jump = beyond - count - cycles(first - outer)
    return summed(weight * jump) / summed(weight)


def edge_kernel(
    names, sizes, rows_step, cols_step,
    wrapped, col_steps, row_steps,
    integ, offset,
    cells, left_out, right_in, corner_above, corner_left, tops, bottom_out, bottoms, inner_row,
    floors, row_sums, steps_across, steps_down, mine_h, mine_y, row_h, top_h, col_h, left_d, carried, ends, ends_in, pair_in, first_inner, left_sums,
    link_recv, top_recv, bottom_recv, row_recv, far_recv, row_in, col_in, far_in,
    load_sem, link_send, top_send, bottom_send, h_send, c_send, d_send, back_send,
):
    row_name, col_name = names
    grid_rows, grid_cols = sizes
    tile_rows, tile_cols = cells.shape
    my_row, my_col = lax.axis_index(row_name), lax.axis_index(col_name)
    down, right = tile_rows // LANES, tile_cols // LANES

    chunks = tile_rows // rows_step
    rest = pl.ds(LANES, tile_cols - LANES)
    regions = [
        (pl.ds(0, tile_rows), pl.ds(0, LANES)),
        (pl.ds(tile_rows - 16, 16), rest),
        (pl.ds(0, 16), rest),
    ]
    for q in range(chunks):
        top = max(q * rows_step, 16)
        bottom = min((q + 1) * rows_step, tile_rows - 16)
        regions.append((pl.ds(top, bottom - top), rest))
    loads = []
    for k, (rows, cols) in enumerate(regions):
        loads.append(
            pltpu.make_async_copy(wrapped.at[0, rows, cols], cells.at[rows, cols], load_sem.at[k])
        )
    for source, target in ((col_steps, steps_across), (row_steps, steps_down)):
        loads.append(pltpu.make_async_copy(source, target, load_sem.at[len(loads)]))

    def start_loads():
        for load in loads:
            load.start()

    def span(low, high, act):
        def step(k, carry):
            act(k)
            return carry

        lax.fori_loop(low, high, step, 0)

    def along_row(low, high, act):
        span(low, high, lambda c: act(my_row, c))

    def along_col(low, high, act):
        span(low, high, lambda r: act(r, my_col))

    has_left, has_right = my_col > 0, my_col < grid_cols - 1
    has_above, has_below = my_row > 0, my_row < grid_rows - 1
    even_row = has_above & (lax.rem(my_row, 2) == 0)
    tail_col = my_col >= grid_cols - 2
    tail = tail_col & has_below & (lax.rem(my_row, 2) == 0)

    def unknown_to(row):
        return (row < my_row) & ((my_row - row > 2) | (tail_col & (lax.rem(row, 2) == 0)))

    unknown_above = sum(jnp.where(unknown_to(k), 1, 0) for k in range(grid_rows))
    near = jnp.where(tail, my_row + 1, jnp.minimum(my_row + 3, grid_rows))
    direct_top = (my_row == 0) & (my_col > 2)
    first_left = jnp.where(my_row == 0, 3, 0)
    lead = (my_row == 0) & (my_col < 3)
    pair = my_col == 1
    paired = (my_row == 0) & pair
    second = (my_row == 0) & (my_col == 3)
    before_second = (my_row == 0) & (my_col == 2)
    greets_left = has_left & (has_below | pair | second | before_second)
    knows_right = has_right & (has_below | (my_col == 0) | paired | before_second)

    def far_below(act):
        low = jnp.where(direct_top, 1, grid_rows)
        span(low, grid_rows, lambda r: span(my_col + 1, grid_cols, lambda c: act(r, c)))

    def left_below(act):
        span(jnp.where(second, 1, grid_rows), grid_rows, lambda r: act(r, my_col - 1))

    def direct_tops(act):
        span(3, jnp.where(has_above, my_col, 0), lambda c: act(0, c))

        @pl.when(has_above & (my_col == 2))
        def _():
            act(0, 3)

    zero_line = jnp.zeros((1, LANES), jnp.float32)
    barrier = pltpu.get_barrier_semaphore()

    def await_signals(semaphore, count):

        @pl.when(count > 0)
        def _():
            pl.semaphore_wait(semaphore, count)

    def greet(semaphore):
        return lambda r, c: pl.semaphore_signal(
            semaphore, inc=1, device_id=(r, c), device_id_type=MESH
        )

    origin = (my_row == 0) & (my_col == 0)

    def greet_above(semaphore, unknown):

        def greet_row(r, c):

            @pl.when(unknown_to(r) == unknown)
            def _():
                greet(semaphore)(r, c)

        along_col(0 if unknown else jnp.maximum(my_row - 2, 0), my_row, greet_row)

    for slots in (row_h, top_h):
        for k in range(grid_cols):
            slots[k] = zero_line

    greet_above(barrier, False)
    along_row(jnp.where(greets_left, my_col - 1, my_col), my_col, greet(barrier))
    start_loads()
    pair_top = (my_row == 0) & (my_col < 2)
    few = my_col + jnp.where(paired, 1, 2)
    along_row(my_col + 1, jnp.where(lead, few, grid_cols), greet(barrier))

    @pl.when(second)
    def _():
        greet(barrier)(0, 0)
        greet(barrier)(0, 1)

    along_col(jnp.where(tail, my_row + 1, my_row + 3), grid_rows, greet(barrier))
    far_below(greet(barrier))
    left_below(greet(barrier))

    def clear(ref, unless):

        @pl.when(jnp.logical_not(unless))
        def _():
            ref[...] = jnp.zeros(ref.shape, ref.dtype)

    clear(right_in, has_right)
    clear(corner_above, has_above)
    clear(corner_left, has_left & has_below)
    clear(mine_y, has_above)

    first = jnp.logical_not(has_below) | tail
    last = (my_row == 0) & (my_col < 2) & jnp.logical_not(first)
    between = jnp.logical_not(first | last)

    feeds = paired | before_second
    weighs_late = last | before_second

    def enter():
        top_sources = jnp.where(paired | second, 1, jnp.maximum(my_col - 3, 0))
        sources = jnp.where(my_row == 0, top_sources, my_col)
        sources = sources + jnp.where(pair_top, 1, 0)
        sources = sources + unknown_above
        sources = sources + jnp.where(has_above, jnp.maximum(my_col - 3, 0), 0)
        sources = sources + jnp.where(has_above & (my_col == 2), 1, 0)
        sources = sources + (near - 1 - my_row) + jnp.where(knows_right, 1, 0)
        await_signals(barrier, sources)

        @pl.when(jnp.logical_not(first | last))
        def _():
            push(0)
            push(4)

        along_row(first_left, jnp.where(greets_left, my_col - 1, my_col), greet(row_in))
        greet_above(col_in, True)
        direct_tops(greet(far_in))

    corner = cells.at[pl.ds(tile_rows - 8, 8), pl.ds(tile_cols - LANES, LANES)]
    links = (
        (left_out, right_in, 0, -1, has_left & jnp.logical_not(before_second), has_right & jnp.logical_not(paired)),
        (corner, corner_above, 1, 0, has_below, has_above),
        (corner, corner_left, 0, 1, has_right & has_below, has_left & has_below),
        (ends, ends_in, 0, 2, paired, second),
        (left_out, pair_in, 0, 1, before_second, second),
    )

    def link_copy(k):
        source, target, d_row, d_col, _, _ = links[k]
        place = (
            lax.rem(my_row + d_row + grid_rows, grid_rows),
            lax.rem(my_col + d_col + grid_cols, grid_cols),
        )
        return pltpu.make_async_remote_copy(
            src_ref=source, dst_ref=target, send_sem=link_send.at[k], recv_sem=link_recv.at[k],
            device_id=place, device_id_type=MESH,
        )

    def push(k):

        @pl.when(links[k][4])
        def _():
            link_copy(k).start()

    def arrived(k):

        @pl.when(links[k][5])
        def _():
            link_copy(k).wait_recv()

    def send(source, target, send_sem, recv_sem, place):
        return pltpu.make_async_remote_copy(
            src_ref=source, dst_ref=target, send_sem=send_sem, recv_sem=recv_sem,
            device_id=place, device_id_type=MESH,
        )

    def top_copy(r, c):
        line = tops.at[my_row]
        return send(line, line, top_send.at[r], top_recv, (r, c))

    def bottom_copy(r, c):
        return send(bottom_out, bottoms.at[my_row], bottom_send.at[r], bottom_recv, (r, c))

    def row_copy(r, c):
        return send(mine_h.at[1], row_h.at[my_col], h_send.at[r], row_recv, (r, c))

    def far_copy(r, c):
        return send(mine_h.at[1], top_h.at[my_col], h_send.at[r], far_recv, (r, c))

    def origin_copy(r, c):
        return send(mine_h.at[1], row_h.at[0], h_send.at[r], link_recv.at[5], (r, c))

    def relay_in(r, c):
        return send(mine_h.at[2], col_h, c_send.at[r], link_recv.at[6], (r, c))

    def relay_left(r, c):
        return send(mine_h.at[0], col_h, h_send.at[r], link_recv.at[6], (r, c))

    def relay_back(r, c):
        return send(mine_h.at[0], row_h.at[1], back_send, link_recv.at[5], (r, c))

    def left_copy(r, c):
        return send(mine_y, left_d, d_send, link_recv.at[7], (r, c))

    def push_tops(low, high, act):
        along_col(jnp.where(has_above, low, grid_rows), high, act)

    def push_bottoms():
        along_col(my_row + 1, near, lambda r, c: bottom_copy(r, c).start())

    def down_weights():
        outer_row = bottom_out[0:right, :]
        bottom_out[right : 2 * right, :] = weights(
            inner_row[...], outer_row,
            corner_left[6:7, LANES - 1 : LANES], corner_left[7:8, LANES - 1 : LANES],
            my_col == 0,
        )

    def push_down():
        pl.when(jnp.logical_not(tail))(lambda: push(1))
        push(2)

        @pl.when(has_below & jnp.logical_not(has_left))
        def _():
            push_bottoms()

    def row_line(row):
        return jnp.concatenate(
            [cells[row : row + 1, k * LANES : (k + 1) * LANES] for k in range(right)], axis=0
        )

    def col_lines(block, low, high):
        turned = [
            cells[k * LANES : (k + 1) * LANES, block * LANES : (block + 1) * LANES].T
            for k in range(down)
        ]
        return [jnp.concatenate([t[j : j + 1, :] for t in turned], axis=0) for j in range(low, high)]

    with jax.named_scope("enter_0"):
        pl.when(first)(enter)
    with jax.named_scope("load_head"):
        loads[0].wait()
    with jax.named_scope("head"):
        head_line = col_lines(0, 0, 1)[0]
        left_out[0:down, :] = head_line
        left_out[down:, :] = line_counts(head_line)
    with jax.named_scope("push_first"):

        @pl.when(first)
        def _():
            push(0)
            push(4)


    with jax.named_scope("load_edges"):
        loads[1].wait()
        loads[2].wait()
        loads[-1].wait()
        loads[-2].wait()
    with jax.named_scope("last_row"):
        outer_row = row_line(tile_rows - 1)
        down_count = left_out[2 * down - 1 :, LANES - 1 :] - steps_down[0].astype(jnp.float32)
        bottom_out[0:right, :] = outer_row
        bottom_out[2 * right :, :] = down_count + line_counts(outer_row)
        inner_row[...] = row_line(tile_rows - 2)

        @pl.when(jnp.logical_not(has_left))
        def _():
            down_weights()

    with jax.named_scope("enter_1"):
        pl.when(between)(enter)

        @pl.when(jnp.logical_not(last))
        def _():
            push_down()

    with jax.named_scope("first_row"):

        @pl.when(has_above)
        def _():
            first_row = row_line(0)
            tops[my_row, 0:right, :] = first_row
            tops[my_row, right:, :] = line_counts(first_row)

        push_tops(my_row + 1, near, lambda r, c: top_copy(r, c).start())

    lane = iota((STRIP, LANES), 1)

    def strip(k, carry):
        rows = pl.ds(pl.multiple_of(k * STRIP, STRIP), STRIP)
        wrapped_around = cells[rows, 0:LANES]
        sums = jnp.zeros((STRIP, LANES), jnp.float32)
        for j in range(right):
            cols = slice(j * LANES, (j + 1) * LANES)
            here = cells[rows, cols]
            rolled = pltpu.roll(here, 1, 1)
            across = cycles(here - jnp.where(lane == 0, wrapped_around, rolled))
            wrapped_around = rolled
            floors[rows, cols] = across.astype(jnp.bfloat16)
            sums = sums + across
        row_sums[rows, :] = sums.astype(jnp.bfloat16)
        return carry

    def weigh_bottom():
        arrived(2)
        down_weights()
        push_bottoms()

    def push_further_bottoms():
        along_col(near, grid_rows, lambda r, c: bottom_copy(r, c).start())

    def weigh_after():
        with jax.named_scope("weigh_after"):
            pl.when(has_below)(weigh_bottom)
            push_further_bottoms()

    def push_further_tops():
        await_signals(col_in, grid_rows - near)
        pl.when(tail)(lambda: push(1))
        push_tops(near, grid_rows, lambda r, c: top_copy(r, c).start())

    per_chunk = rows_step // STRIP
    for q in range(chunks):
        if q == chunks - 1:
            with jax.named_scope("tail_in"):
                pl.when(tail)(push_further_tops)
                pl.when(has_left & has_below & jnp.logical_not(weighs_late))(weigh_bottom)
        with jax.named_scope(f"load_{q}"):
            loads[q + 3].wait()
        with jax.named_scope(f"floors_{q}"):
            lax.fori_loop(
                q * per_chunk, (q + 1) * per_chunk, strip, 0, unroll=math.gcd(per_chunk, 16)
            )
        if q == (chunks - 1) // 2:
            with jax.named_scope("enter_2"):

                @pl.when(last)
                def _():
                    enter()
                    push(0)
                    push_down()

    with jax.named_scope("corner_left"):
        pl.when(has_left & has_below & weighs_late & jnp.logical_not(feeds))(weigh_bottom)

    with jax.named_scope("col_in"):
        pl.when(jnp.logical_not(tail))(push_further_tops)
        pl.when(jnp.logical_not(feeds))(push_further_bottoms)

    relays = (my_col > 0) & (my_col < 4)
    to_relay = jnp.where(paired | second, 1, grid_rows)
    left_side = has_above & jnp.logical_not(has_left)
    to_right = jnp.where(left_side, 1, grid_cols)
    to_row = jnp.where(pair_top, grid_cols, my_col + 1)
    row_end = jnp.where(before_second, 4, grid_cols)

    def pair_places(act):
        span(jnp.where(origin, 0, 2), 2, lambda k: act(0, 1 + 2 * k))

    def hear_one(ref, semaphore):
        pltpu.make_async_copy(ref, ref, semaphore).wait()

    def end_values():
        with jax.named_scope("ends"):
            ones = jnp.ones((16, LANES), jnp.bfloat16)
            pieces = []
            for k in range(down):
                sums = lax.dot_general(
                    ones, row_sums[k * LANES : (k + 1) * LANES, :], (((1,), (1,)), ((), ())),
                    preferred_element_type=jnp.float32,
                )
                pieces.append(sums[0:1, :])
            end_count = left_out[down:, :] + jnp.concatenate(pieces, axis=0)
            end_count = end_count - steps_across[0].astype(jnp.float32)
            return (end_count, *col_lines(right - 1, LANES - 2, LANES))

    def rest_weights(inner_col, outer_col):
        weight = weights(inner_col, outer_col, inner_col[0:1, 0:1], outer_col[0:1, 0:1], True)
        start = (iota(weight.shape, 0) == 0) & (iota(weight.shape, 1) == 0)
        return jnp.where(start & has_above, 0.0, weight)

    def first_weight(inner, outer):
        inner_before = corner_above[7:8, LANES - 2 : LANES - 1]
        outer_before = corner_above[7:8, LANES - 1 : LANES]
        charge = cycles(outer_before - inner_before) + cycles(outer - outer_before)
        charge = charge - cycles(outer - inner) - cycles(inner - inner_before)
        return jnp.where(has_above, 1.0 / (1.0 + jnp.abs(charge)), 0.0)

    def end_sums(weight, outer_col, end_count, first_col, first_count):
        jump = first_count - end_count - cycles(first_col - outer_col)
        return summed(weight * jump), summed(weight), jump[0:1, 0:1]

    def finish_mean(sums, inner, outer):
        jumps, weight, first_jump = sums
        extra = first_weight(inner, outer)
        return jnp.broadcast_to((jumps + extra * first_jump) / (weight + extra), (1, LANES))

    def across():
        end_count, inner_col, outer_col = end_values()
        with jax.named_scope("weights_h"):
            ends[0:down, :] = rest_weights(inner_col, outer_col)
            ends[down : 2 * down, :] = outer_col
            ends[2 * down :, :] = end_count
            first_inner[...] = inner_col[0:1, :]
            push(3)

        pl.when(paired)(weigh_after)

    def across_mean():
        with jax.named_scope("halo_0"):
            arrived(0)
        with jax.named_scope("base_h"):
            sums = end_sums(
                ends[0:down, :], ends[down : 2 * down, :], ends[2 * down :, :],
                right_in[0:down, :], right_in[down:, :],
            )
            arrived(1)
            mine_h[1] = finish_mean(sums, first_inner[0:1, 0:1], ends[down : down + 1, 0:1])
            pair_places(lambda r, c: origin_copy(r, c).start())

    def across_pair():
        with jax.named_scope("pair"):
            hear_one(row_h.at[0], link_recv.at[5])

            @pl.when(paired)
            def _():
                mine_h[2] = row_h[0]

            @pl.when(second)
            def _():
                arrived(4)
                hear_one(row_h.at[2], row_recv)
                arrived(3)
                jumps, weight, _ = end_sums(
                    ends_in[0:down, :], ends_in[down : 2 * down, :], ends_in[2 * down :, :],
                    pair_in[0:down, :], pair_in[down:, :],
                )
                before = jnp.broadcast_to(jumps / weight, (1, LANES))
                row_h[1] = before
                upto = row_h[0] + before
                mine_h[0] = upto
                mine_h[2] = upto + row_h[2]
                mine_h[1] = mine_h[1] + (upto + row_h[2])
                relay_back(0, 2).start()

            along_col(to_relay, grid_rows, lambda r, c: relay_in(r, c).start())

    def await_row():
        known = jnp.where(knows_right, my_col + 1, my_col)
        await_signals(row_in, jnp.where(lead, 0, grid_cols - 1 - known))

    def tell():
        with jax.named_scope("row_in"):
            await_row()
            along_row(to_row, row_end, lambda r, c: row_copy(r, c).start())

        pl.when(before_second)(weigh_after)

    def tell_far():
        with jax.named_scope("far_in"):
            right_count = grid_cols - 1 - my_col + jnp.where(second, 1, 0)
            await_signals(far_in, jnp.where(direct_top, (grid_rows - 1) * right_count, 0))
            left_below(lambda r, c: relay_left(r, c).start())
            far_below(lambda r, c: far_copy(r, c).start())

    def hear(slots, semaphore, first, count):
        for n in range(1, slots.shape[0] - max(first - 1, 0)):

            @pl.when(count == n)
            def _():
                landed = slots.at[pl.ds(first, n)]
                pltpu.make_async_copy(landed, landed, semaphore).wait()

    def hear_above():
        with jax.named_scope("hear_y"):
            hear(tops, top_recv, 1, my_row - 1)
            hear(bottoms, bottom_recv, 0, my_row)

    def sum_above():
        down_here = jnp.zeros((1, 1), jnp.float32)
        for k in range(grid_rows - 1):
            value = mismatch(
                bottoms[k, right : 2 * right, :], bottoms[k, 0:right, :],
                bottoms[k, 2 * right :, :], tops[k + 1, 0:right, :], tops[k + 1, right:, :],
            )
            down_here = down_here + jnp.where(k < my_row, value, 0.0)
        mine_y[...] = jnp.broadcast_to(down_here, mine_y.shape)

    def down_sum():
        hear_above()
        with jax.named_scope("base_y"):
            pl.when(has_above)(sum_above)

    def left_start():
        end_count, inner_col, outer_col = end_values()
        with jax.named_scope("halo_left"):
            arrived(0)
        with jax.named_scope("weights_left"):
            sums = end_sums(
                rest_weights(inner_col, outer_col), outer_col, end_count,
                right_in[0:down, :], right_in[down:, :],
            )
            for k, value in enumerate((*sums, inner_col[0:1, 0:1], outer_col[0:1, 0:1])):
                left_sums[k] = jnp.broadcast_to(value, (1, LANES))

    def left_finish():
        with jax.named_scope("halo_left_1"):
            arrived(1)
            jumps, weight, jump, inner, outer = (left_sums[k] for k in range(5))
            mine_h[1] = finish_mean((jumps, weight, jump), inner, outer)
        hear_above()
        with jax.named_scope("base_left"):
            sum_above()
        with jax.named_scope("row_in_left"):
            await_row()
            along_row(to_right, grid_cols, lambda r, c: left_copy(r, c).start())
            along_row(to_row, row_end, lambda r, c: row_copy(r, c).start())

    def integrate(low, high):
        with jax.named_scope(f"integrate_{low}"):
            upper, lower = triangle(cols_step, 0), triangle(rows_step, 1)
            down_carry = jnp.zeros((1, LANES), jnp.float32) if low == 0 else carried[...]
            for q in range(low, high):
                top = q * rows_step
                rows = pl.ds(top, rows_step)
                head = cells[rows, 0:LANES]
                above = cells[max(top - 1, 0) : max(top, 1), 0:LANES]
                before = jnp.where(iota(head.shape, 0) == 0, above, pltpu.roll(head, 1, 0))
                counts = down_carry + jnp.dot(
                    lower, cycles(head - before).astype(jnp.bfloat16),
                    preferred_element_type=jnp.float32,
                )
                down_carry = counts[rows_step - 1 : rows_step, :]
                carry = counts[:, 0:1]
                for b in range(tile_cols // cols_step):
                    cols = slice(b * cols_step, (b + 1) * cols_step)
                    count = carry + jnp.dot(
                        floors[rows, cols], upper, preferred_element_type=jnp.float32
                    )
                    carry = count[:, cols_step - 1 : cols_step]
                    integ[rows, cols] = cells[rows, cols] * (1.0 / TWO_PI) - count
            if high < chunks:
                carried[...] = down_carry

    odd_row = lax.rem(my_row, 2) == 1
    far_early = (my_row == 0) & (my_col > 3)
    split = (even_row & has_left) | (tail_col & odd_row)
    half = (chunks + 1) // 2
    never = 10
    at_left, at_top, at_pair, at_split, at_second, otherwise = range(6)
    kind = jnp.where(second, at_second, jnp.where(split, at_split, otherwise))
    kind = jnp.where(pair, jnp.where(paired, at_top, at_pair), kind)
    kind = jnp.where(left_side, at_left, kind)

    def pick(*slots):
        chosen = slots[otherwise]
        for k in range(otherwise):
            chosen = jnp.where(kind == k, slots[k], chosen)
        return chosen

    order = (
        (left_start, pick(0, never, never, never, never, never)),
        (left_finish, pick(2, never, never, never, never, never)),
        (across, jnp.where(has_right, pick(never, 0, 1, 1, 1, 0), never)),
        (across_mean, jnp.where(has_right, pick(never, never, 2, 2, 2, 1), never)),
        (across_pair, pick(never, 2, never, never, 3, never)),
        (tell, pick(never, never, 3, 3, 4, 2)),
        (functools.partial(integrate, 0, half), pick(1, 1, 0, 0, 0, jnp.where(far_early, 4, 3))),
        (tell_far, jnp.where(direct_top, jnp.where(second, 5, jnp.where(far_early, 3, 4)), never)),
        (functools.partial(integrate, half, chunks), pick(3, 3, 5, 4, 6, 5)),
        (down_sum, pick(never, never, 4, 5, never, 6)),
    )

    def phase(k, carry):
        for act, at in order:
            pl.when(k == at)(act)
        return carry

    lax.fori_loop(0, len(order), phase, 0)

    pl.when(jnp.logical_not(has_right | left_side))(lambda: arrived(1))

    with jax.named_scope("sent"):
        for k in range(5):

            @pl.when(links[k][4])
            def _():
                link_copy(k).wait_send()

        push_tops(my_row + 1, grid_rows, lambda r, c: top_copy(r, c).wait_send())
        along_col(my_row + 1, grid_rows, lambda r, c: bottom_copy(r, c).wait_send())
        along_col(to_relay, grid_rows, lambda r, c: relay_in(r, c).wait_send())

        def sent(semaphore, count):
            for n in range(1, grid_cols):

                @pl.when(count == n)
                def _():
                    line = row_h.at[pl.ds(0, n)]
                    pltpu.make_async_copy(line, line, semaphore).wait()

        told = jnp.where(origin, 2, jnp.maximum(row_end - to_row, 0))
        sent(h_send.at[my_row], told)
        sent(d_send, jnp.maximum(grid_cols - to_right, 0))
        far_told = grid_cols - 1 - my_col + jnp.where(second, 1, 0)
        far_low = jnp.where(direct_top, 1, grid_rows)
        span(far_low, grid_rows, lambda r: sent(h_send.at[r], far_told))

        @pl.when(second)
        def _():
            relay_back(0, 2).wait_send()

    with jax.named_scope("hear"):
        hear(row_h, row_recv, 3, jnp.where(has_above, 0, my_col - 3))
        hear(row_h, row_recv, 0, jnp.where(has_above, my_col, 0))
        hear(top_h, far_recv, 3, jnp.where(has_above, my_col - 3, 0))

        @pl.when(has_above & relays)
        def _():
            hear_one(col_h, link_recv.at[6])

        @pl.when(before_second)
        def _():
            hear_one(row_h.at[1], link_recv.at[5])

        @pl.when(has_above & has_left)
        def _():
            hear_one(left_d, link_recv.at[7])

    with jax.named_scope("finish"):

        def prefix(slots):
            line = slots[0]
            for k in range(1, grid_cols):
                line = line + slots[k]
            return line

        across_here = prefix(row_h)
        across_top = prefix(top_h) + jnp.where(relays, col_h[...], 0.0)
        across_top = jnp.where(has_above, across_top, across_here)
        down_here = mine_y[...]
        down_left = jnp.where(has_left & has_above, left_d[...], down_here)
        here = left = top = start = zero_line
        for sweep in range(ITERS):
            prefix_across = across_here + (left - here)
            prefix_across_top = across_top + (start - top)
            prefix_down = down_here + (top - here)
            prefix_down_left = down_left + (start - left)
            here = here + 0.5 * (prefix_across + prefix_across_top + prefix_down + prefix_down_left)
            left = left + prefix_down_left
            top = top + prefix_across_top
        offset[...] = jnp.broadcast_to(here, offset.shape)


def place_kernel(parts, integ, offset, out, ready):
    pl.run_scoped(
        functools.partial(place_rows, parts, integ, offset, out, ready),
        pltpu.SemaphoreType.DMA((parts,)),
    )


def place_rows(parts, integ, offset, out, ready, sems):
    step = integ.shape[0] // parts
    shift = offset[0:1, 0:1]
    copies = []
    for q in range(parts):
        rows = pl.ds(q * step, step)
        ready[rows, :] = integ[rows, :] + shift
        copy = pltpu.make_async_copy(ready.at[rows], out.at[rows], sems.at[q])
        copy.start()
        copies.append(copy)
    for copy in copies:
        copy.wait()


def on_device(names, sizes, wrapped, col_steps, row_steps):
    frames, tile_rows, tile_cols = wrapped.shape
    grid_rows, grid_cols = sizes
    down, right = tile_rows // LANES, tile_cols // LANES
    dma = pltpu.SemaphoreType.DMA
    rows_step = math.gcd(tile_rows, 256)
    cols_step = math.gcd(tile_cols, 256)
    f32 = jnp.float32

    def with_local_semaphores(*refs):
        pl.run_scoped(
            functools.partial(edge_kernel, names, sizes, rows_step, cols_step, *refs),
            dma((8,)), dma, dma, dma, dma,
            pltpu.SemaphoreType.REGULAR, pltpu.SemaphoreType.REGULAR, pltpu.SemaphoreType.REGULAR,
            dma((tile_rows // rows_step + 5,)), dma((5,)), dma((grid_rows,)), dma((grid_rows,)),
            dma((grid_rows,)), dma((grid_rows,)), dma, dma,
        )

    call = pl.pallas_call(
        with_local_semaphores,
        out_shape=(
            pltpu.VMEM((tile_rows, tile_cols), f32),
            pltpu.VMEM((8, LANES), f32),
        ),
        in_specs=[
            pl.BlockSpec(memory_space=pltpu.HBM),
            pl.BlockSpec(memory_space=pltpu.HBM),
            pl.BlockSpec(memory_space=pltpu.HBM),
        ],
        out_specs=(
            pl.BlockSpec(memory_space=pltpu.VMEM),
            pl.BlockSpec(memory_space=pltpu.VMEM),
        ),
        scratch_shapes=[
            pltpu.VMEM((tile_rows, tile_cols), f32),
            pltpu.VMEM((2 * down, LANES), f32),
            pltpu.VMEM((2 * down, LANES), f32),
            pltpu.VMEM((8, LANES), f32),
            pltpu.VMEM((8, LANES), f32),
            pltpu.VMEM((grid_rows, 2 * right, LANES), f32),
            pltpu.VMEM((3 * right, LANES), f32),
            pltpu.VMEM((grid_rows, 3 * right, LANES), f32),
            pltpu.VMEM((right, LANES), f32),
            pltpu.VMEM((tile_rows, tile_cols), jnp.bfloat16),
            pltpu.VMEM((tile_rows, LANES), jnp.bfloat16),
            pltpu.VMEM((1, 1, 1), jnp.int32),
            pltpu.VMEM((1, 1, 1), jnp.int32),
            pltpu.VMEM((3, 1, LANES), f32),
            pltpu.VMEM((1, LANES), f32),
            pltpu.VMEM((grid_cols, 1, LANES), f32),
            pltpu.VMEM((grid_cols, 1, LANES), f32),
            pltpu.VMEM((1, LANES), f32),
            pltpu.VMEM((1, LANES), f32),
            pltpu.VMEM((1, LANES), f32),
            pltpu.VMEM((3 * down, LANES), f32),
            pltpu.VMEM((3 * down, LANES), f32),
            pltpu.VMEM((2 * down, LANES), f32),
            pltpu.VMEM((1, LANES), f32),
            pltpu.VMEM((5, 1, LANES), f32),
        ],
        compiler_params=pltpu.CompilerParams(
            collective_id=0, has_side_effects=True, vmem_limit_bytes=57 * 1024 * 1024
        ),
    )
    parts = math.gcd(tile_rows // 8, 16)
    place = pl.pallas_call(
        functools.partial(place_kernel, parts),
        out_shape=jax.ShapeDtypeStruct((tile_rows, tile_cols), f32),
        in_specs=[pl.BlockSpec(memory_space=pltpu.VMEM), pl.BlockSpec(memory_space=pltpu.VMEM)],
        out_specs=pl.BlockSpec(memory_space=pltpu.HBM),
        scratch_shapes=[pltpu.VMEM((tile_rows, tile_cols), f32)],
        compiler_params=pltpu.CompilerParams(vmem_limit_bytes=24 * 1024 * 1024),
    )
    outs = [
        place(*call(wrapped[f : f + 1], col_steps[f : f + 1], row_steps[f : f + 1]))
        for f in range(frames)
    ]
    return jnp.stack(outs)


def solution(mesh):
    spec = P(None, "row", "col")
    sizes = (mesh.shape["row"], mesh.shape["col"])
    return jax.shard_map(
        functools.partial(on_device, ("row", "col"), sizes),
        mesh=mesh, in_specs=(spec, spec, spec), out_specs=spec, check_vma=False,
    )
```

```python
import functools
import math

import jax
import jax.numpy as jnp
from jax import lax
from jax.experimental import pallas as pl
from jax.experimental.pallas import tpu as pltpu
from jax.sharding import PartitionSpec as P

ITERS = 2
TWO_PI = 2.0 * math.pi
MESH = pl.DeviceIdType.MESH
LANES = 128
STRIP = 16


def cycles(change):
    return jnp.floor(change * (1.0 / TWO_PI) + 0.5)


def iota(shape, dim):
    return lax.broadcasted_iota(jnp.int32, shape, dim)


def total(values):
    return jnp.sum(values, axis=1, keepdims=True)


def previous(line, first):
    lane, row = iota(line.shape, 1), iota(line.shape, 0)
    along = pltpu.roll(line, 1, 1)
    across = pltpu.roll(along, 1, 0) if line.shape[0] > 1 else along
    return jnp.where(lane > 0, along, jnp.where(row > 0, across, first))


def summed(line):
    return total(jnp.sum(line, axis=0, keepdims=True))


def triangle(size, dim):
    ordered = iota((size, size), dim) <= iota((size, size), 1 - dim)
    return ordered.astype(jnp.float32).astype(jnp.bfloat16)


def line_counts(line):
    groups = line.shape[0]
    row = iota(line.shape, 0)
    floors = cycles(line - previous(line, line[0:1, 0:1]))
    whole, shift = floors, 1
    while shift < groups:
        whole = whole + jnp.where(row >= shift, pltpu.roll(whole, shift, 0), 0.0)
        shift *= 2
    pair = jnp.concatenate([floors, whole - floors], axis=1)
    pair = jnp.concatenate([pair] * (-(-16 // groups)), axis=0).astype(jnp.bfloat16)
    ones = jnp.ones((LANES, LANES), jnp.bfloat16)
    table = jnp.concatenate([triangle(LANES, 0), ones], axis=0)
    return jnp.dot(pair, table, preferred_element_type=jnp.float32)[0:groups, :]


def weights(inner, outer, inner_before, outer_before, at_image_edge):
    over = cycles(outer - inner)
    over_before = previous(over, cycles(outer_before - inner_before))
    along_outer = cycles(outer - previous(outer, outer_before))
    along_inner = cycles(inner - previous(inner, inner_before))
    charge = over_before + along_outer - over - along_inner
    start = (iota(charge.shape, 1) == 0) & (iota(charge.shape, 0) == 0)
    charge = jnp.where(start & at_image_edge, 0.0, charge)
    return 1.0 / (1.0 + jnp.abs(charge))


def mismatch(weight, outer, count, first, beyond):
    jump = beyond - count - cycles(first - outer)
    return summed(weight * jump) / summed(weight)


def edge_kernel(
    names, sizes, rows_step, cols_step,
    wrapped, col_steps, row_steps,
    integ, offset,
    cells, left_out, right_in, corner_above, corner_left, tops, bottom_out, bottoms, inner_row,
    floors, row_sums, steps_across, steps_down, mine_h, mine_y, row_h, top_h, col_h, left_d, carried, ends, ends_in, pair_in, first_inner, left_sums,
    link_recv, top_recv, bottom_recv, row_recv, far_recv, row_in, tail_in, col_in, far_in,
    load_sem, link_send, top_send, bottom_send, h_send, c_send, d_send, back_send,
):
    row_name, col_name = names
    grid_rows, grid_cols = sizes
    tile_rows, tile_cols = cells.shape
    my_row, my_col = lax.axis_index(row_name), lax.axis_index(col_name)
    down, right = tile_rows // LANES, tile_cols // LANES

    chunks = tile_rows // rows_step
    rest = pl.ds(LANES, tile_cols - LANES)
    regions = [
        (pl.ds(0, tile_rows), pl.ds(0, LANES)),
        (pl.ds(tile_rows - 16, 16), rest),
        (pl.ds(0, 16), rest),
    ]
    for q in range(chunks):
        top = max(q * rows_step, 16)
        bottom = min((q + 1) * rows_step, tile_rows - 16)
        regions.append((pl.ds(top, bottom - top), rest))
    loads = []
    for k, (rows, cols) in enumerate(regions):
        loads.append(
            pltpu.make_async_copy(wrapped.at[0, rows, cols], cells.at[rows, cols], load_sem.at[k])
        )
    for source, target in ((col_steps, steps_across), (row_steps, steps_down)):
        loads.append(pltpu.make_async_copy(source, target, load_sem.at[len(loads)]))

    def start_loads():
        for load in loads:
            load.start()

    def span(low, high, act):
        def step(k, carry):
            act(k)
            return carry

        lax.fori_loop(low, high, step, 0)

    def along_row(low, high, act):
        span(low, high, lambda c: act(my_row, c))

    def along_col(low, high, act):
        span(low, high, lambda r: act(r, my_col))

    has_left, has_right = my_col > 0, my_col < grid_cols - 1
    has_above, has_below = my_row > 0, my_row < grid_rows - 1
    even_row = has_above & (lax.rem(my_row, 2) == 0)
    tail_col = my_col >= grid_cols - 2
    tail = tail_col & has_below & (lax.rem(my_row, 2) == 0)

    def unknown_to(row):
        return (row < my_row) & ((my_row - row > 2) | (tail_col & (lax.rem(row, 2) == 0)))

    unknown_above = sum(jnp.where(unknown_to(k), 1, 0) for k in range(grid_rows))
    near = jnp.where(tail, my_row + 1, jnp.minimum(my_row + 3, grid_rows))
    direct_top = (my_row == 0) & (my_col > 2)
    first_left = jnp.where(my_row == 0, 3, 0)
    lead = (my_row == 0) & (my_col < 3)
    pair = my_col == 1
    paired = (my_row == 0) & pair
    second = (my_row == 0) & (my_col == 3)
    before_second = (my_row == 0) & (my_col == 2)
    greets_left = has_left & (has_below | pair | second | before_second)
    knows_right = has_right & (has_below | (my_col == 0) | paired | before_second)

    def far_below(act):
        low = jnp.where(direct_top, 1, grid_rows)
        span(low, grid_rows, lambda r: span(my_col + 1, grid_cols, lambda c: act(r, c)))

    def left_below(act):
        span(jnp.where(second, 1, grid_rows), grid_rows, lambda r: act(r, my_col - 1))

    def direct_tops(act):
        span(3, jnp.where(has_above, my_col, 0), lambda c: act(0, c))

        @pl.when(has_above & (my_col == 2))
        def _():
            act(0, 3)

    zero_line = jnp.zeros((1, LANES), jnp.float32)
    barrier = pltpu.get_barrier_semaphore()

    def await_signals(semaphore, count):

        @pl.when(count > 0)
        def _():
            pl.semaphore_wait(semaphore, count)

    def greet(semaphore):
        return lambda r, c: pl.semaphore_signal(
            semaphore, inc=1, device_id=(r, c), device_id_type=MESH
        )

    origin = (my_row == 0) & (my_col == 0)

    def greet_above(semaphore, unknown):

        def greet_row(r, c):

            @pl.when(unknown_to(r) == unknown)
            def _():
                greet(semaphore)(r, c)

        along_col(0 if unknown else jnp.maximum(my_row - 2, 0), my_row, greet_row)

    for slots in (row_h, top_h):
        for k in range(grid_cols):
            slots[k] = zero_line

    greet_above(barrier, False)
    along_row(jnp.where(greets_left, my_col - 1, my_col), my_col, greet(barrier))
    start_loads()
    pair_top = (my_row == 0) & (my_col < 2)
    few = my_col + jnp.where(paired, 1, 2)
    along_row(my_col + 1, jnp.where(lead, few, grid_cols), greet(barrier))

    @pl.when(second)
    def _():
        greet(barrier)(0, 0)
        greet(barrier)(0, 1)

    along_col(jnp.where(tail, my_row + 1, my_row + 3), grid_rows, greet(barrier))
    far_below(greet(barrier))
    left_below(greet(barrier))

    def clear(ref, unless):

        @pl.when(jnp.logical_not(unless))
        def _():
            ref[...] = jnp.zeros(ref.shape, ref.dtype)

    clear(right_in, has_right)
    clear(corner_above, has_above)
    clear(corner_left, has_left & has_below)
    clear(mine_y, has_above)

    first = jnp.logical_not(has_below) | tail
    last = (my_row == 0) & (my_col < 2) & jnp.logical_not(first)
    between = jnp.logical_not(first | last)

    feeds = paired | before_second
    weighs_late = last | before_second

    def enter():
        top_sources = jnp.where(paired | second, 1, jnp.maximum(my_col - 3, 0))
        sources = jnp.where(my_row == 0, top_sources, my_col)
        sources = sources + jnp.where(pair_top, 1, 0)
        sources = sources + unknown_above
        sources = sources + jnp.where(has_above, jnp.maximum(my_col - 3, 0), 0)
        sources = sources + jnp.where(has_above & (my_col == 2), 1, 0)
        sources = sources + (near - 1 - my_row) + jnp.where(knows_right, 1, 0)
        await_signals(barrier, sources)

        @pl.when(jnp.logical_not(first | last))
        def _():
            push(0)
            push(4)

        def greet_row(semaphore):
            along_row(first_left, jnp.where(greets_left, my_col - 1, my_col), greet(semaphore))

        pl.when(tail_col)(lambda: greet_row(tail_in))
        pl.when(jnp.logical_not(tail_col))(lambda: greet_row(row_in))
        greet_above(col_in, True)
        direct_tops(greet(far_in))

    corner = cells.at[pl.ds(tile_rows - 8, 8), pl.ds(tile_cols - LANES, LANES)]
    links = (
        (left_out, right_in, 0, -1, has_left & jnp.logical_not(before_second), has_right & jnp.logical_not(paired)),
        (corner, corner_above, 1, 0, has_below, has_above),
        (corner, corner_left, 0, 1, has_right & has_below, has_left & has_below),
        (ends, ends_in, 0, 2, paired, second),
        (left_out, pair_in, 0, 1, before_second, second),
    )

    def link_copy(k):
        source, target, d_row, d_col, _, _ = links[k]
        place = (
            lax.rem(my_row + d_row + grid_rows, grid_rows),
            lax.rem(my_col + d_col + grid_cols, grid_cols),
        )
        return pltpu.make_async_remote_copy(
            src_ref=source, dst_ref=target, send_sem=link_send.at[k], recv_sem=link_recv.at[k],
            device_id=place, device_id_type=MESH,
        )

    def push(k):

        @pl.when(links[k][4])
        def _():
            link_copy(k).start()

    def arrived(k):

        @pl.when(links[k][5])
        def _():
            link_copy(k).wait_recv()

    def send(source, target, send_sem, recv_sem, place):
        return pltpu.make_async_remote_copy(
            src_ref=source, dst_ref=target, send_sem=send_sem, recv_sem=recv_sem,
            device_id=place, device_id_type=MESH,
        )

    def top_copy(r, c):
        line = tops.at[my_row]
        return send(line, line, top_send.at[r], top_recv, (r, c))

    def bottom_copy(r, c):
        return send(bottom_out, bottoms.at[my_row], bottom_send.at[r], bottom_recv, (r, c))

    def row_copy(r, c):
        return send(mine_h.at[1], row_h.at[my_col], h_send.at[r], row_recv, (r, c))

    def far_copy(r, c):
        return send(mine_h.at[1], top_h.at[my_col], h_send.at[r], far_recv, (r, c))

    def origin_copy(r, c):
        return send(mine_h.at[1], row_h.at[0], h_send.at[r], link_recv.at[5], (r, c))

    def relay_in(r, c):
        return send(mine_h.at[2], col_h, c_send.at[r], link_recv.at[6], (r, c))

    def relay_left(r, c):
        return send(mine_h.at[0], col_h, h_send.at[r], link_recv.at[6], (r, c))

    def relay_back(r, c):
        return send(mine_h.at[0], row_h.at[1], back_send, link_recv.at[5], (r, c))

    def left_copy(r, c):
        return send(mine_y, left_d, d_send, link_recv.at[7], (r, c))

    def push_tops(low, high, act):
        along_col(jnp.where(has_above, low, grid_rows), high, act)

    def push_bottoms():
        along_col(my_row + 1, near, lambda r, c: bottom_copy(r, c).start())

    def down_weights():
        outer_row = bottom_out[0:right, :]
        bottom_out[right : 2 * right, :] = weights(
            inner_row[...], outer_row,
            corner_left[6:7, LANES - 1 : LANES], corner_left[7:8, LANES - 1 : LANES],
            my_col == 0,
        )

    def push_down():
        pl.when(jnp.logical_not(tail))(lambda: push(1))
        push(2)

        @pl.when(has_below & jnp.logical_not(has_left))
        def _():
            push_bottoms()

    def row_line(row):
        return jnp.concatenate(
            [cells[row : row + 1, k * LANES : (k + 1) * LANES] for k in range(right)], axis=0
        )

    def col_lines(block, low, high):
        turned = [
            cells[k * LANES : (k + 1) * LANES, block * LANES : (block + 1) * LANES].T
            for k in range(down)
        ]
        return [jnp.concatenate([t[j : j + 1, :] for t in turned], axis=0) for j in range(low, high)]

    with jax.named_scope("enter_0"):
        pl.when(first)(enter)
    with jax.named_scope("load_head"):
        loads[0].wait()
    with jax.named_scope("head"):
        head_line = col_lines(0, 0, 1)[0]
        left_out[0:down, :] = head_line
        left_out[down:, :] = line_counts(head_line)
    with jax.named_scope("push_first"):

        @pl.when(first)
        def _():
            push(0)
            push(4)


    with jax.named_scope("load_edges"):
        loads[1].wait()
        loads[2].wait()
        loads[-1].wait()
        loads[-2].wait()
    with jax.named_scope("last_row"):
        outer_row = row_line(tile_rows - 1)
        down_count = left_out[2 * down - 1 :, LANES - 1 :] - steps_down[0].astype(jnp.float32)
        bottom_out[0:right, :] = outer_row
        bottom_out[2 * right :, :] = down_count + line_counts(outer_row)
        inner_row[...] = row_line(tile_rows - 2)

        @pl.when(jnp.logical_not(has_left))
        def _():
            down_weights()

    with jax.named_scope("enter_1"):
        pl.when(between)(enter)

        @pl.when(jnp.logical_not(last))
        def _():
            push_down()

    with jax.named_scope("first_row"):

        @pl.when(has_above)
        def _():
            first_row = row_line(0)
            tops[my_row, 0:right, :] = first_row
            tops[my_row, right:, :] = line_counts(first_row)

        push_tops(my_row + 1, near, lambda r, c: top_copy(r, c).start())

    lane = iota((STRIP, LANES), 1)

    def strip(k, carry):
        rows = pl.ds(pl.multiple_of(k * STRIP, STRIP), STRIP)
        wrapped_around = cells[rows, 0:LANES]
        sums = jnp.zeros((STRIP, LANES), jnp.float32)
        for j in range(right):
            cols = slice(j * LANES, (j + 1) * LANES)
            here = cells[rows, cols]
            rolled = pltpu.roll(here, 1, 1)
            across = cycles(here - jnp.where(lane == 0, wrapped_around, rolled))
            wrapped_around = rolled
            floors[rows, cols] = across.astype(jnp.bfloat16)
            sums = sums + across
        row_sums[rows, :] = sums.astype(jnp.bfloat16)
        return carry

    def weigh_bottom():
        arrived(2)
        down_weights()
        push_bottoms()

    def push_further_bottoms():
        along_col(near, grid_rows, lambda r, c: bottom_copy(r, c).start())

    def weigh_after():
        with jax.named_scope("weigh_after"):
            pl.when(has_below)(weigh_bottom)
            push_further_bottoms()

    def push_further_tops():
        await_signals(col_in, grid_rows - near)
        pl.when(tail)(lambda: push(1))
        push_tops(near, grid_rows, lambda r, c: top_copy(r, c).start())

    per_chunk = rows_step // STRIP
    for q in range(chunks):
        if q == chunks - 1:
            with jax.named_scope("tail_in"):
                pl.when(tail)(push_further_tops)
                pl.when(has_left & has_below & jnp.logical_not(weighs_late))(weigh_bottom)
        with jax.named_scope(f"load_{q}"):
            loads[q + 3].wait()
        with jax.named_scope(f"floors_{q}"):
            lax.fori_loop(
                q * per_chunk, (q + 1) * per_chunk, strip, 0, unroll=math.gcd(per_chunk, 16)
            )
        if q == (chunks - 1) // 2:
            with jax.named_scope("enter_2"):

                @pl.when(last)
                def _():
                    enter()
                    push(0)
                    push_down()

    with jax.named_scope("corner_left"):
        pl.when(has_left & has_below & weighs_late & jnp.logical_not(feeds))(weigh_bottom)

    with jax.named_scope("col_in"):
        pl.when(jnp.logical_not(tail))(push_further_tops)
        pl.when(jnp.logical_not(feeds))(push_further_bottoms)

    relays = (my_col > 0) & (my_col < 4)
    to_relay = jnp.where(paired | second, 1, grid_rows)
    left_side = has_above & jnp.logical_not(has_left)
    to_right = jnp.where(left_side, 1, grid_cols)
    to_row = jnp.where(pair_top, grid_cols, my_col + 1)
    row_end = jnp.where(before_second, 4, grid_cols)

    def pair_places(act):
        span(jnp.where(origin, 0, 2), 2, lambda k: act(0, 1 + 2 * k))

    def hear_one(ref, semaphore):
        pltpu.make_async_copy(ref, ref, semaphore).wait()

    def end_values():
        with jax.named_scope("ends"):
            ones = jnp.ones((16, LANES), jnp.bfloat16)
            pieces = []
            for k in range(down):
                sums = lax.dot_general(
                    ones, row_sums[k * LANES : (k + 1) * LANES, :], (((1,), (1,)), ((), ())),
                    preferred_element_type=jnp.float32,
                )
                pieces.append(sums[0:1, :])
            end_count = left_out[down:, :] + jnp.concatenate(pieces, axis=0)
            end_count = end_count - steps_across[0].astype(jnp.float32)
            return (end_count, *col_lines(right - 1, LANES - 2, LANES))

    def rest_weights(inner_col, outer_col):
        weight = weights(inner_col, outer_col, inner_col[0:1, 0:1], outer_col[0:1, 0:1], True)
        start = (iota(weight.shape, 0) == 0) & (iota(weight.shape, 1) == 0)
        return jnp.where(start & has_above, 0.0, weight)

    def first_weight(inner, outer):
        inner_before = corner_above[7:8, LANES - 2 : LANES - 1]
        outer_before = corner_above[7:8, LANES - 1 : LANES]
        charge = cycles(outer_before - inner_before) + cycles(outer - outer_before)
        charge = charge - cycles(outer - inner) - cycles(inner - inner_before)
        return jnp.where(has_above, 1.0 / (1.0 + jnp.abs(charge)), 0.0)

    def end_sums(weight, outer_col, end_count, first_col, first_count):
        jump = first_count - end_count - cycles(first_col - outer_col)
        return summed(weight * jump), summed(weight), jump[0:1, 0:1]

    def finish_mean(sums, inner, outer):
        jumps, weight, first_jump = sums
        extra = first_weight(inner, outer)
        return jnp.broadcast_to((jumps + extra * first_jump) / (weight + extra), (1, LANES))

    def across():
        end_count, inner_col, outer_col = end_values()
        with jax.named_scope("weights_h"):
            ends[0:down, :] = rest_weights(inner_col, outer_col)
            ends[down : 2 * down, :] = outer_col
            ends[2 * down :, :] = end_count
            first_inner[...] = inner_col[0:1, :]
            push(3)

        pl.when(paired)(weigh_after)

    def across_mean():
        with jax.named_scope("halo_0"):
            arrived(0)
        with jax.named_scope("base_h"):
            sums = end_sums(
                ends[0:down, :], ends[down : 2 * down, :], ends[2 * down :, :],
                right_in[0:down, :], right_in[down:, :],
            )
            arrived(1)
            mine_h[1] = finish_mean(sums, first_inner[0:1, 0:1], ends[down : down + 1, 0:1])
            pair_places(lambda r, c: origin_copy(r, c).start())

    def across_pair():
        with jax.named_scope("pair"):
            hear_one(row_h.at[0], link_recv.at[5])

            @pl.when(paired)
            def _():
                mine_h[2] = row_h[0]

            @pl.when(second)
            def _():
                arrived(4)
                hear_one(row_h.at[2], row_recv)
                arrived(3)
                jumps, weight, _ = end_sums(
                    ends_in[0:down, :], ends_in[down : 2 * down, :], ends_in[2 * down :, :],
                    pair_in[0:down, :], pair_in[down:, :],
                )
                before = jnp.broadcast_to(jumps / weight, (1, LANES))
                row_h[1] = before
                upto = row_h[0] + before
                mine_h[0] = upto
                mine_h[2] = upto + row_h[2]
                mine_h[1] = mine_h[1] + (upto + row_h[2])
                relay_back(0, 2).start()

            along_col(to_relay, grid_rows, lambda r, c: relay_in(r, c).start())

    inner_cols = grid_cols - 2
    known = jnp.where(knows_right, my_col + 1, my_col)
    inner_unknown = jnp.where(lead, 0, jnp.maximum(inner_cols - 1 - known, 0))
    tail_unknown = jnp.where(lead, 0, grid_cols - 1 - known - inner_unknown)

    def tell_inner():
        await_signals(row_in, inner_unknown)
        along_row(to_right, inner_cols, lambda r, c: left_copy(r, c).start())
        along_row(to_row, jnp.minimum(row_end, inner_cols), lambda r, c: row_copy(r, c).start())

    def tell_tail():
        with jax.named_scope("tail_tell"):
            await_signals(tail_in, tail_unknown)
            along_row(
                jnp.maximum(to_right, inner_cols), grid_cols, lambda r, c: left_copy(r, c).start()
            )
            along_row(
                jnp.maximum(to_row, inner_cols), row_end, lambda r, c: row_copy(r, c).start()
            )

    def tell():
        with jax.named_scope("row_in"):
            tell_inner()
            tell_tail()

        pl.when(before_second)(weigh_after)

    def tell_far():
        with jax.named_scope("far_in"):
            right_count = grid_cols - 1 - my_col + jnp.where(second, 1, 0)
            await_signals(far_in, jnp.where(direct_top, (grid_rows - 1) * right_count, 0))
            left_below(lambda r, c: relay_left(r, c).start())
            far_below(lambda r, c: far_copy(r, c).start())

    def hear(slots, semaphore, first, count):
        for n in range(1, slots.shape[0] - max(first - 1, 0)):

            @pl.when(count == n)
            def _():
                landed = slots.at[pl.ds(first, n)]
                pltpu.make_async_copy(landed, landed, semaphore).wait()

    def hear_above():
        with jax.named_scope("hear_y"):
            hear(tops, top_recv, 1, my_row - 1)
            hear(bottoms, bottom_recv, 0, my_row)

    def sum_above():
        down_here = jnp.zeros((1, 1), jnp.float32)
        for k in range(grid_rows - 1):
            value = mismatch(
                bottoms[k, right : 2 * right, :], bottoms[k, 0:right, :],
                bottoms[k, 2 * right :, :], tops[k + 1, 0:right, :], tops[k + 1, right:, :],
            )
            down_here = down_here + jnp.where(k < my_row, value, 0.0)
        mine_y[...] = jnp.broadcast_to(down_here, mine_y.shape)

    def down_sum():
        hear_above()
        with jax.named_scope("base_y"):
            pl.when(has_above)(sum_above)

    def left_start():
        end_count, inner_col, outer_col = end_values()
        with jax.named_scope("halo_left"):
            arrived(0)
        with jax.named_scope("weights_left"):
            sums = end_sums(
                rest_weights(inner_col, outer_col), outer_col, end_count,
                right_in[0:down, :], right_in[down:, :],
            )
            for k, value in enumerate((*sums, inner_col[0:1, 0:1], outer_col[0:1, 0:1])):
                left_sums[k] = jnp.broadcast_to(value, (1, LANES))

    def left_finish():
        with jax.named_scope("halo_left_1"):
            arrived(1)
            jumps, weight, jump, inner, outer = (left_sums[k] for k in range(5))
            mine_h[1] = finish_mean((jumps, weight, jump), inner, outer)
        hear_above()
        with jax.named_scope("base_left"):
            sum_above()
        with jax.named_scope("row_in_left"):
            tell_inner()

    def integrate(low, high):
        with jax.named_scope(f"integrate_{low}"):
            upper, lower = triangle(cols_step, 0), triangle(rows_step, 1)
            down_carry = jnp.zeros((1, LANES), jnp.float32) if low == 0 else carried[...]
            for q in range(low, high):
                top = q * rows_step
                rows = pl.ds(top, rows_step)
                head = cells[rows, 0:LANES]
                above = cells[max(top - 1, 0) : max(top, 1), 0:LANES]
                before = jnp.where(iota(head.shape, 0) == 0, above, pltpu.roll(head, 1, 0))
                counts = down_carry + jnp.dot(
                    lower, cycles(head - before).astype(jnp.bfloat16),
                    preferred_element_type=jnp.float32,
                )
                down_carry = counts[rows_step - 1 : rows_step, :]
                carry = counts[:, 0:1]
                for b in range(tile_cols // cols_step):
                    cols = slice(b * cols_step, (b + 1) * cols_step)
                    count = carry + jnp.dot(
                        floors[rows, cols], upper, preferred_element_type=jnp.float32
                    )
                    carry = count[:, cols_step - 1 : cols_step]
                    integ[rows, cols] = cells[rows, cols] * (1.0 / TWO_PI) - count
            if high < chunks:
                carried[...] = down_carry

    odd_row = lax.rem(my_row, 2) == 1
    far_early = (my_row == 0) & (my_col > 3)
    split = (even_row & has_left) | (tail_col & odd_row) | (lax.rem(my_col, 2) == 1)
    half = (chunks + 1) // 2
    never = 11
    at_left, at_top, at_pair, at_split, at_second, otherwise = range(6)
    kind = jnp.where(second, at_second, jnp.where(split, at_split, otherwise))
    kind = jnp.where(pair, jnp.where(paired, at_top, at_pair), kind)
    kind = jnp.where(left_side, at_left, kind)

    def pick(*slots):
        chosen = slots[otherwise]
        for k in range(otherwise):
            chosen = jnp.where(kind == k, slots[k], chosen)
        return chosen

    order = (
        (left_start, pick(0, never, never, never, never, never)),
        (left_finish, pick(jnp.where(my_row == 1, 1, 2), never, never, never, never, never)),
        (tell_tail, pick(3, never, never, never, never, never)),
        (across, jnp.where(has_right, pick(never, 0, 1, 1, 1, 0), never)),
        (across_mean, jnp.where(has_right, pick(never, never, 2, 2, 2, 1), never)),
        (across_pair, pick(never, 2, never, never, 3, never)),
        (tell, pick(never, never, 3, 3, 4, 2)),
        (functools.partial(integrate, 0, half), pick(jnp.where(my_row == 1, 2, 1), 1, 0, 0, 0, jnp.where(far_early, 4, 3))),
        (tell_far, jnp.where(direct_top, jnp.where(second, 5, jnp.where(far_early, 3, 4)), never)),
        (functools.partial(integrate, half, chunks), pick(4, 3, 5, 4, 6, 5)),
        (down_sum, pick(never, never, 4, 5, never, 6)),
    )

    def phase(k, carry):
        for act, at in order:
            pl.when(k == at)(act)
        return carry

    lax.fori_loop(0, len(order), phase, 0)

    pl.when(jnp.logical_not(has_right | left_side))(lambda: arrived(1))

    with jax.named_scope("sent"):
        for k in range(5):

            @pl.when(links[k][4])
            def _():
                link_copy(k).wait_send()

        push_tops(my_row + 1, grid_rows, lambda r, c: top_copy(r, c).wait_send())
        along_col(my_row + 1, grid_rows, lambda r, c: bottom_copy(r, c).wait_send())
        along_col(to_relay, grid_rows, lambda r, c: relay_in(r, c).wait_send())

        def sent(semaphore, count):
            for n in range(1, grid_cols):

                @pl.when(count == n)
                def _():
                    line = row_h.at[pl.ds(0, n)]
                    pltpu.make_async_copy(line, line, semaphore).wait()

        told = jnp.where(origin, 2, jnp.maximum(row_end - to_row, 0))
        sent(h_send.at[my_row], told)
        sent(d_send, jnp.maximum(grid_cols - to_right, 0))
        far_told = grid_cols - 1 - my_col + jnp.where(second, 1, 0)
        far_low = jnp.where(direct_top, 1, grid_rows)
        span(far_low, grid_rows, lambda r: sent(h_send.at[r], far_told))

        @pl.when(second)
        def _():
            relay_back(0, 2).wait_send()

    with jax.named_scope("hear"):
        hear(row_h, row_recv, 3, jnp.where(has_above, 0, my_col - 3))
        hear(row_h, row_recv, 0, jnp.where(has_above, my_col, 0))
        hear(top_h, far_recv, 3, jnp.where(has_above, my_col - 3, 0))

        @pl.when(has_above & relays)
        def _():
            hear_one(col_h, link_recv.at[6])

        @pl.when(before_second)
        def _():
            hear_one(row_h.at[1], link_recv.at[5])

        @pl.when(has_above & has_left)
        def _():
            hear_one(left_d, link_recv.at[7])

    with jax.named_scope("finish"):

        def prefix(slots):
            line = slots[0]
            for k in range(1, grid_cols):
                line = line + slots[k]
            return line

        across_here = prefix(row_h)
        across_top = prefix(top_h) + jnp.where(relays, col_h[...], 0.0)
        across_top = jnp.where(has_above, across_top, across_here)
        down_here = mine_y[...]
        down_left = jnp.where(has_left & has_above, left_d[...], down_here)
        here = left = top = start = zero_line
        for sweep in range(ITERS):
            prefix_across = across_here + (left - here)
            prefix_across_top = across_top + (start - top)
            prefix_down = down_here + (top - here)
            prefix_down_left = down_left + (start - left)
            here = here + 0.5 * (prefix_across + prefix_across_top + prefix_down + prefix_down_left)
            left = left + prefix_down_left
            top = top + prefix_across_top
        offset[...] = jnp.broadcast_to(here, offset.shape)


def place_kernel(parts, integ, offset, out, ready):
    pl.run_scoped(
        functools.partial(place_rows, parts, integ, offset, out, ready),
        pltpu.SemaphoreType.DMA((parts,)),
    )


def place_rows(parts, integ, offset, out, ready, sems):
    step = integ.shape[0] // parts
    shift = offset[0:1, 0:1]
    copies = []
    for q in range(parts):
        rows = pl.ds(q * step, step)
        ready[rows, :] = integ[rows, :] + shift
        copy = pltpu.make_async_copy(ready.at[rows], out.at[rows], sems.at[q])
        copy.start()
        copies.append(copy)
    for copy in copies:
        copy.wait()


def on_device(names, sizes, wrapped, col_steps, row_steps):
    frames, tile_rows, tile_cols = wrapped.shape
    grid_rows, grid_cols = sizes
    down, right = tile_rows // LANES, tile_cols // LANES
    dma = pltpu.SemaphoreType.DMA
    rows_step = math.gcd(tile_rows, 256)
    cols_step = math.gcd(tile_cols, 256)
    f32 = jnp.float32

    def with_local_semaphores(*refs):
        pl.run_scoped(
            functools.partial(edge_kernel, names, sizes, rows_step, cols_step, *refs),
            dma((8,)), dma, dma, dma, dma,
            *[pltpu.SemaphoreType.REGULAR] * 4,
            dma((tile_rows // rows_step + 5,)), dma((5,)), dma((grid_rows,)), dma((grid_rows,)),
            dma((grid_rows,)), dma((grid_rows,)), dma, dma,
        )

    call = pl.pallas_call(
        with_local_semaphores,
        out_shape=(
            pltpu.VMEM((tile_rows, tile_cols), f32),
            pltpu.VMEM((8, LANES), f32),
        ),
        in_specs=[
            pl.BlockSpec(memory_space=pltpu.HBM),
            pl.BlockSpec(memory_space=pltpu.HBM),
            pl.BlockSpec(memory_space=pltpu.HBM),
        ],
        out_specs=(
            pl.BlockSpec(memory_space=pltpu.VMEM),
            pl.BlockSpec(memory_space=pltpu.VMEM),
        ),
        scratch_shapes=[
            pltpu.VMEM((tile_rows, tile_cols), f32),
            pltpu.VMEM((2 * down, LANES), f32),
            pltpu.VMEM((2 * down, LANES), f32),
            pltpu.VMEM((8, LANES), f32),
            pltpu.VMEM((8, LANES), f32),
            pltpu.VMEM((grid_rows, 2 * right, LANES), f32),
            pltpu.VMEM((3 * right, LANES), f32),
            pltpu.VMEM((grid_rows, 3 * right, LANES), f32),
            pltpu.VMEM((right, LANES), f32),
            pltpu.VMEM((tile_rows, tile_cols), jnp.bfloat16),
            pltpu.VMEM((tile_rows, LANES), jnp.bfloat16),
            pltpu.VMEM((1, 1, 1), jnp.int32),
            pltpu.VMEM((1, 1, 1), jnp.int32),
            pltpu.VMEM((3, 1, LANES), f32),
            pltpu.VMEM((1, LANES), f32),
            pltpu.VMEM((grid_cols, 1, LANES), f32),
            pltpu.VMEM((grid_cols, 1, LANES), f32),
            pltpu.VMEM((1, LANES), f32),
            pltpu.VMEM((1, LANES), f32),
            pltpu.VMEM((1, LANES), f32),
            pltpu.VMEM((3 * down, LANES), f32),
            pltpu.VMEM((3 * down, LANES), f32),
            pltpu.VMEM((2 * down, LANES), f32),
            pltpu.VMEM((1, LANES), f32),
            pltpu.VMEM((5, 1, LANES), f32),
        ],
        compiler_params=pltpu.CompilerParams(
            collective_id=0, has_side_effects=True, vmem_limit_bytes=57 * 1024 * 1024
        ),
    )
    parts = math.gcd(tile_rows // 8, 16)
    place = pl.pallas_call(
        functools.partial(place_kernel, parts),
        out_shape=jax.ShapeDtypeStruct((tile_rows, tile_cols), f32),
        in_specs=[pl.BlockSpec(memory_space=pltpu.VMEM), pl.BlockSpec(memory_space=pltpu.VMEM)],
        out_specs=pl.BlockSpec(memory_space=pltpu.HBM),
        scratch_shapes=[pltpu.VMEM((tile_rows, tile_cols), f32)],
        compiler_params=pltpu.CompilerParams(vmem_limit_bytes=24 * 1024 * 1024),
    )
    outs = [
        place(*call(wrapped[f : f + 1], col_steps[f : f + 1], row_steps[f : f + 1]))
        for f in range(frames)
    ]
    return jnp.stack(outs)


def solution(mesh):
    spec = P(None, "row", "col")
    sizes = (mesh.shape["row"], mesh.shape["col"])
    return jax.shard_map(
        functools.partial(on_device, ("row", "col"), sizes),
        mesh=mesh, in_specs=(spec, spec, spec), out_specs=spec, check_vma=False,
    )
```

```python
import functools
import math

import jax
import jax.numpy as jnp
from jax import lax
from jax.experimental import pallas as pl
from jax.experimental.pallas import tpu as pltpu
from jax.sharding import PartitionSpec as P

ITERS = 2
TWO_PI = 2.0 * math.pi
MESH = pl.DeviceIdType.MESH
LANES = 128
STRIP = 16


def cycles(change):
    return jnp.floor(change * (1.0 / TWO_PI) + 0.5)


def iota(shape, dim):
    return lax.broadcasted_iota(jnp.int32, shape, dim)


def total(values):
    return jnp.sum(values, axis=1, keepdims=True)


def previous(line, first):
    lane, row = iota(line.shape, 1), iota(line.shape, 0)
    along = pltpu.roll(line, 1, 1)
    across = pltpu.roll(along, 1, 0) if line.shape[0] > 1 else along
    return jnp.where(lane > 0, along, jnp.where(row > 0, across, first))


def summed(line):
    return total(jnp.sum(line, axis=0, keepdims=True))


def triangle(size, dim):
    ordered = iota((size, size), dim) <= iota((size, size), 1 - dim)
    return ordered.astype(jnp.float32).astype(jnp.bfloat16)


def line_counts(line):
    groups = line.shape[0]
    row = iota(line.shape, 0)
    floors = cycles(line - previous(line, line[0:1, 0:1]))
    whole, shift = floors, 1
    while shift < groups:
        whole = whole + jnp.where(row >= shift, pltpu.roll(whole, shift, 0), 0.0)
        shift *= 2
    pair = jnp.concatenate([floors, whole - floors], axis=1)
    pair = jnp.concatenate([pair] * (-(-16 // groups)), axis=0).astype(jnp.bfloat16)
    ones = jnp.ones((LANES, LANES), jnp.bfloat16)
    table = jnp.concatenate([triangle(LANES, 0), ones], axis=0)
    return jnp.dot(pair, table, preferred_element_type=jnp.float32)[0:groups, :]


def weights(inner, outer, inner_before, outer_before, at_image_edge):
    over = cycles(outer - inner)
    over_before = previous(over, cycles(outer_before - inner_before))
    along_outer = cycles(outer - previous(outer, outer_before))
    along_inner = cycles(inner - previous(inner, inner_before))
    charge = over_before + along_outer - over - along_inner
    start = (iota(charge.shape, 1) == 0) & (iota(charge.shape, 0) == 0)
    charge = jnp.where(start & at_image_edge, 0.0, charge)
    return 1.0 / (1.0 + jnp.abs(charge))


def mismatch(weight, outer, count, first, beyond):
    jump = beyond - count - cycles(first - outer)
    return summed(weight * jump) / summed(weight)


def edge_kernel(
    names, sizes, rows_step, cols_step,
    wrapped, col_steps, row_steps,
    integ, offset,
    cells, left_out, right_in, corner_above, corner_left, tops, bottom_out, bottoms, inner_row,
    floors, row_sums, steps_across, steps_down, mine_h, mine_y, row_h, top_h, col_h, left_d, carried, ends, ends_in, pair_in, first_inner, left_sums,
    link_recv, top_recv, bottom_recv, row_recv, far_recv, row_in, tail_in, col_in, far_in,
    load_sem, link_send, top_send, bottom_send, h_send, c_send, d_send, back_send,
):
    row_name, col_name = names
    grid_rows, grid_cols = sizes
    tile_rows, tile_cols = cells.shape
    my_row, my_col = lax.axis_index(row_name), lax.axis_index(col_name)
    down, right = tile_rows // LANES, tile_cols // LANES

    chunks = tile_rows // rows_step
    rest = pl.ds(LANES, tile_cols - LANES)
    regions = [
        (pl.ds(0, tile_rows), pl.ds(0, LANES)),
        (pl.ds(tile_rows - 16, 16), rest),
        (pl.ds(0, 16), rest),
    ]
    for q in range(chunks):
        top = max(q * rows_step, 16)
        bottom = min((q + 1) * rows_step, tile_rows - 16)
        regions.append((pl.ds(top, bottom - top), rest))
    loads = []
    for k, (rows, cols) in enumerate(regions):
        loads.append(
            pltpu.make_async_copy(wrapped.at[0, rows, cols], cells.at[rows, cols], load_sem.at[k])
        )
    for source, target in ((col_steps, steps_across), (row_steps, steps_down)):
        loads.append(pltpu.make_async_copy(source, target, load_sem.at[len(loads)]))

    def start_loads():
        for load in loads:
            load.start()

    def span(low, high, act):
        def step(k, carry):
            act(k)
            return carry

        lax.fori_loop(low, high, step, 0)

    def along_row(low, high, act):
        span(low, high, lambda c: act(my_row, c))

    def along_col(low, high, act):
        span(low, high, lambda r: act(r, my_col))

    has_left, has_right = my_col > 0, my_col < grid_cols - 1
    has_above, has_below = my_row > 0, my_row < grid_rows - 1
    even_row = has_above & (lax.rem(my_row, 2) == 0)
    tail_col = my_col >= grid_cols - 2
    tail = tail_col & has_below & (lax.rem(my_row, 2) == 0)

    def unknown_to(row):
        return (row < my_row) & ((my_row - row > 2) | (tail_col & (lax.rem(row, 2) == 0)))

    unknown_above = sum(jnp.where(unknown_to(k), 1, 0) for k in range(grid_rows))
    near = jnp.where(tail, my_row + 1, jnp.minimum(my_row + 3, grid_rows))
    direct_top = (my_row == 0) & (my_col > 2)
    first_left = jnp.where(my_row == 0, 3, 0)
    lead = (my_row == 0) & (my_col < 3)
    pair = my_col == 1
    paired = (my_row == 0) & pair
    second = (my_row == 0) & (my_col == 3)
    before_second = (my_row == 0) & (my_col == 2)
    greets_left = has_left & (has_below | pair | second | before_second)
    knows_right = has_right & (has_below | (my_col == 0) | paired | before_second)

    def far_below(act):
        low = jnp.where(direct_top, 1, grid_rows)
        span(low, grid_rows, lambda r: span(my_col + 1, grid_cols, lambda c: act(r, c)))

    def left_below(act):
        span(jnp.where(second, 1, grid_rows), grid_rows, lambda r: act(r, my_col - 1))

    def direct_tops(act):
        span(3, jnp.where(has_above, my_col, 0), lambda c: act(0, c))

        @pl.when(has_above & (my_col == 2))
        def _():
            act(0, 3)

    zero_line = jnp.zeros((1, LANES), jnp.float32)
    barrier = pltpu.get_barrier_semaphore()

    def await_signals(semaphore, count):

        @pl.when(count > 0)
        def _():
            pl.semaphore_wait(semaphore, count)

    def greet(semaphore):
        return lambda r, c: pl.semaphore_signal(
            semaphore, inc=1, device_id=(r, c), device_id_type=MESH
        )

    origin = (my_row == 0) & (my_col == 0)

    def greet_above(semaphore, unknown):

        def greet_row(r, c):

            @pl.when(unknown_to(r) == unknown)
            def _():
                greet(semaphore)(r, c)

        along_col(0 if unknown else jnp.maximum(my_row - 2, 0), my_row, greet_row)

    for slots in (row_h, top_h):
        for k in range(grid_cols):
            slots[k] = zero_line

    greet_above(barrier, False)
    along_row(jnp.where(greets_left, my_col - 1, my_col), my_col, greet(barrier))
    start_loads()
    pair_top = (my_row == 0) & (my_col < 2)
    few = my_col + jnp.where(paired, 1, 2)
    along_row(my_col + 1, jnp.where(lead, few, grid_cols), greet(barrier))

    @pl.when(second)
    def _():
        greet(barrier)(0, 0)
        greet(barrier)(0, 1)

    along_col(jnp.where(tail, my_row + 1, my_row + 3), grid_rows, greet(barrier))
    far_below(greet(barrier))
    left_below(greet(barrier))

    def clear(ref, unless):

        @pl.when(jnp.logical_not(unless))
        def _():
            ref[...] = jnp.zeros(ref.shape, ref.dtype)

    clear(right_in, has_right)
    clear(corner_above, has_above)
    clear(corner_left, has_left & has_below)
    clear(mine_y, has_above)

    first = jnp.logical_not(has_below) | tail
    last = (my_row == 0) & (my_col < 2) & jnp.logical_not(first)
    between = jnp.logical_not(first | last)

    feeds = paired | before_second
    weighs_late = last | before_second

    def enter():
        top_sources = jnp.where(paired | second, 1, jnp.maximum(my_col - 3, 0))
        sources = jnp.where(my_row == 0, top_sources, my_col)
        sources = sources + jnp.where(pair_top, 1, 0)
        sources = sources + unknown_above
        sources = sources + jnp.where(has_above, jnp.maximum(my_col - 3, 0), 0)
        sources = sources + jnp.where(has_above & (my_col == 2), 1, 0)
        sources = sources + (near - 1 - my_row) + jnp.where(knows_right, 1, 0)
        await_signals(barrier, sources)

        @pl.when(jnp.logical_not(first | last))
        def _():
            push(0)
            push(4)

        def greet_row(semaphore):
            along_row(first_left, jnp.where(greets_left, my_col - 1, my_col), greet(semaphore))

        pl.when(tail_col)(lambda: greet_row(tail_in))
        pl.when(jnp.logical_not(tail_col))(lambda: greet_row(row_in))
        greet_above(col_in, True)
        direct_tops(greet(far_in))

    corner = cells.at[pl.ds(tile_rows - 8, 8), pl.ds(tile_cols - LANES, LANES)]
    links = (
        (left_out, right_in, 0, -1, has_left & jnp.logical_not(before_second), has_right & jnp.logical_not(paired)),
        (corner, corner_above, 1, 0, has_below, has_above),
        (corner, corner_left, 0, 1, has_right & has_below, has_left & has_below),
        (ends, ends_in, 0, 2, paired, second),
        (left_out, pair_in, 0, 1, before_second, second),
    )

    def link_copy(k):
        source, target, d_row, d_col, _, _ = links[k]
        place = (
            lax.rem(my_row + d_row + grid_rows, grid_rows),
            lax.rem(my_col + d_col + grid_cols, grid_cols),
        )
        return pltpu.make_async_remote_copy(
            src_ref=source, dst_ref=target, send_sem=link_send.at[k], recv_sem=link_recv.at[k],
            device_id=place, device_id_type=MESH,
        )

    def push(k):

        @pl.when(links[k][4])
        def _():
            link_copy(k).start()

    def arrived(k):

        @pl.when(links[k][5])
        def _():
            link_copy(k).wait_recv()

    def send(source, target, send_sem, recv_sem, place):
        return pltpu.make_async_remote_copy(
            src_ref=source, dst_ref=target, send_sem=send_sem, recv_sem=recv_sem,
            device_id=place, device_id_type=MESH,
        )

    def top_copy(r, c):
        line = tops.at[my_row]
        return send(line, line, top_send.at[r], top_recv, (r, c))

    def bottom_copy(r, c):
        return send(bottom_out, bottoms.at[my_row], bottom_send.at[r], bottom_recv, (r, c))

    def row_copy(r, c):
        return send(mine_h.at[1], row_h.at[my_col], h_send.at[r], row_recv, (r, c))

    def far_copy(r, c):
        return send(mine_h.at[1], top_h.at[my_col], h_send.at[r], far_recv, (r, c))

    def origin_copy(r, c):
        return send(mine_h.at[1], row_h.at[0], h_send.at[r], link_recv.at[5], (r, c))

    def relay_in(r, c):
        return send(mine_h.at[2], col_h, c_send.at[r], link_recv.at[6], (r, c))

    def relay_left(r, c):
        return send(mine_h.at[0], col_h, h_send.at[r], link_recv.at[6], (r, c))

    def relay_back(r, c):
        return send(mine_h.at[0], row_h.at[1], back_send, link_recv.at[5], (r, c))

    def left_copy(r, c):
        return send(mine_y, left_d, d_send, link_recv.at[7], (r, c))

    def push_tops(low, high, act):
        along_col(jnp.where(has_above, low, grid_rows), high, act)

    def push_bottoms():
        along_col(my_row + 1, near, lambda r, c: bottom_copy(r, c).start())

    def down_weights():
        outer_row = bottom_out[0:right, :]
        bottom_out[right : 2 * right, :] = weights(
            inner_row[...], outer_row,
            corner_left[6:7, LANES - 1 : LANES], corner_left[7:8, LANES - 1 : LANES],
            my_col == 0,
        )

    def push_down():

        @pl.when(has_below & jnp.logical_not(has_left))
        def _():
            push_bottoms()

        pl.when(jnp.logical_not(tail))(lambda: push(1))
        push(2)

    def row_line(row):
        return jnp.concatenate(
            [cells[row : row + 1, k * LANES : (k + 1) * LANES] for k in range(right)], axis=0
        )

    def col_lines(block, low, high):
        turned = [
            cells[k * LANES : (k + 1) * LANES, block * LANES : (block + 1) * LANES].T
            for k in range(down)
        ]
        return [jnp.concatenate([t[j : j + 1, :] for t in turned], axis=0) for j in range(low, high)]

    with jax.named_scope("enter_0"):
        pl.when(first)(enter)
    with jax.named_scope("load_head"):
        loads[0].wait()
    with jax.named_scope("head"):
        head_line = col_lines(0, 0, 1)[0]
        left_out[0:down, :] = head_line
        left_out[down:, :] = line_counts(head_line)
    with jax.named_scope("push_first"):

        @pl.when(first)
        def _():
            push(0)
            push(4)


    with jax.named_scope("load_edges"):
        loads[1].wait()
        loads[2].wait()
        loads[-1].wait()
        loads[-2].wait()
    with jax.named_scope("last_row"):
        outer_row = row_line(tile_rows - 1)
        down_count = left_out[2 * down - 1 :, LANES - 1 :] - steps_down[0].astype(jnp.float32)
        bottom_out[0:right, :] = outer_row
        bottom_out[2 * right :, :] = down_count + line_counts(outer_row)
        inner_row[...] = row_line(tile_rows - 2)

        @pl.when(jnp.logical_not(has_left))
        def _():
            down_weights()

    with jax.named_scope("enter_1"):
        pl.when(between)(enter)

        @pl.when(jnp.logical_not(last))
        def _():
            push_down()

    with jax.named_scope("first_row"):

        @pl.when(has_above)
        def _():
            first_row = row_line(0)
            tops[my_row, 0:right, :] = first_row
            tops[my_row, right:, :] = line_counts(first_row)

        push_tops(my_row + 1, near, lambda r, c: top_copy(r, c).start())

    lane = iota((STRIP, LANES), 1)

    def strip(k, carry):
        rows = pl.ds(pl.multiple_of(k * STRIP, STRIP), STRIP)
        wrapped_around = cells[rows, 0:LANES]
        sums = jnp.zeros((STRIP, LANES), jnp.float32)
        for j in range(right):
            cols = slice(j * LANES, (j + 1) * LANES)
            here = cells[rows, cols]
            rolled = pltpu.roll(here, 1, 1)
            across = cycles(here - jnp.where(lane == 0, wrapped_around, rolled))
            wrapped_around = rolled
            floors[rows, cols] = across.astype(jnp.bfloat16)
            sums = sums + across
        row_sums[rows, :] = sums.astype(jnp.bfloat16)
        return carry

    def weigh_bottom():
        arrived(2)
        down_weights()
        push_bottoms()

    def push_further_bottoms():
        along_col(near, grid_rows, lambda r, c: bottom_copy(r, c).start())

    def weigh_after():
        with jax.named_scope("weigh_after"):
            pl.when(has_below)(weigh_bottom)
            push_further_bottoms()

    def push_further_tops():
        await_signals(col_in, grid_rows - near)
        pl.when(tail)(lambda: push(1))
        push_tops(near, grid_rows, lambda r, c: top_copy(r, c).start())

    per_chunk = rows_step // STRIP
    for q in range(chunks):
        if q == chunks - 1:
            with jax.named_scope("tail_in"):
                pl.when(tail)(push_further_tops)
                pl.when(has_left & has_below & jnp.logical_not(weighs_late))(weigh_bottom)
        with jax.named_scope(f"load_{q}"):
            loads[q + 3].wait()
        with jax.named_scope(f"floors_{q}"):
            lax.fori_loop(
                q * per_chunk, (q + 1) * per_chunk, strip, 0, unroll=math.gcd(per_chunk, 16)
            )
        if q == (chunks - 1) // 2:
            with jax.named_scope("enter_2"):

                @pl.when(last)
                def _():
                    enter()
                    push(0)
                    push_down()

    with jax.named_scope("corner_left"):
        pl.when(has_left & has_below & weighs_late & jnp.logical_not(feeds))(weigh_bottom)

    with jax.named_scope("col_in"):
        pl.when(jnp.logical_not(tail))(push_further_tops)
        pl.when(jnp.logical_not(feeds))(push_further_bottoms)

    relays = (my_col > 0) & (my_col < 4)
    to_relay = jnp.where(paired | second, 1, grid_rows)
    left_side = has_above & jnp.logical_not(has_left)
    to_right = jnp.where(left_side, 1, grid_cols)
    to_row = jnp.where(pair_top, grid_cols, my_col + 1)
    row_end = jnp.where(before_second, 4, grid_cols)

    def pair_places(act):
        span(jnp.where(origin, 0, 2), 2, lambda k: act(0, 1 + 2 * k))

    def hear_one(ref, semaphore):
        pltpu.make_async_copy(ref, ref, semaphore).wait()

    def end_values():
        with jax.named_scope("ends"):
            ones = jnp.ones((16, LANES), jnp.bfloat16)
            pieces = []
            for k in range(down):
                sums = lax.dot_general(
                    ones, row_sums[k * LANES : (k + 1) * LANES, :], (((1,), (1,)), ((), ())),
                    preferred_element_type=jnp.float32,
                )
                pieces.append(sums[0:1, :])
            end_count = left_out[down:, :] + jnp.concatenate(pieces, axis=0)
            end_count = end_count - steps_across[0].astype(jnp.float32)
            return (end_count, *col_lines(right - 1, LANES - 2, LANES))

    def rest_weights(inner_col, outer_col):
        weight = weights(inner_col, outer_col, inner_col[0:1, 0:1], outer_col[0:1, 0:1], True)
        start = (iota(weight.shape, 0) == 0) & (iota(weight.shape, 1) == 0)
        return jnp.where(start & has_above, 0.0, weight)

    def first_weight(inner, outer):
        inner_before = corner_above[7:8, LANES - 2 : LANES - 1]
        outer_before = corner_above[7:8, LANES - 1 : LANES]
        charge = cycles(outer_before - inner_before) + cycles(outer - outer_before)
        charge = charge - cycles(outer - inner) - cycles(inner - inner_before)
        return jnp.where(has_above, 1.0 / (1.0 + jnp.abs(charge)), 0.0)

    def end_sums(weight, outer_col, end_count, first_col, first_count):
        jump = first_count - end_count - cycles(first_col - outer_col)
        return summed(weight * jump), summed(weight), jump[0:1, 0:1]

    def finish_mean(sums, inner, outer):
        jumps, weight, first_jump = sums
        extra = first_weight(inner, outer)
        return jnp.broadcast_to((jumps + extra * first_jump) / (weight + extra), (1, LANES))

    def across():
        end_count, inner_col, outer_col = end_values()
        with jax.named_scope("weights_h"):
            ends[0:down, :] = rest_weights(inner_col, outer_col)
            ends[down : 2 * down, :] = outer_col
            ends[2 * down :, :] = end_count
            first_inner[...] = inner_col[0:1, :]
            push(3)

        pl.when(paired)(weigh_after)

    def across_mean():
        with jax.named_scope("halo_0"):
            arrived(0)
        with jax.named_scope("base_h"):
            sums = end_sums(
                ends[0:down, :], ends[down : 2 * down, :], ends[2 * down :, :],
                right_in[0:down, :], right_in[down:, :],
            )
            arrived(1)
            mine_h[1] = finish_mean(sums, first_inner[0:1, 0:1], ends[down : down + 1, 0:1])
            pair_places(lambda r, c: origin_copy(r, c).start())

    def across_pair():
        with jax.named_scope("pair"):
            hear_one(row_h.at[0], link_recv.at[5])

            @pl.when(paired)
            def _():
                mine_h[2] = row_h[0]

            @pl.when(second)
            def _():
                arrived(4)
                hear_one(row_h.at[2], row_recv)
                arrived(3)
                jumps, weight, _ = end_sums(
                    ends_in[0:down, :], ends_in[down : 2 * down, :], ends_in[2 * down :, :],
                    pair_in[0:down, :], pair_in[down:, :],
                )
                before = jnp.broadcast_to(jumps / weight, (1, LANES))
                row_h[1] = before
                upto = row_h[0] + before
                mine_h[0] = upto
                mine_h[2] = upto + row_h[2]
                mine_h[1] = mine_h[1] + (upto + row_h[2])
                relay_back(0, 2).start()

            along_col(to_relay, grid_rows, lambda r, c: relay_in(r, c).start())

    inner_cols = grid_cols - 2
    known = jnp.where(knows_right, my_col + 1, my_col)
    inner_unknown = jnp.where(lead, 0, jnp.maximum(inner_cols - 1 - known, 0))
    tail_unknown = jnp.where(lead, 0, grid_cols - 1 - known - inner_unknown)

    def tell_inner():
        await_signals(row_in, inner_unknown)
        along_row(to_right, inner_cols, lambda r, c: left_copy(r, c).start())
        along_row(to_row, jnp.minimum(row_end, inner_cols), lambda r, c: row_copy(r, c).start())

    def tell_tail():
        with jax.named_scope("tail_tell"):
            await_signals(tail_in, tail_unknown)
            along_row(
                jnp.maximum(to_right, inner_cols), grid_cols, lambda r, c: left_copy(r, c).start()
            )
            along_row(
                jnp.maximum(to_row, inner_cols), row_end, lambda r, c: row_copy(r, c).start()
            )

    def tell():
        with jax.named_scope("row_in"):
            tell_inner()
            tell_tail()

        pl.when(before_second)(weigh_after)

    def tell_far():
        with jax.named_scope("far_in"):
            right_count = grid_cols - 1 - my_col + jnp.where(second, 1, 0)
            await_signals(far_in, jnp.where(direct_top, (grid_rows - 1) * right_count, 0))
            left_below(lambda r, c: relay_left(r, c).start())
            far_below(lambda r, c: far_copy(r, c).start())

    def hear(slots, semaphore, first, count):
        for n in range(1, slots.shape[0] - max(first - 1, 0)):

            @pl.when(count == n)
            def _():
                landed = slots.at[pl.ds(first, n)]
                pltpu.make_async_copy(landed, landed, semaphore).wait()

    def hear_above():
        with jax.named_scope("hear_y"):
            hear(tops, top_recv, 1, my_row - 1)
            hear(bottoms, bottom_recv, 0, my_row)

    def sum_above():
        down_here = jnp.zeros((1, 1), jnp.float32)
        for k in range(grid_rows - 1):
            value = mismatch(
                bottoms[k, right : 2 * right, :], bottoms[k, 0:right, :],
                bottoms[k, 2 * right :, :], tops[k + 1, 0:right, :], tops[k + 1, right:, :],
            )
            down_here = down_here + jnp.where(k < my_row, value, 0.0)
        mine_y[...] = jnp.broadcast_to(down_here, mine_y.shape)

    def down_sum():
        hear_above()
        with jax.named_scope("base_y"):
            pl.when(has_above)(sum_above)

    def left_start():
        end_count, inner_col, outer_col = end_values()
        with jax.named_scope("halo_left"):
            arrived(0)
        with jax.named_scope("weights_left"):
            sums = end_sums(
                rest_weights(inner_col, outer_col), outer_col, end_count,
                right_in[0:down, :], right_in[down:, :],
            )
            for k, value in enumerate((*sums, inner_col[0:1, 0:1], outer_col[0:1, 0:1])):
                left_sums[k] = jnp.broadcast_to(value, (1, LANES))

    def left_finish():
        with jax.named_scope("halo_left_1"):
            arrived(1)
            jumps, weight, jump, inner, outer = (left_sums[k] for k in range(5))
            mine_h[1] = finish_mean((jumps, weight, jump), inner, outer)
        hear_above()
        with jax.named_scope("base_left"):
            sum_above()
        with jax.named_scope("row_in_left"):
            tell_inner()

    def integrate(low, high):
        with jax.named_scope(f"integrate_{low}"):
            upper, lower = triangle(cols_step, 0), triangle(rows_step, 1)
            down_carry = jnp.zeros((1, LANES), jnp.float32) if low == 0 else carried[...]
            for q in range(low, high):
                top = q * rows_step
                rows = pl.ds(top, rows_step)
                head = cells[rows, 0:LANES]
                above = cells[max(top - 1, 0) : max(top, 1), 0:LANES]
                before = jnp.where(iota(head.shape, 0) == 0, above, pltpu.roll(head, 1, 0))
                counts = down_carry + jnp.dot(
                    lower, cycles(head - before).astype(jnp.bfloat16),
                    preferred_element_type=jnp.float32,
                )
                down_carry = counts[rows_step - 1 : rows_step, :]
                carry = counts[:, 0:1]
                for b in range(tile_cols // cols_step):
                    cols = slice(b * cols_step, (b + 1) * cols_step)
                    count = carry + jnp.dot(
                        floors[rows, cols], upper, preferred_element_type=jnp.float32
                    )
                    carry = count[:, cols_step - 1 : cols_step]
                    integ[rows, cols] = cells[rows, cols] * (1.0 / TWO_PI) - count
            if high < chunks:
                carried[...] = down_carry

    odd_row = lax.rem(my_row, 2) == 1
    far_early = (my_row == 0) & (my_col > 3)
    split = (even_row & has_left) | (tail_col & odd_row) | (lax.rem(my_col, 2) == 1)
    half = (chunks + 1) // 2
    never = 11
    at_left, at_top, at_pair, at_split, at_second, otherwise = range(6)
    kind = jnp.where(second, at_second, jnp.where(split, at_split, otherwise))
    kind = jnp.where(pair, jnp.where(paired, at_top, at_pair), kind)
    kind = jnp.where(left_side, at_left, kind)

    def pick(*slots):
        chosen = slots[otherwise]
        for k in range(otherwise):
            chosen = jnp.where(kind == k, slots[k], chosen)
        return chosen

    order = (
        (left_start, pick(0, never, never, never, never, never)),
        (left_finish, pick(jnp.where(my_row == 1, 1, 2), never, never, never, never, never)),
        (tell_tail, pick(3, never, never, never, never, never)),
        (across, jnp.where(has_right, pick(never, 0, 1, 1, 1, 0), never)),
        (across_mean, jnp.where(has_right, pick(never, never, 2, 2, 2, 1), never)),
        (across_pair, pick(never, 2, never, never, 3, never)),
        (tell, pick(never, never, 3, 3, 4, 2)),
        (functools.partial(integrate, 0, half), pick(jnp.where(my_row == 1, 2, 1), 1, 0, 0, 0, jnp.where(far_early, 4, 3))),
        (tell_far, jnp.where(direct_top, jnp.where(second, 5, jnp.where(far_early, 3, 4)), never)),
        (functools.partial(integrate, half, chunks), pick(4, 3, 5, 4, 6, 5)),
        (down_sum, pick(never, never, 4, 5, never, 6)),
    )

    def phase(k, carry):
        for act, at in order:
            pl.when(k == at)(act)
        return carry

    lax.fori_loop(0, len(order), phase, 0)

    pl.when(jnp.logical_not(has_right | left_side))(lambda: arrived(1))

    with jax.named_scope("sent"):
        for k in range(5):

            @pl.when(links[k][4])
            def _():
                link_copy(k).wait_send()

        push_tops(my_row + 1, grid_rows, lambda r, c: top_copy(r, c).wait_send())
        along_col(my_row + 1, grid_rows, lambda r, c: bottom_copy(r, c).wait_send())
        along_col(to_relay, grid_rows, lambda r, c: relay_in(r, c).wait_send())

        def sent(semaphore, count):
            for n in range(1, grid_cols):

                @pl.when(count == n)
                def _():
                    line = row_h.at[pl.ds(0, n)]
                    pltpu.make_async_copy(line, line, semaphore).wait()

        told = jnp.where(origin, 2, jnp.maximum(row_end - to_row, 0))
        sent(h_send.at[my_row], told)
        sent(d_send, jnp.maximum(grid_cols - to_right, 0))
        far_told = grid_cols - 1 - my_col + jnp.where(second, 1, 0)
        far_low = jnp.where(direct_top, 1, grid_rows)
        span(far_low, grid_rows, lambda r: sent(h_send.at[r], far_told))

        @pl.when(second)
        def _():
            relay_back(0, 2).wait_send()

    with jax.named_scope("hear"):
        hear(row_h, row_recv, 3, jnp.where(has_above, 0, my_col - 3))
        hear(row_h, row_recv, 0, jnp.where(has_above, my_col, 0))
        hear(top_h, far_recv, 3, jnp.where(has_above, my_col - 3, 0))

        @pl.when(has_above & relays)
        def _():
            hear_one(col_h, link_recv.at[6])

        @pl.when(before_second)
        def _():
            hear_one(row_h.at[1], link_recv.at[5])

        @pl.when(has_above & has_left)
        def _():
            hear_one(left_d, link_recv.at[7])

    with jax.named_scope("finish"):

        def prefix(slots):
            line = slots[0]
            for k in range(1, grid_cols):
                line = line + slots[k]
            return line

        across_here = prefix(row_h)
        across_top = prefix(top_h) + jnp.where(relays, col_h[...], 0.0)
        across_top = jnp.where(has_above, across_top, across_here)
        down_here = mine_y[...]
        down_left = jnp.where(has_left & has_above, left_d[...], down_here)
        here = left = top = start = zero_line
        for sweep in range(ITERS):
            prefix_across = across_here + (left - here)
            prefix_across_top = across_top + (start - top)
            prefix_down = down_here + (top - here)
            prefix_down_left = down_left + (start - left)
            here = here + 0.5 * (prefix_across + prefix_across_top + prefix_down + prefix_down_left)
            left = left + prefix_down_left
            top = top + prefix_across_top
        offset[...] = jnp.broadcast_to(here, offset.shape)


def place_kernel(parts, integ, offset, out, ready):
    pl.run_scoped(
        functools.partial(place_rows, parts, integ, offset, out, ready),
        pltpu.SemaphoreType.DMA((parts,)),
    )


def place_rows(parts, integ, offset, out, ready, sems):
    step = integ.shape[0] // parts
    shift = offset[0:1, 0:1]
    copies = []
    for q in range(parts):
        rows = pl.ds(q * step, step)
        ready[rows, :] = integ[rows, :] + shift
        copy = pltpu.make_async_copy(ready.at[rows], out.at[rows], sems.at[q])
        copy.start()
        copies.append(copy)
    for copy in copies:
        copy.wait()


def on_device(names, sizes, wrapped, col_steps, row_steps):
    frames, tile_rows, tile_cols = wrapped.shape
    grid_rows, grid_cols = sizes
    down, right = tile_rows // LANES, tile_cols // LANES
    dma = pltpu.SemaphoreType.DMA
    rows_step = math.gcd(tile_rows, 256)
    cols_step = math.gcd(tile_cols, 256)
    f32 = jnp.float32

    def with_local_semaphores(*refs):
        pl.run_scoped(
            functools.partial(edge_kernel, names, sizes, rows_step, cols_step, *refs),
            dma((8,)), dma, dma, dma, dma,
            *[pltpu.SemaphoreType.REGULAR] * 4,
            dma((tile_rows // rows_step + 5,)), dma((5,)), dma((grid_rows,)), dma((grid_rows,)),
            dma((grid_rows,)), dma((grid_rows,)), dma, dma,
        )

    call = pl.pallas_call(
        with_local_semaphores,
        out_shape=(
            pltpu.VMEM((tile_rows, tile_cols), f32),
            pltpu.VMEM((8, LANES), f32),
        ),
        in_specs=[
            pl.BlockSpec(memory_space=pltpu.HBM),
            pl.BlockSpec(memory_space=pltpu.HBM),
            pl.BlockSpec(memory_space=pltpu.HBM),
        ],
        out_specs=(
            pl.BlockSpec(memory_space=pltpu.VMEM),
            pl.BlockSpec(memory_space=pltpu.VMEM),
        ),
        scratch_shapes=[
            pltpu.VMEM((tile_rows, tile_cols), f32),
            pltpu.VMEM((2 * down, LANES), f32),
            pltpu.VMEM((2 * down, LANES), f32),
            pltpu.VMEM((8, LANES), f32),
            pltpu.VMEM((8, LANES), f32),
            pltpu.VMEM((grid_rows, 2 * right, LANES), f32),
            pltpu.VMEM((3 * right, LANES), f32),
            pltpu.VMEM((grid_rows, 3 * right, LANES), f32),
            pltpu.VMEM((right, LANES), f32),
            pltpu.VMEM((tile_rows, tile_cols), jnp.bfloat16),
            pltpu.VMEM((tile_rows, LANES), jnp.bfloat16),
            pltpu.VMEM((1, 1, 1), jnp.int32),
            pltpu.VMEM((1, 1, 1), jnp.int32),
            pltpu.VMEM((3, 1, LANES), f32),
            pltpu.VMEM((1, LANES), f32),
            pltpu.VMEM((grid_cols, 1, LANES), f32),
            pltpu.VMEM((grid_cols, 1, LANES), f32),
            pltpu.VMEM((1, LANES), f32),
            pltpu.VMEM((1, LANES), f32),
            pltpu.VMEM((1, LANES), f32),
            pltpu.VMEM((3 * down, LANES), f32),
            pltpu.VMEM((3 * down, LANES), f32),
            pltpu.VMEM((2 * down, LANES), f32),
            pltpu.VMEM((1, LANES), f32),
            pltpu.VMEM((5, 1, LANES), f32),
        ],
        compiler_params=pltpu.CompilerParams(
            collective_id=0, has_side_effects=True, vmem_limit_bytes=57 * 1024 * 1024
        ),
    )
    parts = math.gcd(tile_rows // 8, 32)
    place = pl.pallas_call(
        functools.partial(place_kernel, parts),
        out_shape=jax.ShapeDtypeStruct((tile_rows, tile_cols), f32),
        in_specs=[pl.BlockSpec(memory_space=pltpu.VMEM), pl.BlockSpec(memory_space=pltpu.VMEM)],
        out_specs=pl.BlockSpec(memory_space=pltpu.HBM),
        scratch_shapes=[pltpu.VMEM((tile_rows, tile_cols), f32)],
        compiler_params=pltpu.CompilerParams(vmem_limit_bytes=24 * 1024 * 1024),
    )
    outs = [
        place(*call(wrapped[f : f + 1], col_steps[f : f + 1], row_steps[f : f + 1]))
        for f in range(frames)
    ]
    return jnp.stack(outs)


def solution(mesh):
    spec = P(None, "row", "col")
    sizes = (mesh.shape["row"], mesh.shape["col"])
    return jax.shard_map(
        functools.partial(on_device, ("row", "col"), sizes),
        mesh=mesh, in_specs=(spec, spec, spec), out_specs=spec, check_vma=False,
    )
```
